32 devices in a mesh: dp: 4 (over y, z), tp: 8 (over x, core).
Axes of the slice: x: 4, y: 2, z: 2, core: 2. Of those that a mesh axis runs over, the one named last changes fastest.
The devices are a block of a 4x4x8 slice.
Arguments:
- y_one: float32 [32, 32, 2048], P('dp'), parts along dimension 0
- y_two: float32 [32, 32, 2048], P('dp'), parts along dimension 0
- dy_one: float32 [32, 32, 2048], P('dp'), parts along dimension 0
- dy_two: float32 [32, 32, 2048], P('dp'), parts along dimension 0
- seq_lens: int32 [32], P('dp'), parts along dimension 0
- w_query: bfloat16 [1, 2048, 16, 128], P(None, None, 'tp')
- w_key: bfloat16 [1, 2048, 8, 128], P(None, None, 'tp')
- w_value: bfloat16 [1, 2048, 8, 128], P(None, None, 'tp')
- w_out: bfloat16 [1, 16, 128, 2048], P(None, 'tp')
- w_up: bfloat16 [1, 2048, 8192], P(None, None, 'tp')
- w_down: bfloat16 [1, 8192, 2048], P(None, 'tp')
Outputs:
- output 1: float32 [32, 32, 2048], P('dp'), parts along dimension 0
- output 2: float32 [32, 32, 2048], P('dp'), parts along dimension 0
- output 3: float32 [32, 32, 2048], P('dp'), parts along dimension 0
- output 4: float32 [32, 32, 2048], P('dp'), parts along dimension 0
- output 5: float32 [4, 2048, 16, 128], P('dp', None, 'tp'), parts along dimension 0
- output 6: float32 [4, 2048, 8, 128], P('dp', None, 'tp'), parts along dimension 0
- output 7: float32 [4, 2048, 8, 128], P('dp', None, 'tp'), parts along dimension 0
- output 8: float32 [4, 16, 128, 2048], P('dp', 'tp'), parts along dimension 0
- output 9: float32 [4, 2048, 8192], P('dp', None, 'tp'), parts along dimension 0
- output 10: float32 [4, 8192, 2048], P('dp', 'tp'), parts along dimension 0
There are 4 independent parts. The reference program is written for one: setup_inputs(seed, part) draws one part's arguments, and reference() takes and returns one part's arrays. A program takes and returns all parts, laid end to end along the dimension named above; an argument that names none is the same for every part.
All inputs are finite; a program needn't handle non-finite values.
Results may differ from the reference program's by a relative error of at most 0.00909837.
Values are sent between devices in bfloat16 or wider.
A program may use at most 768 MiB of HBM per device.

```python
import functools
import jax
import jax.numpy as jnp
from jax import lax

D = 2048
HEADS = 16
KV_HEADS = 1
HEAD = 128
FF = 8192
LAYERS = 1
SEQS = 1
SEQ = 32
TP = 8
KV_SLOTS = max(KV_HEADS, TP)
REPEAT = KV_SLOTS // KV_HEADS
GROUP = HEADS // KV_SLOTS
BATCH = SEQS * TP
TOKENS = BATCH * SEQ
EPS = 1e-5
SCORE_SCALE = HEAD ** -0.5
OUT_GAIN = 0.5 * (SEQ / 64) ** 0.25


def normal_weights(rng_key, arr_shape, scale_std):
    return (jax.random.normal(rng_key, arr_shape, jnp.float32) * scale_std).astype(jnp.bfloat16)


def draw_lengths(rng_key):
    len_key, top_key, low_key = jax.random.split(rng_key, 3)
    seq_lens = jax.random.randint(len_key, (BATCH,), SEQ // 4, SEQ + 1)
    top_idx = jax.random.randint(top_key, (), 0, BATCH)
    low_idx = (top_idx + jax.random.randint(low_key, (), 1, BATCH)) % BATCH
    positions = jnp.arange(BATCH)
    seq_lens = jnp.where(positions == top_idx, SEQ, seq_lens)
    seq_lens = jnp.where(positions == low_idx, SEQ // 4, seq_lens)
    return seq_lens.astype(jnp.int32)


def setup_inputs(seed: int = 0, part: int = 0) -> dict:
    weight_keys = jax.random.split(jax.random.key(seed), 6)
    part_keys = jax.random.split(jax.random.fold_in(jax.random.key(seed + 1), part), 5)
    act_shape = (BATCH, SEQ, D)
    key_heads = normal_weights(weight_keys[1], (LAYERS, D, KV_HEADS, HEAD), D ** -0.5)
    value_heads = normal_weights(weight_keys[2], (LAYERS, D, KV_HEADS, HEAD), D ** -0.5)
    return {
        'y_one': jax.random.normal(part_keys[0], act_shape, jnp.float32),
        'y_two': jax.random.normal(part_keys[1], act_shape, jnp.float32),
        'dy_one': jax.random.normal(part_keys[2], act_shape, jnp.float32),
        'dy_two': jax.random.normal(part_keys[3], act_shape, jnp.float32),
        'seq_lens': draw_lengths(part_keys[4]),
        'w_query': normal_weights(weight_keys[0], (LAYERS, D, HEADS, HEAD), 2.0 * D ** -0.5),
        'w_key': jnp.repeat(key_heads, REPEAT, axis=2),
        'w_value': jnp.repeat(value_heads, REPEAT, axis=2),
        'w_out': normal_weights(weight_keys[3], (LAYERS, HEADS, HEAD, D), OUT_GAIN * (HEADS * HEAD) ** -0.5),
        'w_up': normal_weights(weight_keys[4], (LAYERS, D, FF), D ** -0.5),
        'w_down': normal_weights(weight_keys[5], (LAYERS, FF, D), 0.6 * FF ** -0.5),
    }


def rms_norm(x_val):
    inv_rms = lax.rsqrt(jnp.mean(x_val * x_val, axis=-1, keepdims=True) + EPS)
    return x_val * inv_rms, inv_rms


def rms_back(normed, inv_rms, grad_norm):
    return inv_rms * (grad_norm - normed * jnp.mean(grad_norm * normed, axis=-1, keepdims=True))


def attend_seq(operands):
    q_seq, k_seq, v_seq, dout_seq, seq_len = operands
    q_grp = q_seq.reshape(SEQ, KV_SLOTS, GROUP, HEAD).astype(jnp.float32)
    k_full = k_seq.astype(jnp.float32)
    v_full = v_seq.astype(jnp.float32)
    dout_grp = dout_seq.reshape(SEQ, KV_SLOTS, GROUP, HEAD).astype(jnp.float32)
    row_pos = jnp.arange(SEQ)[:, None]
    col_pos = jnp.arange(SEQ)[None, :]
    visible = (col_pos <= row_pos) & (col_pos < seq_len)
    scores = jnp.einsum('igre,jge->grij', q_grp, k_full) * SCORE_SCALE
    scores = jnp.where(visible, scores, -1e30)
    attn_probs = jax.nn.softmax(scores, axis=-1)
    probs_b = attn_probs.astype(jnp.bfloat16).astype(jnp.float32)
    attn_out = jnp.einsum('grij,jge->igre', probs_b, v_full).astype(jnp.bfloat16)
    d_value = jnp.einsum('grij,igre->jge', probs_b, dout_grp).astype(jnp.bfloat16)
    d_probs = jnp.einsum('igre,jge->grij', dout_grp, v_full)
    d_scores = attn_probs * (d_probs - jnp.sum(d_probs * attn_probs, axis=-1, keepdims=True)) * SCORE_SCALE
    d_scores = d_scores.astype(jnp.bfloat16).astype(jnp.float32)
    d_query = jnp.einsum('grij,jge->igre', d_scores, k_full).astype(jnp.bfloat16)
    d_key = jnp.einsum('grij,igre->jge', d_scores, q_grp).astype(jnp.bfloat16)
    return attn_out.reshape(SEQ, HEADS, HEAD), d_query.reshape(SEQ, HEADS, HEAD), d_key, d_value


def layer_back(seq_lens, carry, layer_w):
    y_one, y_two, dy_one, dy_two = carry
    w_query, w_key, w_value, w_out, w_up, w_down = layer_w
    norm_g, inv_g = rms_norm(y_one.reshape(TOKENS, D))
    norm_g_b = norm_g.astype(jnp.bfloat16)
    pre_act = jnp.dot(norm_g_b, w_up, preferred_element_type=jnp.float32)
    act_val, gelu_back = jax.vjp(jax.nn.gelu, pre_act)
    act_b = act_val.astype(jnp.bfloat16)
    g_branch = jnp.dot(act_b, w_down, preferred_element_type=jnp.float32)
    x_two = y_two - g_branch.reshape(BATCH, SEQ, D)
    dy2_b = dy_two.reshape(TOKENS, D).astype(jnp.bfloat16)
    d_act = jnp.dot(dy2_b, w_down.T, preferred_element_type=jnp.float32)
    d_pre = gelu_back(d_act)[0].astype(jnp.bfloat16)
    dw_down = jnp.dot(act_b.T, dy2_b, preferred_element_type=jnp.float32)
    dw_up = jnp.dot(norm_g_b.T, d_pre, preferred_element_type=jnp.float32)
    grad_norm_g = jnp.dot(d_pre, w_up.T, preferred_element_type=jnp.float32)
    dy_one = dy_one + rms_back(norm_g, inv_g, grad_norm_g).reshape(BATCH, SEQ, D)

    norm_f, inv_f = rms_norm(x_two.reshape(TOKENS, D))
    norm_f_b = norm_f.astype(jnp.bfloat16)
    wq_flat = w_query.reshape(D, HEADS * HEAD)
    wk_flat = w_key.reshape(D, KV_SLOTS * HEAD)
    wv_flat = w_value.reshape(D, KV_SLOTS * HEAD)
    wo_flat = w_out.reshape(HEADS * HEAD, D)
    q_all = jnp.dot(norm_f_b, wq_flat, preferred_element_type=jnp.float32).astype(jnp.bfloat16).reshape(BATCH, SEQ, HEADS, HEAD)
    k_all = jnp.dot(norm_f_b, wk_flat, preferred_element_type=jnp.float32).astype(jnp.bfloat16).reshape(BATCH, SEQ, KV_SLOTS, HEAD)
    v_all = jnp.dot(norm_f_b, wv_flat, preferred_element_type=jnp.float32).astype(jnp.bfloat16).reshape(BATCH, SEQ, KV_SLOTS, HEAD)
    dy1_b = dy_one.reshape(TOKENS, D).astype(jnp.bfloat16)
    d_attn = jnp.dot(dy1_b, wo_flat.T, preferred_element_type=jnp.float32).astype(jnp.bfloat16).reshape(BATCH, SEQ, HEADS, HEAD)
    attn_out, d_query, d_key, d_value = lax.map(attend_seq, (q_all, k_all, v_all, d_attn, seq_lens))
    out_flat = attn_out.reshape(TOKENS, HEADS * HEAD)
    f_branch = jnp.dot(out_flat, wo_flat, preferred_element_type=jnp.float32)
    x_one = y_one - f_branch.reshape(BATCH, SEQ, D)
    dw_out = jnp.dot(out_flat.T, dy1_b, preferred_element_type=jnp.float32).reshape(HEADS, HEAD, D)
    dq_flat = d_query.reshape(TOKENS, HEADS * HEAD)
    dk_flat = d_key.reshape(TOKENS, KV_SLOTS * HEAD)
    dv_flat = d_value.reshape(TOKENS, KV_SLOTS * HEAD)
    dw_query = jnp.dot(norm_f_b.T, dq_flat, preferred_element_type=jnp.float32).reshape(D, HEADS, HEAD)
    dw_key = jnp.dot(norm_f_b.T, dk_flat, preferred_element_type=jnp.float32).reshape(D, KV_SLOTS, HEAD)
    dw_value = jnp.dot(norm_f_b.T, dv_flat, preferred_element_type=jnp.float32).reshape(D, KV_SLOTS, HEAD)
    grad_norm_f = (jnp.dot(dq_flat, wq_flat.T, preferred_element_type=jnp.float32)
                   + jnp.dot(dk_flat, wk_flat.T, preferred_element_type=jnp.float32)
                   + jnp.dot(dv_flat, wv_flat.T, preferred_element_type=jnp.float32))
    dx_two = dy_two + rms_back(norm_f, inv_f, grad_norm_f).reshape(BATCH, SEQ, D)
    return (x_one, x_two, dy_one, dx_two), (dw_query, dw_key, dw_value, dw_out, dw_up, dw_down)


def reference(y_one, y_two, dy_one, dy_two, seq_lens, w_query, w_key, w_value, w_out, w_up, w_down):
    end_state, layer_grads = lax.scan(functools.partial(layer_back, seq_lens), (y_one, y_two, dy_one, dy_two), (w_query, w_key, w_value, w_out, w_up, w_down), reverse=True)
    return (end_state[0], end_state[1], end_state[2], end_state[3], layer_grads[0], layer_grads[1], layer_grads[2], layer_grads[3], layer_grads[4], layer_grads[5])
```

```python
import functools
import jax
import jax.numpy as jnp
from jax import lax
from jax.experimental import pallas as pl
from jax.experimental.pallas import tpu as pltpu
from jax.sharding import PartitionSpec as P

F32 = jnp.float32
BF16 = jnp.bfloat16
EPS = 1e-5
MASK_VALUE = -1e30
GELU_C = 0.7978845608028654
GELU_A = 0.044715
MESH = pl.DeviceIdType.MESH
ANY = pl.BlockSpec(memory_space=pl.ANY)

N_CHUNKS = 4
N_SUMS = 4
N_MSGS = 12

LOAD_US = 2.5
MSG_US = ((1.5, 1.0),) + ((2.8, 1.9),) * 6 + ((5.6, 1.9),) * 2 + ((2.8, 1.9),) * 2 + ((1.5, 1.0),)
STEP_US = {'G1': 3.6, 'G2': 3.2, 'G3': 4.0, 'G4': 4.0, 'ATF': 8.0, 'ATO': 2.0, 'ATB': 9.6, 'ATG': 3.6}
SUM_US = {'F0': 0.03, 'F1': 0.2, 'F2R': 0.05, 'F2L': 0.05, 'F3': 0.25, 'F4R': 0.03, 'F4L': 0.03, 'F5': 0.03, 'F6': 0.03}
SENDS = {'F0': (0,), 'F1': (1, 2, 3, 4), 'F2R': (5,), 'F2L': (6,), 'F3': (7, 8), 'F4R': (9,), 'F4L': (10,), 'F5': (11,)}
RECVS = {'F1': (0,), 'F2R': (1,), 'F2L': (2,), 'F3': (3, 4, 5, 6), 'F4R': (7,), 'F4L': (8,), 'F5': (9, 10), 'F6': (11,)}
AFTER = {'F1': ('F0',), 'F2R': ('F1',), 'F2L': ('F1',), 'F3': ('F2R', 'F2L'), 'F4R': ('F3',), 'F4L': ('F3',),
         'F5': ('F4R', 'F4L'), 'F6': ('F5',)}
SOURCE = ('G2', 'G4', 'ATO', 'ATG')
NEEDS = {'G1': (), 'G2': ('G1',), 'G3': ('G1',), 'G4': ('G3',), 'ATF': (), 'ATO': ('ATF',), 'ATB': ('ATF',), 'ATG': ('ATB',)}
RANK = ('G1', 'G2', 'ATF', 'ATO', 'ATB', 'ATG', 'G3', 'G4')


def plan_order():
    todo = {}
    for c in range(N_CHUNKS):
        for name, pre in NEEDS.items():
            needs = [(p, c) for p in pre]
            if name in ('ATF', 'ATB'):
                needs.append(('F6', int(name == 'ATB'), c))
            todo[name, c] = (needs, STEP_US[name] / N_CHUNKS / 2, ())
        for a in range(N_SUMS):
            for name, cost in SUM_US.items():
                needs = [(p, a, c) for p in AFTER.get(name, ())] + [(i, a, c) for i in RECVS.get(name, ())]
                if name == 'F0':
                    needs.append((SOURCE[a], c))
                todo[name, a, c] = (needs, cost, SENDS.get(name, ()))

    def rank(key):
        if key[0] in STEP_US:
            pos = RANK.index(key[0])
            return (-1, key[1], pos) if pos < 2 else (1, pos, key[1])
        return (0,) + key[1:] + (key[0],)

    now, order, done, free = LOAD_US, [], {}, {}
    while todo:
        ready = {k: max([done[n] for n in v[0]], default=0.0) for k, v in todo.items() if all(n in done for n in v[0])}
        now = max(now, min(ready.values()))
        key = min((k for k, at in ready.items() if at <= now), key=rank)
        _, cost, sends = todo.pop(key)
        now += cost
        done[key] = now
        order.append(key)
        for i in sends:
            link = 0 if i in (0, 11) else 1 + i % 2
            wire, delay = MSG_US[i]
            start = max(now, free.get(link, 0.0))
            free[link] = start + wire / N_CHUNKS
            done[(i,) + key[1:]] = free[link] + delay
    return order


def mm(lhs, rhs):
    return jnp.dot(lhs, rhs, preferred_element_type=F32)


def mm_nt(lhs, rhs):
    return lax.dot_general(lhs, rhs, (((1,), (1,)), ((), ())), preferred_element_type=F32)


def mm_tn(lhs, rhs):
    return lax.dot_general(lhs, rhs, (((0,), (0,)), ((), ())), preferred_element_type=F32)


def inv_rms(x_val):
    return lax.rsqrt(jnp.mean(x_val * x_val, axis=-1, keepdims=True) + EPS)


def rms_back(x_val, grad_norm):
    inv = inv_rms(x_val)
    normed = x_val * inv
    return inv * (grad_norm - normed * jnp.mean(grad_norm * normed, axis=-1, keepdims=True))


def block_kernel(n_tp, head_dim, seq_len,
                 lens_ref, y1_hbm, y2_hbm, dy1_hbm, dy2_hbm, wq_hbm, wk_hbm, wv_hbm, wo_hbm, w1_hbm, w2_hbm,
                 x1_hbm, x2_hbm, dx1_hbm, dx2_hbm, ng_hbm, nf_hbm, act_hbm, dpre_hbm, attn_hbm, dqkv_hbm,
                 w1, w2, wqkv, wo, y1, dy2, y2_own, dy1_own, ng, nf, act, dact, dpre, qkv, prob, attn, dqkv,
                 part, d2d, ring1, ring2, full,
                 load_sem, out_sem, send_sem, recv_sem):
    tokens, width = y1.shape
    ff = w1.shape[1]
    qdim = attn.shape[1]
    n_heads = qdim // head_dim
    chunk = tokens // N_CHUNKS
    half = chunk // 2
    piece = half // (n_tp // 2)
    hw = width // 2
    n_chips = n_tp // 2

    me = lax.axis_index('tp')
    core = lax.rem(me, 2)
    chip = lax.div(me, 2)
    partner = me + 1 - 2 * core
    right = lax.rem(me + 2, n_tp)
    left = lax.rem(me + n_tp - 2, n_tp)
    chip_r = lax.rem(chip + 1, n_chips)
    chip_l = lax.rem(chip + n_chips - 1, n_chips)
    chip_o = lax.rem(chip + 2, n_chips)

    def half_rows(c, k):
        return pl.ds(pl.multiple_of(c * chunk + k * half, half), half)

    def piece_rows(c, x):
        return pl.ds(pl.multiple_of(c * chunk + core * half + x * piece, piece), piece)

    def own_rows(c):
        return pl.ds(c * piece, piece)

    lo, hi = pl.ds(0, hw), pl.ds(hw, hw)

    barrier = pltpu.get_barrier_semaphore()
    for dev in (partner, left, right):
        pl.semaphore_signal(barrier, inc=1, device_id={'tp': dev}, device_id_type=MESH)

    loads = {}

    def load(name, src, dst):
        loads[name] = pltpu.make_async_copy(src, dst, load_sem.at[len(loads)])
        loads[name].start()

    def arrived(*names):
        for name in names:
            if name in loads:
                loads.pop(name).wait()

    n_blk = ff // 256
    waits = []

    def load_all():
        c_rows = [pl.ds(c * chunk, chunk) for c in range(N_CHUNKS)]
        load_list = [(('y1', 0), y1_hbm.at[c_rows[0]], y1.at[c_rows[0]])]
        load_list += [(('w1', j), w1_hbm.at[:, pl.ds(j * 256, 256)], w1.at[:, pl.ds(j * 256, 256)]) for j in range(n_blk)]
        load_list += [(('y1', c), y1_hbm.at[c_rows[c]], y1.at[c_rows[c]]) for c in range(1, N_CHUNKS)]
        load_list += [(('w2',), w2_hbm, w2), (('dy2',), dy2_hbm, dy2)]
        for c in range(N_CHUNKS):
            load_list += [(('y2o', c), y2_hbm.at[piece_rows(c, chip)], y2_own.at[own_rows(c)]),
                          (('dy1o', c), dy1_hbm.at[piece_rows(c, chip)], dy1_own.at[own_rows(c)])]
        kv = head_dim
        load_list += [(('wqkv', 0), wq_hbm, wqkv.at[:, pl.ds(0, qdim)]),
                      (('wqkv', 1), wk_hbm, wqkv.at[:, pl.ds(qdim, kv)]),
                      (('wqkv', 2), wv_hbm, wqkv.at[:, pl.ds(qdim + kv, kv)]),
                      (('wo',), wo_hbm, wo)]
        for i, (name, src, dst) in enumerate(load_list):
            copy = pltpu.make_async_copy(src, dst, load_sem.at[i])
            copy.start()
            loads[name] = copy

    outs = []

    def store(src, dst):
        copy = pltpu.make_async_copy(src, dst, out_sem.at[len(outs)])
        copy.start()
        outs.append(copy)

    def msg(a, c, i):
        rows_own, rows_r, rows_l, rows_o = (piece_rows(c, x) for x in (chip, chip_r, chip_l, chip_o))
        u = a * N_CHUNKS + c
        slot = pl.ds(u * piece, piece)
        pa, oa = part.at[a], full.at[a]
        if i == 0:
            src, dst, dev = pa.at[half_rows(c, 1 - core)], d2d.at[pl.ds(u * half, half)], partner
        elif i == 1:
            src, dst, dev = pa.at[rows_o, lo], ring1.at[0, slot], right
        elif i == 2:
            src, dst, dev = pa.at[rows_o, hi], ring1.at[1, slot], left
        elif i == 3:
            src, dst, dev = pa.at[rows_r, hi], ring2.at[0, slot, hi], right
        elif i == 4:
            src, dst, dev = pa.at[rows_l, lo], ring2.at[1, slot, lo], left
        elif i == 5:
            src, dst, dev = pa.at[rows_r, lo], ring2.at[0, slot, lo], right
        elif i == 6:
            src, dst, dev = pa.at[rows_l, hi], ring2.at[1, slot, hi], left
        elif i == 7:
            src, dst, dev = oa.at[rows_own], oa.at[rows_own], right
        elif i == 8:
            src, dst, dev = oa.at[rows_own], oa.at[rows_own], left
        elif i == 9:
            src, dst, dev = oa.at[rows_l, lo], oa.at[rows_l, lo], right
        elif i == 10:
            src, dst, dev = oa.at[rows_r, hi], oa.at[rows_r, hi], left
        else:
            src, dst, dev = oa.at[half_rows(c, core)], oa.at[half_rows(c, core)], partner
        return pltpu.make_async_remote_copy(src, dst, send_sem.at[i, u], recv_sem.at[i, u],
                                            device_id={'tp': dev}, device_id_type=MESH)

    def send(a, c, *ids):
        for i in ids:
            msg(a, c, i).start()

    def recv(a, c, *ids):
        for i in ids:
            msg(a, c, i).wait_recv()

    state = {'met': False}

    def f0(a, c):
        if not state['met']:
            pl.semaphore_wait(barrier, 3)
            state['met'] = True
        send(a, c, 0)

    def f1(a, c):
        recv(a, c, 0)
        rows = half_rows(c, core)
        part[a, rows] = part[a, rows] + d2d[pl.ds((a * N_CHUNKS + c) * half, half)]
        send(a, c, 1, 2, 3, 4)

    def f2r(a, c):
        recv(a, c, 1)
        rows = piece_rows(c, chip_r)
        part[a, rows, lo] = part[a, rows, lo] + ring1[0, pl.ds((a * N_CHUNKS + c) * piece, piece)]
        send(a, c, 5)

    def f2l(a, c):
        recv(a, c, 2)
        rows = piece_rows(c, chip_l)
        part[a, rows, hi] = part[a, rows, hi] + ring1[1, pl.ds((a * N_CHUNKS + c) * piece, piece)]
        send(a, c, 6)

    def f3(a, c):
        recv(a, c, 3, 4, 5, 6)
        rows = piece_rows(c, chip)
        slot = pl.ds((a * N_CHUNKS + c) * piece, piece)
        total = part[a, rows] + ring2[0, slot] + ring2[1, slot]
        if a == 0:
            arrived(('y2o', c))
            out = y2_own[own_rows(c)] - total
        elif a == 1:
            arrived(('dy1o', c))
            out = dy1_own[own_rows(c)] + rms_back(y1[rows], total)
        elif a == 2:
            out = y1[rows] - total
        else:
            out = dy2[rows] + rms_back(full[0, rows], total)
        full[a, rows] = out
        send(a, c, 7, 8)

    def f4r(a, c):
        recv(a, c, 7)
        send(a, c, 9)

    def f4l(a, c):
        recv(a, c, 8)
        send(a, c, 10)

    def f5(a, c):
        recv(a, c, 9, 10)
        send(a, c, 11)

    def f6(a, c):
        recv(a, c, 11)
        rows = pl.ds(c * chunk, chunk)
        store(full.at[a, rows], (x2_hbm, dx1_hbm, x1_hbm, dx2_hbm)[a].at[rows])

    def g1(c):
        rows = pl.ds(c * chunk, chunk)
        arrived(('y1', c))
        y_val = y1[rows]
        ng[rows] = (y_val * inv_rms(y_val)).astype(BF16)
        store(ng.at[rows], ng_hbm.at[rows])

        def gelu_block(j):
            cols = pl.ds(pl.multiple_of(j * 256, 256), 256)
            pre = mm(ng[rows], w1[:, cols])
            inner = GELU_C * (pre + GELU_A * (pre * pre * pre))
            th = jnp.tanh(inner)
            act[rows, cols] = (0.5 * pre * (1.0 + th)).astype(BF16)
            dact[rows, cols] = 0.5 * (1.0 + th) + (0.5 * pre) * (1.0 - th * th) * (
                GELU_C * (1.0 + (3.0 * GELU_A) * (pre * pre)))

        if c == 0:
            for j in range(n_blk):
                arrived(('w1', j))
                gelu_block(j)
        else:
            pl.loop(0, n_blk)(gelu_block)
        store(act.at[rows], act_hbm.at[rows])

    def g2(c):
        rows = pl.ds(c * chunk, chunk)
        arrived(('w2',))

        @pl.loop(0, width // 512)
        def _(j):
            cols = pl.ds(pl.multiple_of(j * 512, 512), 512)
            part[0, rows, cols] = mm(act[rows], w2[:, cols])

    def g3(c):
        rows = pl.ds(c * chunk, chunk)
        arrived(('dy2',))

        @pl.loop(0, n_blk)
        def _(j):
            cols = pl.ds(pl.multiple_of(j * 256, 256), 256)
            d_act = mm_nt(dy2[rows].astype(BF16), w2[cols])
            dpre[rows, cols] = (dact[rows, cols] * d_act).astype(BF16)

        store(dpre.at[rows], dpre_hbm.at[rows])

    def g4(c):
        rows = pl.ds(c * chunk, chunk)

        @pl.loop(0, width // 256)
        def _(j):
            cols = pl.ds(pl.multiple_of(j * 256, 256), 256)
            part[1, rows, cols] = mm_nt(dpre[rows], w1[cols])

    def atf(c):
        rows = pl.ds(c * chunk, chunk)
        arrived(*(('wqkv', i) for i in range(3)))
        x_val = full[0, rows]
        nf[rows] = (x_val * inv_rms(x_val)).astype(BF16)
        store(nf.at[rows], nf_hbm.at[rows])
        qkv[rows] = mm(nf[rows], wqkv[...]).astype(BF16)
        key = qkv[rows, pl.ds(qdim, head_dim)]
        val = qkv[rows, pl.ds(qdim + head_dim, head_dim)]
        n_seqs = chunk // seq_len
        row_pos = lax.broadcasted_iota(jnp.int32, (chunk, chunk), 0)
        col_pos = lax.broadcasted_iota(jnp.int32, (chunk, chunk), 1)
        visible = jnp.zeros((chunk, chunk), jnp.bool_)
        for s in range(n_seqs):
            base = s * seq_len
            stop = base + lens_ref[c * n_seqs + s]
            visible = visible | ((row_pos >= base) & (row_pos < base + seq_len)
                                 & (col_pos >= base) & (col_pos < stop) & (col_pos <= row_pos))
        for h in range(n_heads):
            cols = pl.ds(h * head_dim, head_dim)
            scores = mm_nt(qkv[rows, cols], key) * (head_dim ** -0.5)
            scores = jnp.where(visible, scores, MASK_VALUE)
            exps = jnp.exp(scores - jnp.max(scores, axis=-1, keepdims=True))
            probs = exps / jnp.sum(exps, axis=-1, keepdims=True)
            prob[h, rows] = probs
            attn[rows, cols] = mm(probs.astype(BF16), val).astype(BF16)
        store(attn.at[rows], attn_hbm.at[rows])

    def ato(c):
        rows = pl.ds(c * chunk, chunk)
        arrived(('wo',))

        @pl.loop(0, width // 512)
        def _(j):
            cols = pl.ds(pl.multiple_of(j * 512, 512), 512)
            part[2, rows, cols] = mm(attn[rows], wo[:, cols])

    def atb(c):
        rows = pl.ds(c * chunk, chunk)
        d_attn = mm_nt(full[1, rows].astype(BF16), wo[...]).astype(BF16)
        key = qkv[rows, pl.ds(qdim, head_dim)]
        val = qkv[rows, pl.ds(qdim + head_dim, head_dim)]
        d_key = jnp.zeros((chunk, head_dim), F32)
        d_val = jnp.zeros((chunk, head_dim), F32)
        for h in range(n_heads):
            cols = pl.ds(h * head_dim, head_dim)
            d_head = d_attn[:, h * head_dim:(h + 1) * head_dim]
            probs = prob[h, rows]
            d_probs = mm_nt(d_head, val)
            d_scores = probs * (d_probs - jnp.sum(probs * d_probs, axis=-1, keepdims=True)) * (head_dim ** -0.5)
            d_scores = d_scores.astype(BF16)
            dqkv[rows, cols] = mm(d_scores, key).astype(BF16)
            d_key = d_key + mm_tn(d_scores, qkv[rows, cols])
            d_val = d_val + mm_tn(probs.astype(BF16), d_head)
        dqkv[rows, pl.ds(qdim, head_dim)] = d_key.astype(BF16)
        dqkv[rows, pl.ds(qdim + head_dim, head_dim)] = d_val.astype(BF16)
        store(dqkv.at[rows], dqkv_hbm.at[rows])

    def atg(c):
        rows = pl.ds(c * chunk, chunk)

        @pl.loop(0, width // 256)
        def _(j):
            cols = pl.ds(pl.multiple_of(j * 256, 256), 256)
            part[3, rows, cols] = mm_nt(dqkv[rows], wqkv[cols])

    steps = {'F0': f0, 'F1': f1, 'F2R': f2r, 'F2L': f2l, 'F3': f3, 'F4R': f4r, 'F4L': f4l, 'F5': f5, 'F6': f6,
             'G1': g1, 'G2': g2, 'G3': g3, 'G4': g4, 'ATF': atf, 'ATO': ato, 'ATB': atb, 'ATG': atg}
    load_all()
    for name, *where in plan_order():
        steps[name](*where)
    for copy in outs:
        copy.wait()
    for a in range(N_SUMS):
        for c in range(N_CHUNKS):
            for i in range(N_MSGS):
                msg(a, c, i).wait_send()


def block_call(n_tp, seq_lens, y_one, y_two, dy_one, dy_two, w_query, w_key, w_value, w_out, w_up, w_down):
    n_batch, seq_len, width = y_one.shape
    tokens = n_batch * seq_len
    n_heads, head_dim = w_query.shape[1], w_query.shape[2]
    ff = w_up.shape[1]
    qdim = n_heads * head_dim
    qkv_dim = qdim + 2 * head_dim
    chunk = tokens // N_CHUNKS
    units = N_SUMS * N_CHUNKS
    half = chunk // 2
    piece = half // (n_tp // 2)
    acts = tuple(v.reshape(tokens, width) for v in (y_one, y_two, dy_one, dy_two))
    weights = (w_query.reshape(width, qdim), w_key.reshape(width, head_dim), w_value.reshape(width, head_dim),
               w_out.reshape(qdim, width), w_up, w_down)
    sds = jax.ShapeDtypeStruct
    out_shape = [sds((tokens, width), F32)] * 4 + [
        sds((tokens, width), BF16), sds((tokens, width), BF16), sds((tokens, ff), BF16), sds((tokens, ff), BF16),
        sds((tokens, qdim), BF16), sds((tokens, qkv_dim), BF16)]
    vm = pltpu.VMEM
    scratch = [
        vm((width, ff), BF16), vm((ff, width), BF16), vm((width, qkv_dim), BF16), vm((qdim, width), BF16),
        vm((tokens, width), F32), vm((tokens, width), F32),
        vm((N_CHUNKS * piece, width), F32), vm((N_CHUNKS * piece, width), F32),
        vm((tokens, width), BF16), vm((tokens, width), BF16),
        vm((tokens, ff), BF16), vm((tokens, ff), F32), vm((tokens, ff), BF16),
        vm((tokens, qkv_dim), BF16), vm((n_heads, tokens, chunk), F32), vm((tokens, qdim), BF16),
        vm((tokens, qkv_dim), BF16),
        vm((N_SUMS, tokens, width), F32), vm((units * half, width), F32),
        vm((2, units * piece, width // 2), F32), vm((2, units * piece, width), F32),
        vm((N_SUMS, tokens, width), F32),
        pltpu.SemaphoreType.DMA((32,)), pltpu.SemaphoreType.DMA((48,)),
        pltpu.SemaphoreType.DMA((N_MSGS, units)), pltpu.SemaphoreType.DMA((N_MSGS, units)),
    ]
    return pl.pallas_call(
        functools.partial(block_kernel, n_tp, head_dim, seq_len),
        out_shape=out_shape,
        in_specs=[pl.BlockSpec(memory_space=pltpu.SMEM)] + [ANY] * 10,
        out_specs=[ANY] * len(out_shape),
        scratch_shapes=scratch,
        name='block_back',
        compiler_params=pltpu.CompilerParams(collective_id=0, has_side_effects=True,
                                             vmem_limit_bytes=60 * 1024 * 1024),
        cost_estimate=pl.CostEstimate(flops=10 ** 10, bytes_accessed=3 * 10 ** 7, transcendentals=10 ** 6),
    )(seq_lens, *acts, *weights)


def weight_grads(dy_two, dx1, ng, nf, act, dpre, attn, dqkv, n_heads, head_dim):
    qdim = n_heads * head_dim
    e_val, c_val = dy_two.astype(BF16), dx1.astype(BF16)
    dw_down = mm_tn(act, e_val)
    dw_up = mm_tn(ng, dpre)
    dw_out = mm_tn(attn, c_val)
    dw_query = mm_tn(nf, dqkv[:, :qdim])
    dw_key = mm_tn(nf, dqkv[:, qdim:qdim + head_dim])
    dw_value = mm_tn(nf, dqkv[:, qdim + head_dim:])
    return dw_query, dw_key, dw_value, dw_out, dw_up, dw_down


def solution(mesh):
    n_tp = mesh.shape['tp']
    act_spec = P('dp', None, None)
    w_specs = (P(None, None, 'tp', None), P(None, None, 'tp', None), P(None, None, 'tp', None),
               P(None, 'tp', None, None), P(None, None, 'tp'), P(None, 'tp', None))
    g_specs = (P('dp', None, 'tp', None), P('dp', None, 'tp', None), P('dp', None, 'tp', None),
               P('dp', 'tp', None, None), P('dp', None, 'tp'), P('dp', 'tp', None))

    def local_fn(y_one, y_two, dy_one, dy_two, seq_lens, w_query, w_key, w_value, w_out, w_up, w_down):
        n_heads, head_dim = w_query.shape[2], w_query.shape[3]
        tokens, width = y_one.shape[0] * y_one.shape[1], y_one.shape[2]
        ws = tuple(w[0] for w in (w_query, w_key, w_value, w_out, w_up, w_down))
        x1, x2, dx1, dx2, ng, nf, act, dpre, attn, dqkv = block_call(
            n_tp, seq_lens, y_one, y_two, dy_one, dy_two, *ws)
        dw = weight_grads(dy_two.reshape(tokens, width), dx1, ng, nf, act, dpre, attn, dqkv, n_heads, head_dim)
        dw = tuple(g.reshape((1,) + w.shape) for g, w in zip(dw, ws))
        return tuple(v.reshape(y_one.shape) for v in (x1, x2, dx1, dx2)) + dw

    return jax.shard_map(local_fn, mesh=mesh,
                         in_specs=(act_spec,) * 4 + (P('dp'),) + w_specs,
                         out_specs=(act_spec,) * 4 + g_specs,
                         check_vma=False)
```

```python
import functools
import jax
import jax.numpy as jnp
from jax import lax
from jax.experimental import pallas as pl
from jax.experimental.pallas import tpu as pltpu
from jax.sharding import PartitionSpec as P

F32 = jnp.float32
BF16 = jnp.bfloat16
EPS = 1e-5
MASK_VALUE = -1e30
GELU_C = 0.7978845608028654
GELU_A = 0.044715
MESH = pl.DeviceIdType.MESH
ANY = pl.BlockSpec(memory_space=pl.ANY)

N_CHUNKS = 4
N_GROUPS = 2
N_PARTS = 2
N_SUMS = 4
N_MSGS = 12

LOAD_US = 3.5
STEP_US = {'G1': 1.0, 'G2': 0.9, 'G3': 0.9, 'G4': 0.6, 'PREP': 1.0, 'ATF': 1.6, 'ATO': 0.6, 'ATB': 2.0, 'ATG': 1.2}
SUM_US = {'F0': 0.03, 'F1': 0.2, 'F2R': 0.05, 'F2L': 0.05, 'F3': 0.25, 'F4R': 0.03, 'F4L': 0.03, 'F5': 0.03, 'F6': 0.03}
SENDS = {'F0': (0,), 'F1': (1, 2, 3, 4), 'F2R': (5,), 'F2L': (6,), 'F3': (7, 8), 'F4R': (9,), 'F4L': (10,), 'F5': (11,)}
RECVS = {'F1': (0,), 'F2R': (1,), 'F2L': (2,), 'F3': (3, 4, 5, 6), 'F4R': (7,), 'F4L': (8,), 'F5': (9, 10), 'F6': (11,)}
AFTER = {'F1': ('F0',), 'F2R': ('F1',), 'F2L': ('F1',), 'F3': ('F2R', 'F2L'), 'F4R': ('F3',), 'F4L': ('F3',),
         'F5': ('F4R', 'F4L'), 'F6': ('F5',)}
MSG_US = ((1.5, 1.0),) + ((2.8, 1.9),) * 6 + ((5.6, 1.9),) * 2 + ((2.8, 1.9),) * 2 + ((1.5, 1.0),)
RANK = ('G1', 'G2', 'ATF', 'ATO', 'ATB', 'ATG', 'G3', 'G4', 'PREP')


def plan_order():
    per = N_CHUNKS // N_GROUPS
    todo = {}

    def add(key, needs, sends=()):
        todo[key] = (needs, STEP_US[key[0]] if key[0] in STEP_US else SUM_US[key[0]], sends)

    for g in range(N_GROUPS):
        chunks = range(g * per, (g + 1) * per)
        add(('G1', g), [])
        add(('G2', g), [('G1', g)])
        add(('ATF', g), [('F6', 0, c) for c in chunks] + [('PREP',)])
        add(('ATO', g), [('ATF', g)])
        add(('ATB', g), [('F6', 1, c) for c in chunks] + [('ATF', g)])
        add(('ATG', g), [('ATB', g)])
    for j in range(N_PARTS):
        add(('G3', j), [('G1', g) for g in range(N_GROUPS)])
        add(('G4', j), [('G3', k) for k in range(N_PARTS)])
    add(('PREP',), [('G4', j) for j in range(N_PARTS)])
    for c in range(N_CHUNKS):
        g = c // per
        source = ([('G2', g)], [('G4', j) for j in range(N_PARTS)], [('ATO', g)], [('ATG', g)])
        for a in range(N_SUMS):
            for name in SUM_US:
                needs = [(p, a, c) for p in AFTER.get(name, ())] + [(i, a, c) for i in RECVS.get(name, ())]
                add((name, a, c), needs + source[a] if name == 'F0' else needs, SENDS.get(name, ()))

    def rank(key):
        if key[0] in STEP_US:
            pos = RANK.index(key[0])
            return (-1, key[1], pos) if pos < 2 else (1, pos) + key[1:]
        return (0,) + key[1:] + (key[0],)

    now, order, done, free = LOAD_US, [], {}, {}
    while todo:
        ready = {k: max([done[n] for n in v[0]], default=0.0) for k, v in todo.items() if all(n in done for n in v[0])}
        now = max(now, min(ready.values()))
        key = min((k for k, at in ready.items() if at <= now), key=rank)
        _, cost, sends = todo.pop(key)
        now += cost
        done[key] = now
        order.append(key)
        for i in sends:
            link = 0 if i in (0, 11) else 1 + i % 2
            wire, delay = MSG_US[i]
            start = max(now, free.get(link, 0.0))
            free[link] = start + wire / N_CHUNKS
            done[(i,) + key[1:]] = free[link] + delay
    return order


def mm(lhs, rhs):
    return jnp.dot(lhs, rhs, preferred_element_type=F32)


def mm_nt(lhs, rhs):
    return lax.dot_general(lhs, rhs, (((1,), (1,)), ((), ())), preferred_element_type=F32)


def mm_tn(lhs, rhs):
    return lax.dot_general(lhs, rhs, (((0,), (0,)), ((), ())), preferred_element_type=F32)


def inv_rms(x_val):
    return lax.rsqrt(jnp.mean(x_val * x_val, axis=-1, keepdims=True) + EPS)


def rms_back(x_val, grad_norm):
    inv = inv_rms(x_val)
    normed = x_val * inv
    return inv * (grad_norm - normed * jnp.mean(grad_norm * normed, axis=-1, keepdims=True))


def block_kernel(n_tp, head_dim, seq_len,
                 lens_ref, y1_hbm, y2_hbm, dy1_hbm, dy2_hbm, wq_hbm, wk_hbm, wv_hbm, wo_hbm, w1_hbm, w2_hbm,
                 x1_hbm, x2_hbm, dx1_hbm, dx2_hbm, ng_hbm, nf_hbm, act_hbm, dpre_hbm, attn_hbm, dqkv_hbm,
                 w1, w2, wqkv, wo, wq_raw, wq_f, y1, dy2, dyb, y2_own, dy1_own, ng, nf, act, dact, dpre, qkv, prob, attn, dqkv,
                 part, d2d, ring1, ring2, full,
                 load_sem, out_sem, send_sem, recv_sem):
    tokens, width = y1.shape
    ff = w1.shape[1]
    qdim = attn.shape[1]
    n_heads = qdim // head_dim
    chunk = tokens // N_CHUNKS
    half = chunk // 2
    piece = half // (n_tp // 2)
    hw = width // 2
    n_chips = n_tp // 2

    me = lax.axis_index('tp')
    core = lax.rem(me, 2)
    chip = lax.div(me, 2)
    partner = me + 1 - 2 * core
    right = lax.rem(me + 2, n_tp)
    left = lax.rem(me + n_tp - 2, n_tp)
    chip_r = lax.rem(chip + 1, n_chips)
    chip_l = lax.rem(chip + n_chips - 1, n_chips)
    chip_o = lax.rem(chip + 2, n_chips)

    def half_rows(c, k):
        return pl.ds(pl.multiple_of(c * chunk + k * half, half), half)

    def piece_rows(c, x):
        return pl.ds(pl.multiple_of(c * chunk + core * half + x * piece, piece), piece)

    def own_rows(c):
        return pl.ds(c * piece, piece)

    lo, hi = pl.ds(0, hw), pl.ds(hw, hw)

    barrier = pltpu.get_barrier_semaphore()
    for dev in (partner, left, right):
        pl.semaphore_signal(barrier, inc=1, device_id={'tp': dev}, device_id_type=MESH)

    loads = {}

    def arrived(*names):
        for name in names:
            if name in loads:
                loads.pop(name).wait()

    n_blk = ff // 256

    def load_all():
        groups = [pl.ds(g * (tokens // N_GROUPS), tokens // N_GROUPS) for g in range(N_GROUPS)]
        blocks = [pl.ds(j * 256, 256) for j in range(n_blk)]
        todo = [(('y1', 0), y1_hbm.at[groups[0]], y1.at[groups[0]])]
        todo += [(('w1', j), w1_hbm.at[:, blk], w1.at[:, blk]) for j, blk in enumerate(blocks)]
        todo += [(('y1', g), y1_hbm.at[groups[g]], y1.at[groups[g]]) for g in range(1, N_GROUPS)]
        todo += [(('w2',), w2_hbm, w2), (('dy2',), dy2_hbm, dy2)]
        for c in range(N_CHUNKS):
            todo += [(('y2o', c), y2_hbm.at[piece_rows(c, chip)], y2_own.at[own_rows(c)]),
                     (('dy1o', c), dy1_hbm.at[piece_rows(c, chip)], dy1_own.at[own_rows(c)])]
        todo += [(('wq',), wq_hbm, wq_raw),
                 (('wk',), wk_hbm, wqkv.at[:, pl.ds(qdim, head_dim)]),
                 (('wv',), wv_hbm, wqkv.at[:, pl.ds(qdim + head_dim, head_dim)]),
                 (('wo',), wo_hbm, wo)]
        for i, (name, src, dst) in enumerate(todo):
            loads[name] = pltpu.make_async_copy(src, dst, load_sem.at[i])
            loads[name].start()

    outs = []

    def store(src, dst):
        copy = pltpu.make_async_copy(src, dst, out_sem.at[len(outs)])
        copy.start()
        outs.append(copy)

    def msg(a, c, i):
        rows_own, rows_r, rows_l, rows_o = (piece_rows(c, x) for x in (chip, chip_r, chip_l, chip_o))
        u = a * N_CHUNKS + c
        slot = pl.ds(u * piece, piece)
        pa, oa = part.at[a], full.at[a]
        if i == 0:
            src, dst, dev = pa.at[half_rows(c, 1 - core)], d2d.at[pl.ds(u * half, half)], partner
        elif i == 1:
            src, dst, dev = pa.at[rows_o, lo], ring1.at[0, slot], right
        elif i == 2:
            src, dst, dev = pa.at[rows_o, hi], ring1.at[1, slot], left
        elif i == 3:
            src, dst, dev = pa.at[rows_r, hi], ring2.at[0, slot, hi], right
        elif i == 4:
            src, dst, dev = pa.at[rows_l, lo], ring2.at[1, slot, lo], left
        elif i == 5:
            src, dst, dev = pa.at[rows_r, lo], ring2.at[0, slot, lo], right
        elif i == 6:
            src, dst, dev = pa.at[rows_l, hi], ring2.at[1, slot, hi], left
        elif i == 7:
            src, dst, dev = oa.at[rows_own], oa.at[rows_own], right
        elif i == 8:
            src, dst, dev = oa.at[rows_own], oa.at[rows_own], left
        elif i == 9:
            src, dst, dev = oa.at[rows_l, lo], oa.at[rows_l, lo], right
        elif i == 10:
            src, dst, dev = oa.at[rows_r, hi], oa.at[rows_r, hi], left
        else:
            src, dst, dev = oa.at[half_rows(c, core)], oa.at[half_rows(c, core)], partner
        return pltpu.make_async_remote_copy(src, dst, send_sem.at[i, u], recv_sem.at[i, u],
                                            device_id={'tp': dev}, device_id_type=MESH)

    def send(a, c, *ids):
        for i in ids:
            msg(a, c, i).start()

    def recv(a, c, *ids):
        for i in ids:
            msg(a, c, i).wait_recv()

    state = {'met': False}

    def f0(a, c):
        if not state['met']:
            pl.semaphore_wait(barrier, 3)
            state['met'] = True
        send(a, c, 0)

    def f1(a, c):
        recv(a, c, 0)
        rows = half_rows(c, core)
        part[a, rows] = part[a, rows] + d2d[pl.ds((a * N_CHUNKS + c) * half, half)]
        send(a, c, 1, 2, 3, 4)

    def f2r(a, c):
        recv(a, c, 1)
        rows = piece_rows(c, chip_r)
        part[a, rows, lo] = part[a, rows, lo] + ring1[0, pl.ds((a * N_CHUNKS + c) * piece, piece)]
        send(a, c, 5)

    def f2l(a, c):
        recv(a, c, 2)
        rows = piece_rows(c, chip_l)
        part[a, rows, hi] = part[a, rows, hi] + ring1[1, pl.ds((a * N_CHUNKS + c) * piece, piece)]
        send(a, c, 6)

    def f3(a, c):
        recv(a, c, 3, 4, 5, 6)
        rows = piece_rows(c, chip)
        slot = pl.ds((a * N_CHUNKS + c) * piece, piece)
        total = part[a, rows] + ring2[0, slot] + ring2[1, slot]
        if a == 0:
            arrived(('y2o', c))
            out = y2_own[own_rows(c)] - total
        elif a == 1:
            arrived(('dy1o', c))
            out = dy1_own[own_rows(c)] + rms_back(y1[rows], total)
        elif a == 2:
            out = y1[rows] - total
        else:
            out = dy2[rows] + rms_back(full[0, rows], total)
        full[a, rows] = out
        send(a, c, 7, 8)

    def f4r(a, c):
        recv(a, c, 7)
        send(a, c, 9)

    def f4l(a, c):
        recv(a, c, 8)
        send(a, c, 10)

    def f5(a, c):
        recv(a, c, 9, 10)
        send(a, c, 11)

    def f6(a, c):
        recv(a, c, 11)
        rows = pl.ds(c * chunk, chunk)
        store(full.at[a, rows], (x2_hbm, dx1_hbm, x1_hbm, dx2_hbm)[a].at[rows])

    group = tokens // N_GROUPS

    def group_rows(g):
        return pl.ds(g * group, group)

    def g1(g):
        rows = group_rows(g)
        arrived(('y1', g))
        y_val = y1[rows]
        ng[rows] = (y_val * inv_rms(y_val)).astype(BF16)
        store(ng.at[rows], ng_hbm.at[rows])
        for j in range(n_blk):
            cols = pl.ds(j * 256, 256)
            arrived(('w1', j))
            pre = mm(ng[rows], w1[:, cols])
            th = jnp.tanh(GELU_C * (pre + GELU_A * (pre * pre * pre)))
            act[rows, cols] = (0.5 * pre * (1.0 + th)).astype(BF16)
            dact[rows, cols] = 0.5 * (1.0 + th) + (0.5 * pre) * (1.0 - th * th) * (
                GELU_C * (1.0 + (3.0 * GELU_A) * (pre * pre)))
        store(act.at[rows], act_hbm.at[rows])

    def g2(g):
        rows = group_rows(g)
        arrived(('w2',))
        part[0, rows] = mm(act[rows], w2[...])

    def g3(j):
        arrived(('dy2',))
        cols = pl.ds(j * (ff // N_PARTS), ff // N_PARTS)
        if j == 0:
            dyb[...] = dy2[...].astype(BF16)
        dpre[:, cols] = (dact[:, cols] * mm_nt(dyb[...], w2[cols])).astype(BF16)
        store(dpre.at[:, cols], dpre_hbm.at[:, cols])

    def g4(j):
        cols = pl.ds(j * (width // N_PARTS), width // N_PARTS)
        part[1, :, cols] = mm_nt(dpre[...], w1[cols])

    def prep():
        arrived(('wq',))
        wq_f[...] = wq_raw[...].astype(F32)
        for h in range(n_heads):
            wqkv[:, pl.ds(h * head_dim, head_dim)] = wq_f[pl.ds(h, width, stride=n_heads)].astype(BF16)

    def atf(g):
        rows = group_rows(g)
        arrived(('wk',), ('wv',))
        x_val = full[0, rows]
        nf[rows] = (x_val * inv_rms(x_val)).astype(BF16)
        store(nf.at[rows], nf_hbm.at[rows])
        qkv[rows] = mm(nf[rows], wqkv[...]).astype(BF16)
        key = qkv[rows, pl.ds(qdim, head_dim)]
        val = qkv[rows, pl.ds(qdim + head_dim, head_dim)]
        n_seqs = group // seq_len
        row_pos = lax.broadcasted_iota(jnp.int32, (group, group), 0)
        col_pos = lax.broadcasted_iota(jnp.int32, (group, group), 1)
        visible = jnp.zeros((group, group), jnp.bool_)
        for s in range(n_seqs):
            base = s * seq_len
            stop = base + lens_ref[g * n_seqs + s]
            visible = visible | ((row_pos >= base) & (row_pos < base + seq_len)
                                 & (col_pos >= base) & (col_pos < stop) & (col_pos <= row_pos))
        for h in range(n_heads):
            cols = pl.ds(h * head_dim, head_dim)
            scores = mm_nt(qkv[rows, cols], key) * (head_dim ** -0.5)
            scores = jnp.where(visible, scores, MASK_VALUE)
            exps = jnp.exp(scores - jnp.max(scores, axis=-1, keepdims=True))
            probs = exps / jnp.sum(exps, axis=-1, keepdims=True)
            prob[h, rows] = probs
            attn[rows, cols] = mm(probs.astype(BF16), val).astype(BF16)
        store(attn.at[rows], attn_hbm.at[rows])

    def ato(g):
        rows = group_rows(g)
        arrived(('wo',))
        part[2, rows] = mm(attn[rows], wo[...])

    def atb(g):
        rows = group_rows(g)
        d_attn = mm_nt(full[1, rows].astype(BF16), wo[...]).astype(BF16)
        key = qkv[rows, pl.ds(qdim, head_dim)]
        val = qkv[rows, pl.ds(qdim + head_dim, head_dim)]
        d_key = jnp.zeros((group, head_dim), F32)
        d_val = jnp.zeros((group, head_dim), F32)
        for h in range(n_heads):
            cols = pl.ds(h * head_dim, head_dim)
            d_head = d_attn[:, h * head_dim:(h + 1) * head_dim]
            probs = prob[h, rows]
            d_probs = mm_nt(d_head, val)
            d_scores = probs * (d_probs - jnp.sum(probs * d_probs, axis=-1, keepdims=True)) * (head_dim ** -0.5)
            d_scores = d_scores.astype(BF16)
            dqkv[rows, cols] = mm(d_scores, key).astype(BF16)
            d_key = d_key + mm_tn(d_scores, qkv[rows, cols])
            d_val = d_val + mm_tn(probs.astype(BF16), d_head)
        dqkv[rows, pl.ds(qdim, head_dim)] = d_key.astype(BF16)
        dqkv[rows, pl.ds(qdim + head_dim, head_dim)] = d_val.astype(BF16)
        store(dqkv.at[rows], dqkv_hbm.at[rows])

    def atg(g):
        rows = group_rows(g)
        part[3, rows] = mm_nt(dqkv[rows], wqkv[...])

    steps = {'F0': f0, 'F1': f1, 'F2R': f2r, 'F2L': f2l, 'F3': f3, 'F4R': f4r, 'F4L': f4l, 'F5': f5, 'F6': f6,
             'G1': g1, 'G2': g2, 'G3': g3, 'G4': g4, 'PREP': prep, 'ATF': atf, 'ATO': ato, 'ATB': atb, 'ATG': atg}
    load_all()
    for name, *where in plan_order():
        steps[name](*where)
    for copy in outs:
        copy.wait()
    for a in range(N_SUMS):
        for c in range(N_CHUNKS):
            for i in range(N_MSGS):
                msg(a, c, i).wait_send()


def block_call(n_tp, seq_lens, y_one, y_two, dy_one, dy_two, w_query, w_key, w_value, w_out, w_up, w_down):
    n_batch, seq_len, width = y_one.shape
    tokens = n_batch * seq_len
    n_heads, head_dim = w_query.shape[1], w_query.shape[2]
    ff = w_up.shape[1]
    qdim = n_heads * head_dim
    qkv_dim = qdim + 2 * head_dim
    units = N_SUMS * N_CHUNKS
    half = tokens // N_CHUNKS // 2
    piece = half // (n_tp // 2)
    acts = tuple(v.reshape(tokens, width) for v in (y_one, y_two, dy_one, dy_two))
    weights = (w_query.reshape(width * n_heads, head_dim), w_key.reshape(width, head_dim), w_value.reshape(width, head_dim),
               w_out.reshape(qdim, width), w_up, w_down)
    sds = jax.ShapeDtypeStruct
    out_shape = [sds((tokens, width), F32)] * 4 + [
        sds((tokens, width), BF16), sds((tokens, width), BF16), sds((tokens, ff), BF16), sds((tokens, ff), BF16),
        sds((tokens, qdim), BF16), sds((tokens, qkv_dim), BF16)]
    vm = pltpu.VMEM
    scratch = [
        vm((width, ff), BF16), vm((ff, width), BF16), vm((width, qkv_dim), BF16), vm((qdim, width), BF16),
        vm((width * n_heads, head_dim), BF16), vm((width * n_heads, head_dim), F32),
        vm((tokens, width), F32), vm((tokens, width), F32), vm((tokens, width), BF16),
        vm((N_CHUNKS * piece, width), F32), vm((N_CHUNKS * piece, width), F32),
        vm((tokens, width), BF16), vm((tokens, width), BF16),
        vm((tokens, ff), BF16), vm((tokens, ff), F32), vm((tokens, ff), BF16),
        vm((tokens, qkv_dim), BF16), vm((n_heads, tokens, tokens // N_GROUPS), F32), vm((tokens, qdim), BF16),
        vm((tokens, qkv_dim), BF16),
        vm((N_SUMS, tokens, width), F32), vm((units * half, width), F32),
        vm((2, units * piece, width // 2), F32), vm((2, units * piece, width), F32),
        vm((N_SUMS, tokens, width), F32),
        pltpu.SemaphoreType.DMA((32,)), pltpu.SemaphoreType.DMA((48,)),
        pltpu.SemaphoreType.DMA((N_MSGS, units)), pltpu.SemaphoreType.DMA((N_MSGS, units)),
    ]
    return pl.pallas_call(
        functools.partial(block_kernel, n_tp, head_dim, seq_len),
        out_shape=out_shape,
        in_specs=[pl.BlockSpec(memory_space=pltpu.SMEM)] + [ANY] * 10,
        out_specs=[ANY] * len(out_shape),
        scratch_shapes=scratch,
        name='block_back',
        compiler_params=pltpu.CompilerParams(collective_id=0, has_side_effects=True,
                                             vmem_limit_bytes=60 * 1024 * 1024),
        cost_estimate=pl.CostEstimate(flops=10 ** 10, bytes_accessed=3 * 10 ** 7, transcendentals=10 ** 6),
    )(seq_lens, *acts, *weights)


def grads_kernel(head_dim, n_blk,
                 x1_in, x2_in, dx1_in, dx2_in, dy2_in, ng_in, nf_in, act_in, dpre_in, attn_in, dqkv_in,
                 x1_out, x2_out, dx1_out, dx2_out, dwq_out, dwk_out, dwv_out, dwo_out, dw1_out, dw2_out,
                 state, dy2, ng, nf, act, dpre, attn, dqkv, e_val, c_val, dwq, dwk, dwv, dwo, dw1, dw2,
                 in_sem, out_sem):
    ins = {}
    todo = [('act', act_in, act), ('dy2', dy2_in, dy2), ('ng', ng_in, ng), ('dpre', dpre_in, dpre),
            ('dx1', dx1_in, state.at[2]), ('attn', attn_in, attn), ('nf', nf_in, nf), ('dqkv', dqkv_in, dqkv),
            ('x1', x1_in, state.at[0]), ('x2', x2_in, state.at[1]), ('dx2', dx2_in, state.at[3])]
    for i, (name, src, dst) in enumerate(todo):
        ins[name] = pltpu.make_async_copy(src, dst, in_sem.at[i])
        ins[name].start()

    def arrived(*names):
        for name in names:
            if name in ins:
                ins.pop(name).wait()

    outs = []

    def store(src, dst):
        outs.append(pltpu.make_async_copy(src, dst, out_sem.at[len(outs)]))
        outs[-1].start()

    width, ff = dw1.shape
    qdim = attn.shape[1]
    n_heads = qdim // head_dim
    arrived('act', 'dy2')
    e_val[...] = dy2[...].astype(BF16)
    rows2, rows1 = ff // n_blk, width // n_blk
    for j in range(n_blk):
        rows = pl.ds(j * rows2, rows2)
        dw2[rows] = mm_tn(act[:, rows], e_val[...])
        store(dw2.at[rows], dw2_out.at[rows])
    arrived('ng', 'dpre')
    for j in range(n_blk):
        rows = pl.ds(j * rows1, rows1)
        dw1[rows] = mm_tn(ng[:, rows], dpre[...])
        store(dw1.at[rows], dw1_out.at[rows])
    arrived('dx1', 'attn')
    c_val[...] = state[2].astype(BF16)
    store(state.at[2], dx1_out)
    for h in range(n_heads):
        rows = pl.ds(h * head_dim, head_dim)
        dwo[rows] = mm_tn(attn[:, rows], c_val[...])
        store(dwo.at[rows], dwo_out.at[rows])
    for name, i, out in (('x1', 0, x1_out), ('x2', 1, x2_out), ('dx2', 3, dx2_out)):
        arrived(name)
        store(state.at[i], out)
    arrived('nf', 'dqkv')
    for j in range(n_blk // 2):
        step = width // (n_blk // 2)
        rows = pl.ds(j * step, step)
        grad = mm_tn(nf[:, rows], dqkv[...])
        for h in range(n_heads):
            dwq[pl.ds(j * step * n_heads + h, step, stride=n_heads)] = grad[:, h * head_dim:(h + 1) * head_dim]
        dwk[rows] = grad[:, qdim:qdim + head_dim]
        dwv[rows] = grad[:, qdim + head_dim:]
        rows_q = pl.ds(j * step * n_heads, step * n_heads)
        store(dwq.at[rows_q], dwq_out.at[rows_q])
        store(dwk.at[rows], dwk_out.at[rows])
        store(dwv.at[rows], dwv_out.at[rows])
    for copy in outs:
        copy.wait()


def grads_call(dy_two, x1, x2, dx1, dx2, ng, nf, act, dpre, attn, dqkv, n_heads, head_dim):
    tokens, width = x1.shape
    ff, qdim, qkv_dim = act.shape[1], attn.shape[1], dqkv.shape[1]
    sds, vm = jax.ShapeDtypeStruct, pltpu.VMEM
    dw_shapes = [(width * n_heads, head_dim), (width, head_dim), (width, head_dim), (qdim, width), (width, ff), (ff, width)]
    scratch = [vm((4, tokens, width), F32), vm((tokens, width), F32), vm((tokens, width), BF16), vm((tokens, width), BF16),
               vm((tokens, ff), BF16), vm((tokens, ff), BF16), vm((tokens, qdim), BF16), vm((tokens, qkv_dim), BF16),
               vm((tokens, width), BF16), vm((tokens, width), BF16)]
    scratch += [vm(s, F32) for s in dw_shapes]
    scratch += [pltpu.SemaphoreType.DMA((16,)), pltpu.SemaphoreType.DMA((48,))]
    return pl.pallas_call(
        functools.partial(grads_kernel, head_dim, 8),
        out_shape=[sds((tokens, width), F32)] * 4 + [sds(s, F32) for s in dw_shapes],
        in_specs=[ANY] * 11,
        out_specs=[ANY] * 10,
        scratch_shapes=scratch,
        name='weight_grads',
        compiler_params=pltpu.CompilerParams(vmem_limit_bytes=60 * 1024 * 1024),
        cost_estimate=pl.CostEstimate(flops=4 * 10 ** 9, bytes_accessed=4 * 10 ** 7, transcendentals=0),
    )(x1, x2, dx1, dx2, dy_two, ng, nf, act, dpre, attn, dqkv)


def solution(mesh):
    n_tp = mesh.shape['tp']
    act_spec = P('dp', None, None)
    w_specs = (P(None, None, 'tp', None), P(None, None, 'tp', None), P(None, None, 'tp', None),
               P(None, 'tp', None, None), P(None, None, 'tp'), P(None, 'tp', None))
    g_specs = (P('dp', None, 'tp', None), P('dp', None, 'tp', None), P('dp', None, 'tp', None),
               P('dp', 'tp', None, None), P('dp', None, 'tp'), P('dp', 'tp', None))

    def local_fn(y_one, y_two, dy_one, dy_two, seq_lens, w_query, w_key, w_value, w_out, w_up, w_down):
        n_heads, head_dim = w_query.shape[2], w_query.shape[3]
        tokens, width = y_one.shape[0] * y_one.shape[1], y_one.shape[2]
        ws = tuple(w[0] for w in (w_query, w_key, w_value, w_out, w_up, w_down))
        saved = block_call(n_tp, seq_lens, y_one, y_two, dy_one, dy_two, *ws)
        res = grads_call(dy_two.reshape(tokens, width), *saved, n_heads, head_dim)
        dw = tuple(g.reshape((1,) + w.shape) for g, w in zip(res[4:], ws))
        return tuple(v.reshape(y_one.shape) for v in res[:4]) + dw

    return jax.shard_map(local_fn, mesh=mesh,
                         in_specs=(act_spec,) * 4 + (P('dp'),) + w_specs,
                         out_specs=(act_spec,) * 4 + g_specs,
                         check_vma=False)
```

```python
import functools
import jax
import jax.numpy as jnp
from jax import lax
from jax.experimental import pallas as pl
from jax.experimental.pallas import tpu as pltpu
from jax.sharding import PartitionSpec as P

F32 = jnp.float32
BF16 = jnp.bfloat16
EPS = 1e-5
MASK_VALUE = -1e30
GELU_C = 0.7978845608028654
GELU_A = 0.044715
MESH = pl.DeviceIdType.MESH
ANY = pl.BlockSpec(memory_space=pl.ANY)

N_CHUNKS = 4
N_GROUPS = 2
N_PARTS = 2
N_SUMS = 4
N_MSGS = 12
RECV_SLOT = (0, 1, 2, 3, 3, 3, 3, 4, 5, 6, 6, 7)

LOAD_US = 3.5
STEP_US = {'G1': 1.0, 'G2': 0.9, 'G3': 0.9, 'G4': 0.6, 'PREP': 1.0, 'ATF': 1.6, 'ATO': 0.6, 'ATB': 2.0, 'ATG': 1.2}
SUM_US = {'F0': 0.03, 'F1': 0.2, 'F2R': 0.05, 'F2L': 0.05, 'F3': 0.25, 'F4R': 0.03, 'F4L': 0.03, 'F5': 0.03, 'F6': 0.03}
SENDS = {'F0': (0,), 'F1': (1, 2, 3, 4), 'F2R': (5,), 'F2L': (6,), 'F3': (7, 8), 'F4R': (9,), 'F4L': (10,), 'F5': (11,)}
RECVS = {'F1': (0,), 'F2R': (1,), 'F2L': (2,), 'F3': (3, 4, 5, 6), 'F4R': (7,), 'F4L': (8,), 'F5': (9, 10), 'F6': (11,)}
AFTER = {'F1': ('F0',), 'F2R': ('F1',), 'F2L': ('F1',), 'F3': ('F2R', 'F2L'), 'F4R': ('F3',), 'F4L': ('F3',),
         'F5': ('F4R', 'F4L'), 'F6': ('F5',)}
MSG_US = ((1.5, 1.0),) + ((2.8, 1.9),) * 6 + ((5.6, 1.9),) * 2 + ((2.8, 1.9),) * 2 + ((1.5, 1.0),)
RANK = ('G1', 'G2', 'ATF', 'ATO', 'ATB', 'ATG', 'G3', 'G4', 'PREP')


def plan_order():
    per = N_CHUNKS // N_GROUPS
    todo = {}

    def add(key, needs, sends=()):
        todo[key] = (needs, STEP_US[key[0]] if key[0] in STEP_US else SUM_US[key[0]], sends)

    for g in range(N_GROUPS):
        chunks = range(g * per, (g + 1) * per)
        add(('G1', g), [])
        add(('G2', g), [('G1', g)])
        add(('ATF', g), [('F6', 0, c) for c in chunks] + [('PREP',)])
        add(('ATO', g), [('ATF', g)])
        add(('ATB', g), [('F6', 1, c) for c in chunks] + [('ATF', g)])
        add(('ATG', g), [('ATB', g)])
    for j in range(N_PARTS):
        add(('G3', j), [('G1', g) for g in range(N_GROUPS)])
        add(('G4', j), [('G3', k) for k in range(N_PARTS)])
    add(('PREP',), [('G4', j) for j in range(N_PARTS)])
    for c in range(N_CHUNKS):
        g = c // per
        source = ([('G2', g)], [('G4', j) for j in range(N_PARTS)], [('ATO', g)], [('ATG', g)])
        for a in range(N_SUMS):
            for name in SUM_US:
                needs = [(p, a, c) for p in AFTER.get(name, ())] + [(i, a, c) for i in RECVS.get(name, ())]
                add((name, a, c), needs + source[a] if name == 'F0' else needs, SENDS.get(name, ()))

    def rank(key):
        if key[0] in STEP_US:
            pos = RANK.index(key[0])
            return (-1, key[1], pos) if pos < 2 else (1, pos) + key[1:]
        return (0,) + key[1:] + (key[0],)

    now, order, done, free = LOAD_US, [], {}, {}
    while todo:
        ready = {k: max([done[n] for n in v[0]], default=0.0) for k, v in todo.items() if all(n in done for n in v[0])}
        now = max(now, min(ready.values()))
        key = min((k for k, at in ready.items() if at <= now), key=rank)
        _, cost, sends = todo.pop(key)
        now += cost
        done[key] = now
        order.append(key)
        for i in sends:
            link = 0 if i in (0, 11) else 1 + i % 2
            wire, delay = MSG_US[i]
            start = max(now, free.get(link, 0.0))
            free[link] = start + wire / N_CHUNKS
            done[(i,) + key[1:]] = free[link] + delay
    return order


def mm(lhs, rhs):
    return jnp.dot(lhs, rhs, preferred_element_type=F32)


def mm_nt(lhs, rhs):
    return lax.dot_general(lhs, rhs, (((1,), (1,)), ((), ())), preferred_element_type=F32)


def mm_tn(lhs, rhs):
    return lax.dot_general(lhs, rhs, (((0,), (0,)), ((), ())), preferred_element_type=F32)


def inv_rms(x_val):
    return lax.rsqrt(jnp.mean(x_val * x_val, axis=-1, keepdims=True) + EPS)


def rms_back(x_val, grad_norm):
    inv = inv_rms(x_val)
    normed = x_val * inv
    return inv * (grad_norm - normed * jnp.mean(grad_norm * normed, axis=-1, keepdims=True))


def block_kernel(n_tp, head_dim, seq_len,
                 lens_ref, y1_hbm, y2_hbm, dy1_hbm, dy2_hbm, wq_hbm, wk_hbm, wv_hbm, wo_hbm, w1_hbm, w2_hbm,
                 x2, dx1, x1, dx2, ng, nf, act, dpre, attn, dqkv, dyb,
                 w1, w2, wqkv, wo, wq_raw, wq_f, y1, dy2, y2_own, dy1_own, dact, qkv, prob,
                 part, d2d, ring1, ring2,
                 load_sem, send_sem, recv_sem):
    full = (x2, dx1, x1, dx2)
    tokens, width = y1.shape
    ff = w1.shape[1]
    qdim = attn.shape[1]
    n_heads = qdim // head_dim
    chunk = tokens // N_CHUNKS
    half = chunk // 2
    piece = half // (n_tp // 2)
    hw = width // 2
    n_chips = n_tp // 2

    me = lax.axis_index('tp')
    core = lax.rem(me, 2)
    chip = lax.div(me, 2)
    partner = me + 1 - 2 * core
    right = lax.rem(me + 2, n_tp)
    left = lax.rem(me + n_tp - 2, n_tp)
    chip_r = lax.rem(chip + 1, n_chips)
    chip_l = lax.rem(chip + n_chips - 1, n_chips)
    chip_o = lax.rem(chip + 2, n_chips)

    def half_rows(c, k):
        return pl.ds(pl.multiple_of(c * chunk + k * half, half), half)

    def piece_rows(c, x):
        return pl.ds(pl.multiple_of(c * chunk + core * half + x * piece, piece), piece)

    def own_rows(c):
        return pl.ds(c * piece, piece)

    lo, hi = pl.ds(0, hw), pl.ds(hw, hw)

    barrier = pltpu.get_barrier_semaphore()
    for dev in (partner, left, right):
        pl.semaphore_signal(barrier, inc=1, device_id={'tp': dev}, device_id_type=MESH)

    loads = {}

    def arrived(*names):
        for name in names:
            if name in loads:
                loads.pop(name).wait()

    n_blk = ff // 256

    def load_all():
        groups = [pl.ds(g * (tokens // N_GROUPS), tokens // N_GROUPS) for g in range(N_GROUPS)]
        blocks = [pl.ds(j * 256, 256) for j in range(n_blk)]
        todo = [(('y1', 0), y1_hbm.at[groups[0]], y1.at[groups[0]])]
        todo += [(('w1', j), w1_hbm.at[:, blk], w1.at[:, blk]) for j, blk in enumerate(blocks)]
        todo += [(('y1', g), y1_hbm.at[groups[g]], y1.at[groups[g]]) for g in range(1, N_GROUPS)]
        todo += [(('w2',), w2_hbm, w2), (('dy2',), dy2_hbm, dy2)]
        todo += [(('wq',), wq_hbm, wq_raw),
                 (('wk',), wk_hbm, wqkv.at[:, pl.ds(qdim, head_dim)]),
                 (('wv',), wv_hbm, wqkv.at[:, pl.ds(qdim + head_dim, head_dim)]),
                 (('wo',), wo_hbm, wo)]
        for i, (name, src, dst) in enumerate(todo):
            loads[name] = pltpu.make_async_copy(src, dst, load_sem.at[i])
            loads[name].start()
            if name == ('dy2',):
                for k, src_hbm, own in ((14, y2_hbm, y2_own), (15, dy1_hbm, dy1_own)):
                    for c in range(N_CHUNKS):
                        pltpu.make_async_copy(src_hbm.at[piece_rows(c, chip)], own.at[own_rows(c)], load_sem.at[k]).start()
                    loads['own', k] = pltpu.make_async_copy(own, own, load_sem.at[k])

    def shared(a, c):
        return a % 2 * N_CHUNKS + c

    def msg(a, c, i):
        rows_own, rows_r, rows_l, rows_o = (piece_rows(c, x) for x in (chip, chip_r, chip_l, chip_o))
        u = a * N_CHUNKS + c
        slot = pl.ds(u * piece, piece)
        pa, oa = part.at[a], full[a]
        if i == 0:
            src, dst, dev = pa.at[half_rows(c, 1 - core)], d2d.at[pl.ds(u * half, half)], partner
        elif i == 1:
            src, dst, dev = pa.at[rows_o, lo], ring1.at[0, slot], right
        elif i == 2:
            src, dst, dev = pa.at[rows_o, hi], ring1.at[1, slot], left
        elif i == 3:
            src, dst, dev = pa.at[rows_r, hi], ring2.at[0, slot, hi], right
        elif i == 4:
            src, dst, dev = pa.at[rows_l, lo], ring2.at[1, slot, lo], left
        elif i == 5:
            src, dst, dev = pa.at[rows_r, lo], ring2.at[0, slot, lo], right
        elif i == 6:
            src, dst, dev = pa.at[rows_l, hi], ring2.at[1, slot, hi], left
        elif i == 7:
            src, dst, dev = oa.at[rows_own], oa.at[rows_own], right
        elif i == 8:
            src, dst, dev = oa.at[rows_own], oa.at[rows_own], left
        elif i == 9:
            src, dst, dev = oa.at[rows_l, lo], oa.at[rows_l, lo], right
        elif i == 10:
            src, dst, dev = oa.at[rows_r, hi], oa.at[rows_r, hi], left
        else:
            src, dst, dev = oa.at[half_rows(c, core)], oa.at[half_rows(c, core)], partner
        return pltpu.make_async_remote_copy(src, dst, send_sem.at[i], recv_sem.at[RECV_SLOT[i], shared(a, c)],
                                            device_id={'tp': dev}, device_id_type=MESH)

    def send(a, c, *ids):
        for i in ids:
            msg(a, c, i).start()

    def recv(a, c, *slots):
        u = pl.ds((a * N_CHUNKS + c) * piece, piece)
        own = full[a].at[piece_rows(c, chip)]
        whole = (d2d.at[pl.ds((a * N_CHUNKS + c) * half, half)], ring1.at[0, u], ring1.at[1, u], ring2.at[:, u],
                 own, own, own, full[a].at[half_rows(c, core)])
        for s in slots:
            pltpu.make_async_copy(whole[s], whole[s], recv_sem.at[s, shared(a, c)]).wait()

    state = {'met': False}

    def f0(a, c):
        if not state['met']:
            pl.semaphore_wait(barrier, 3)
            state['met'] = True
        send(a, c, 0)

    def f1(a, c):
        recv(a, c, 0)
        rows = half_rows(c, core)
        part[a, rows] = part[a, rows] + d2d[pl.ds((a * N_CHUNKS + c) * half, half)]
        send(a, c, 1, 2, 3, 4)

    def f2r(a, c):
        recv(a, c, 1)
        rows = piece_rows(c, chip_r)
        part[a, rows, lo] = part[a, rows, lo] + ring1[0, pl.ds((a * N_CHUNKS + c) * piece, piece)]
        send(a, c, 5)

    def f2l(a, c):
        recv(a, c, 2)
        rows = piece_rows(c, chip_l)
        part[a, rows, hi] = part[a, rows, hi] + ring1[1, pl.ds((a * N_CHUNKS + c) * piece, piece)]
        send(a, c, 6)

    def f3(a, c):
        recv(a, c, 3)
        rows = piece_rows(c, chip)
        slot = pl.ds((a * N_CHUNKS + c) * piece, piece)
        total = part[a, rows] + ring2[0, slot] + ring2[1, slot]
        if a == 0:
            arrived(('own', 14))
            out = y2_own[own_rows(c)] - total
        elif a == 1:
            arrived(('own', 15))
            out = dy1_own[own_rows(c)] + rms_back(y1[rows], total)
        elif a == 2:
            out = y1[rows] - total
        else:
            out = dy2[rows] + rms_back(x2[rows], total)
        full[a][rows] = out
        send(a, c, 7, 8)

    def f4r(a, c):
        recv(a, c, 4)
        send(a, c, 9)

    def f4l(a, c):
        recv(a, c, 5)
        send(a, c, 10)

    def f5(a, c):
        recv(a, c, 6)
        send(a, c, 11)

    def f6(a, c):
        recv(a, c, 7)

    group = tokens // N_GROUPS

    def group_rows(g):
        return pl.ds(g * group, group)

    def g1(g):
        rows = group_rows(g)
        arrived(('y1', g))
        y_val = y1[rows]
        ng[rows] = (y_val * inv_rms(y_val)).astype(BF16)
        for j in range(n_blk):
            cols = pl.ds(j * 256, 256)
            arrived(('w1', j))
            pre = mm(ng[rows], w1[:, cols])
            th = jnp.tanh(GELU_C * (pre + GELU_A * (pre * pre * pre)))
            act[rows, cols] = (0.5 * pre * (1.0 + th)).astype(BF16)
            dact[rows, cols] = 0.5 * (1.0 + th) + (0.5 * pre) * (1.0 - th * th) * (
                GELU_C * (1.0 + (3.0 * GELU_A) * (pre * pre)))

    def g2(g):
        rows = group_rows(g)
        arrived(('w2',))
        part[0, rows] = mm(act[rows], w2[...])

    def g3(j):
        arrived(('dy2',))
        cols = pl.ds(j * (ff // N_PARTS), ff // N_PARTS)
        if j == 0:
            dyb[...] = dy2[...].astype(BF16)
        dpre[:, cols] = (dact[:, cols] * mm_nt(dyb[...], w2[cols])).astype(BF16)

    def g4(j):
        cols = pl.ds(j * (width // N_PARTS), width // N_PARTS)
        part[1, :, cols] = mm_nt(dpre[...], w1[cols])

    def prep():
        arrived(('wq',))
        wq_f[...] = wq_raw[...].astype(F32)
        for h in range(n_heads):
            wqkv[:, pl.ds(h * head_dim, head_dim)] = wq_f[pl.ds(h, width, stride=n_heads)].astype(BF16)

    def atf(g):
        rows = group_rows(g)
        arrived(('wk',), ('wv',))
        x_val = x2[rows]
        nf[rows] = (x_val * inv_rms(x_val)).astype(BF16)
        qkv[rows] = mm(nf[rows], wqkv[...]).astype(BF16)
        key = qkv[rows, pl.ds(qdim, head_dim)]
        val = qkv[rows, pl.ds(qdim + head_dim, head_dim)]
        n_seqs = group // seq_len
        row_pos = lax.broadcasted_iota(jnp.int32, (group, group), 0)
        col_pos = lax.broadcasted_iota(jnp.int32, (group, group), 1)
        visible = jnp.zeros((group, group), jnp.bool_)
        for s in range(n_seqs):
            base = s * seq_len
            stop = base + lens_ref[g * n_seqs + s]
            visible = visible | ((row_pos >= base) & (row_pos < base + seq_len)
                                 & (col_pos >= base) & (col_pos < stop) & (col_pos <= row_pos))
        for h in range(n_heads):
            cols = pl.ds(h * head_dim, head_dim)
            scores = mm_nt(qkv[rows, cols], key) * (head_dim ** -0.5)
            scores = jnp.where(visible, scores, MASK_VALUE)
            exps = jnp.exp(scores - jnp.max(scores, axis=-1, keepdims=True))
            probs = exps / jnp.sum(exps, axis=-1, keepdims=True)
            prob[h, rows] = probs
            attn[rows, cols] = mm(probs.astype(BF16), val).astype(BF16)

    def ato(g):
        rows = group_rows(g)
        arrived(('wo',))
        part[2, rows] = mm(attn[rows], wo[...])

    def atb(g):
        rows = group_rows(g)
        d_attn = mm_nt(dx1[rows].astype(BF16), wo[...]).astype(BF16)
        key = qkv[rows, pl.ds(qdim, head_dim)]
        val = qkv[rows, pl.ds(qdim + head_dim, head_dim)]
        d_key = jnp.zeros((group, head_dim), F32)
        d_val = jnp.zeros((group, head_dim), F32)
        for h in range(n_heads):
            cols = pl.ds(h * head_dim, head_dim)
            d_head = d_attn[:, h * head_dim:(h + 1) * head_dim]
            probs = prob[h, rows]
            d_probs = mm_nt(d_head, val)
            d_scores = probs * (d_probs - jnp.sum(probs * d_probs, axis=-1, keepdims=True)) * (head_dim ** -0.5)
            d_scores = d_scores.astype(BF16)
            dqkv[rows, cols] = mm(d_scores, key).astype(BF16)
            d_key = d_key + mm_tn(d_scores, qkv[rows, cols])
            d_val = d_val + mm_tn(probs.astype(BF16), d_head)
        dqkv[rows, pl.ds(qdim, head_dim)] = d_key.astype(BF16)
        dqkv[rows, pl.ds(qdim + head_dim, head_dim)] = d_val.astype(BF16)

    def atg(g):
        rows = group_rows(g)
        part[3, rows] = mm_nt(dqkv[rows], wqkv[...])

    steps = {'F0': f0, 'F1': f1, 'F2R': f2r, 'F2L': f2l, 'F3': f3, 'F4R': f4r, 'F4L': f4l, 'F5': f5, 'F6': f6,
             'G1': g1, 'G2': g2, 'G3': g3, 'G4': g4, 'PREP': prep, 'ATF': atf, 'ATO': ato, 'ATB': atb, 'ATG': atg}
    load_all()
    for name, *where in plan_order():
        steps[name](*where)
    sent = (d2d,) + (ring1.at[0],) * 6 + (ring2.at[0],) * 2 + (ring1.at[0],) * 2 + (d2d,)
    for i in range(N_MSGS):
        pltpu.make_async_copy(sent[i], sent[i], send_sem.at[i]).wait()


def block_call(n_tp, seq_lens, y_one, y_two, dy_one, dy_two, w_query, w_key, w_value, w_out, w_up, w_down):
    n_batch, seq_len, width = y_one.shape
    tokens = n_batch * seq_len
    n_heads, head_dim = w_query.shape[1], w_query.shape[2]
    ff = w_up.shape[1]
    qdim = n_heads * head_dim
    qkv_dim = qdim + 2 * head_dim
    units = N_SUMS * N_CHUNKS
    half = tokens // N_CHUNKS // 2
    piece = half // (n_tp // 2)
    acts = tuple(v.reshape(tokens, width) for v in (y_one, y_two, dy_one, dy_two))
    weights = (w_query.reshape(width * n_heads, head_dim), w_key.reshape(width, head_dim), w_value.reshape(width, head_dim),
               w_out.reshape(qdim, width), w_up, w_down)
    vm = pltpu.VMEM
    out_shape = [vm((tokens, width), F32)] * 4 + [
        vm((tokens, width), BF16), vm((tokens, width), BF16), vm((tokens, ff), BF16), vm((tokens, ff), BF16),
        vm((tokens, qdim), BF16), vm((tokens, qkv_dim), BF16), vm((tokens, width), BF16)]
    scratch = [
        vm((width, ff), BF16), vm((ff, width), BF16), vm((width, qkv_dim), BF16), vm((qdim, width), BF16),
        vm((width * n_heads, head_dim), BF16), vm((width * n_heads, head_dim), F32),
        vm((tokens, width), F32), vm((tokens, width), F32),
        vm((N_CHUNKS * piece, width), F32), vm((N_CHUNKS * piece, width), F32),
        vm((tokens, ff), F32), vm((tokens, qkv_dim), BF16), vm((n_heads, tokens, tokens // N_GROUPS), F32),
        vm((N_SUMS, tokens, width), F32), vm((units * half, width), F32),
        vm((2, units * piece, width // 2), F32), vm((2, units * piece, width), F32),
        pltpu.SemaphoreType.DMA((16,)), pltpu.SemaphoreType.DMA((N_MSGS,)), pltpu.SemaphoreType.DMA((8, units // 2)),
    ]
    return pl.pallas_call(
        functools.partial(block_kernel, n_tp, head_dim, seq_len),
        out_shape=out_shape,
        in_specs=[pl.BlockSpec(memory_space=pltpu.SMEM)] + [ANY] * 10,
        out_specs=[pl.BlockSpec(memory_space=pltpu.VMEM)] * len(out_shape),
        scratch_shapes=scratch,
        name='block_back',
        compiler_params=pltpu.CompilerParams(collective_id=0, has_side_effects=True,
                                             vmem_limit_bytes=46 * 1024 * 1024),
        cost_estimate=pl.CostEstimate(flops=10 ** 10, bytes_accessed=3 * 10 ** 7, transcendentals=10 ** 6),
    )(seq_lens, *acts, *weights)


def grads_kernel(head_dim, n_blk,
                 x2, dx1, x1, dx2, ng, nf, act, dpre, attn, dqkv, e_val,
                 x2_out, dx1_out, x1_out, dx2_out, dwq_out, dwk_out, dwv_out, dwo_out, dw1_out, dw2_out,
                 c_val, dwq, dwk, dwv, dwo, dw1, dw2, out_sem):
    outs = []

    def store(src, dst):
        outs.append(pltpu.make_async_copy(src, dst, out_sem.at[len(outs)]))
        outs[-1].start()

    store(x2, x2_out)
    store(dx1, dx1_out)
    width, ff = dw1.shape
    qdim = attn.shape[1]
    n_heads = qdim // head_dim
    rows2, rows1 = ff // n_blk, width // n_blk
    for j in range(n_blk):
        rows = pl.ds(j * rows2, rows2)
        dw2[rows] = mm_tn(act[:, rows], e_val[...])
        store(dw2.at[rows], dw2_out.at[rows])
    for j in range(n_blk):
        rows = pl.ds(j * rows1, rows1)
        dw1[rows] = mm_tn(ng[:, rows], dpre[...])
        store(dw1.at[rows], dw1_out.at[rows])
    store(x1, x1_out)
    store(dx2, dx2_out)
    c_val[...] = dx1[...].astype(BF16)
    for h in range(n_heads):
        rows = pl.ds(h * head_dim, head_dim)
        dwo[rows] = mm_tn(attn[:, rows], c_val[...])
        store(dwo.at[rows], dwo_out.at[rows])
    for j in range(n_blk // 2):
        step = width // (n_blk // 2)
        rows = pl.ds(j * step, step)
        grad = mm_tn(nf[:, rows], dqkv[...])
        for h in range(n_heads):
            dwq[pl.ds(j * step * n_heads + h, step, stride=n_heads)] = grad[:, h * head_dim:(h + 1) * head_dim]
        dwk[rows] = grad[:, qdim:qdim + head_dim]
        dwv[rows] = grad[:, qdim + head_dim:]
        rows_q = pl.ds(j * step * n_heads, step * n_heads)
        store(dwq.at[rows_q], dwq_out.at[rows_q])
        store(dwk.at[rows], dwk_out.at[rows])
        store(dwv.at[rows], dwv_out.at[rows])
    for copy in outs:
        copy.wait()


def grads_call(n_heads, head_dim, *saved):
    tokens, width = saved[0].shape
    ff, qdim = saved[6].shape[1], n_heads * head_dim
    sds, vm = jax.ShapeDtypeStruct, pltpu.VMEM
    dw_shapes = [(width * n_heads, head_dim), (width, head_dim), (width, head_dim), (qdim, width), (width, ff), (ff, width)]
    scratch = [vm((tokens, width), BF16)] + [vm(s, F32) for s in dw_shapes] + [pltpu.SemaphoreType.DMA((40,))]
    return pl.pallas_call(
        functools.partial(grads_kernel, head_dim, 8),
        out_shape=[sds((tokens, width), F32)] * 4 + [sds(s, F32) for s in dw_shapes],
        in_specs=[pl.BlockSpec(memory_space=pltpu.VMEM)] * len(saved),
        out_specs=[ANY] * 10,
        scratch_shapes=scratch,
        name='weight_grads',
        compiler_params=pltpu.CompilerParams(vmem_limit_bytes=34 * 1024 * 1024),
        cost_estimate=pl.CostEstimate(flops=4 * 10 ** 9, bytes_accessed=4 * 10 ** 7, transcendentals=0),
    )(*saved)


def solution(mesh):
    n_tp = mesh.shape['tp']
    act_spec = P('dp', None, None)
    w_specs = (P(None, None, 'tp', None), P(None, None, 'tp', None), P(None, None, 'tp', None),
               P(None, 'tp', None, None), P(None, None, 'tp'), P(None, 'tp', None))
    g_specs = (P('dp', None, 'tp', None), P('dp', None, 'tp', None), P('dp', None, 'tp', None),
               P('dp', 'tp', None, None), P('dp', None, 'tp'), P('dp', 'tp', None))

    def local_fn(y_one, y_two, dy_one, dy_two, seq_lens, w_query, w_key, w_value, w_out, w_up, w_down):
        n_heads, head_dim = w_query.shape[2], w_query.shape[3]
        ws = tuple(w[0] for w in (w_query, w_key, w_value, w_out, w_up, w_down))
        saved = block_call(n_tp, seq_lens, y_one, y_two, dy_one, dy_two, *ws)
        res = grads_call(n_heads, head_dim, *saved)
        dw = tuple(g.reshape((1,) + w.shape) for g, w in zip(res[4:], ws))
        return tuple(v.reshape(y_one.shape) for v in (res[2], res[0], res[1], res[3])) + dw

    return jax.shard_map(local_fn, mesh=mesh,
                         in_specs=(act_spec,) * 4 + (P('dp'),) + w_specs,
                         out_specs=(act_spec,) * 4 + g_specs,
                         check_vma=False)
```

```python
import functools
import jax
import jax.numpy as jnp
from jax import lax
from jax.experimental import pallas as pl
from jax.experimental.pallas import tpu as pltpu
from jax.sharding import PartitionSpec as P

F32 = jnp.float32
BF16 = jnp.bfloat16
EPS = 1e-5
MASK_VALUE = -1e30
GELU_C = 0.7978845608028654
GELU_A = 0.044715
MESH = pl.DeviceIdType.MESH
ANY = pl.BlockSpec(memory_space=pl.ANY)

N_CHUNKS = 4
N_GROUPS = 2
N_SUMS = 4
N_MSGS = 16
RECV_SLOT = (0, 1, 2, 3, 3, 3, 3, 4, 5, 6, 6, 7, 8, 7, 7, 7)

LOAD_US = 4.0
STEP_US = {'G1': 0.8, 'G2': 0.4, 'G3': 0.7, 'G4': 0.6, 'PREP': 1.0, 'ATF': 1.6, 'ATO': 0.3, 'ATB': 2.0, 'ATG': 0.6}
SUM_US = {'F0A': 0.03, 'F0B': 0.03, 'F1A': 0.1, 'F1B': 0.1, 'F2R': 0.05, 'F2L': 0.05, 'F3': 0.25, 'F4R': 0.03,
          'F4L': 0.03, 'F5': 0.03, 'F6': 0.03}
SENDS = {'F0A': (0,), 'F0B': (12,), 'F1A': (1, 4), 'F1B': (2, 3), 'F2R': (5,), 'F2L': (6,), 'F3': (7, 8, 11),
         'F4R': (9, 13), 'F4L': (10, 14), 'F5': (15,)}
RECVS = {'F1A': (0,), 'F1B': (12,), 'F2R': (1,), 'F2L': (2,), 'F3': (3, 4, 5, 6), 'F4R': (7,), 'F4L': (8,), 'F5': (9, 10),
         'F6': (11, 13, 14, 15)}
AFTER = {'F1A': ('F0A',), 'F1B': ('F0B',), 'F2R': ('F1A',), 'F2L': ('F1B',), 'F3': ('F2R', 'F2L'), 'F4R': ('F3',),
         'F4L': ('F3',), 'F5': ('F4R', 'F4L'), 'F6': ('F5',)}
MSG_US = ((0.8, 1.0),) + ((2.8, 1.9),) * 6 + ((5.6, 1.9),) * 2 + ((2.8, 1.9),) * 2 + ((0.4, 1.0), (0.8, 1.0)) + ((0.4, 1.0),) * 3
SAME_CHIP = (0, 11, 12, 13, 14, 15)
RANK = ('G1', 'G2', 'ATF', 'ATO', 'ATB', 'ATG', 'G3', 'G4', 'PREP')
BACKLOG_US = 5


def plan_order():
    per = N_CHUNKS // N_GROUPS
    todo = {}

    def add(key, needs, sends=()):
        todo[key] = (needs, STEP_US[key[0]] if key[0] in STEP_US else SUM_US[key[0]], sends)

    for g in range(N_GROUPS):
        chunks = range(g * per, (g + 1) * per)
        add(('G1', g), [('G2', g - 1, 1)] if g else [])
        add(('ATF', g), [('F6', 0, c) for c in chunks] + [('PREP',)])
        add(('ATB', g), [('F6', 1, c) for c in chunks] + [('ATF', g)])
        for j in range(2):
            add(('G2', g, j), [('G1', g)])
            add(('ATO', g, j), [('ATF', g)])
            add(('ATG', g, j), [('ATB', g)])
    for j in range(2):
        add(('G3', j), [('G1', g) for g in range(N_GROUPS)])
        add(('G4', j), [('G3', 0), ('G3', 1)])
    add(('PREP',), [('G4', 0), ('G4', 1)])
    for c in range(N_CHUNKS):
        g = c // per
        for a in range(N_SUMS):
            for name in SUM_US:
                needs = [(p, a, c) for p in AFTER.get(name, ())] + [(i, a, c) for i in RECVS.get(name, ())]
                if name in ('F0A', 'F0B'):
                    j = int(name == 'F0B')
                    needs.append((('G2', g, j), ('G4', j), ('ATO', g, j), ('ATG', g, j))[a])
                add((name, a, c), needs, SENDS.get(name, ()))

    def rank(key):
        if key[0] in STEP_US:
            return (1, RANK.index(key[0])) + key[1:]
        return (0,) + key[1:] + (key[0],)

    now, order, done, free = LOAD_US, [], {}, {}
    while todo:
        ready = {}
        for key, (needs, _, sends) in todo.items():
            if all(n in done for n in needs):
                queue = max([free.get(1 + i % 2, 0.0) for i in sends if i not in SAME_CHIP], default=0.0)
                ready[key] = max([done[n] for n in needs] + [queue - BACKLOG_US])
        now = max(now, min(ready.values()))
        key = min((k for k, at in ready.items() if at <= now), key=rank)
        _, cost, sends = todo.pop(key)
        now += cost
        done[key] = now
        order.append(key)
        for i in sends:
            link = 0 if i in SAME_CHIP else 1 + i % 2
            wire, delay = MSG_US[i]
            start = max(now, free.get(link, 0.0))
            free[link] = start + wire / N_CHUNKS
            done[(i,) + key[1:]] = free[link] + delay
    return order


def mm(lhs, rhs):
    return jnp.dot(lhs, rhs, preferred_element_type=F32)


def mm_nt(lhs, rhs):
    return lax.dot_general(lhs, rhs, (((1,), (1,)), ((), ())), preferred_element_type=F32)


def mm_tn(lhs, rhs):
    return lax.dot_general(lhs, rhs, (((0,), (0,)), ((), ())), preferred_element_type=F32)


def inv_rms(x_val):
    return lax.rsqrt(jnp.mean(x_val * x_val, axis=-1, keepdims=True) + EPS)


def rms_back(x_val, grad_norm):
    inv = inv_rms(x_val)
    normed = x_val * inv
    return inv * (grad_norm - normed * jnp.mean(grad_norm * normed, axis=-1, keepdims=True))


def block_kernel(n_tp, head_dim, seq_len,
                 lens_ref, y1_hbm, y2_hbm, dy1_hbm, dy2_hbm, wq_hbm, wk_hbm, wv_hbm, wo_hbm, w1_hbm, w2_hbm,
                 x2, dx1, x1, dx2, ng, nf, act, dpre, attn, dqkv, dyb,
                 w1, w2, wqkv, wo, wq_raw, wq_f, y1, dy2, y2_own, dy1_own, dact, qkv, prob,
                 part, d2d, ring1, ring2,
                 load_sem, send_sem, recv_sem):
    full = (x2, dx1, x1, dx2)
    tokens, width = y1.shape
    ff = w1.shape[1]
    qdim = attn.shape[1]
    n_heads = qdim // head_dim
    chunk = tokens // N_CHUNKS
    half = chunk // 2
    piece = half // (n_tp // 2)
    hw = width // 2
    n_chips = n_tp // 2

    me = lax.axis_index('tp')
    core = lax.rem(me, 2)
    chip = lax.div(me, 2)
    partner = me + 1 - 2 * core
    right = lax.rem(me + 2, n_tp)
    left = lax.rem(me + n_tp - 2, n_tp)
    chip_r = lax.rem(chip + 1, n_chips)
    chip_l = lax.rem(chip + n_chips - 1, n_chips)
    chip_o = lax.rem(chip + 2, n_chips)

    def half_rows(c, k):
        return pl.ds(pl.multiple_of(c * chunk + k * half, half), half)

    def piece_rows(c, x):
        return pl.ds(pl.multiple_of(c * chunk + core * half + x * piece, piece), piece)

    def own_rows(c):
        return pl.ds(c * piece, piece)

    lo, hi = pl.ds(0, hw), pl.ds(hw, hw)

    barrier = pltpu.get_barrier_semaphore()
    for dev in (partner, left, right):
        pl.semaphore_signal(barrier, inc=1, device_id={'tp': dev}, device_id_type=MESH)

    loads = {}

    def arrived(*names):
        for name in names:
            if name in loads:
                loads.pop(name).wait()

    n_blk = ff // 256

    free_sems = list(range(16))

    def load(name, *copies):
        sem = load_sem.at[free_sems.pop(0)]
        for src, dst in copies:
            pltpu.make_async_copy(src, dst, sem).start()
        whole = copies[0][1] if len(copies) == 1 else {'y2': y2_own, 'dy1': dy1_own}[name[0]]
        loads[name] = pltpu.make_async_copy(whole, whole, sem)

    def load_first():
        groups = [pl.ds(g * (tokens // N_GROUPS), tokens // N_GROUPS) for g in range(N_GROUPS)]
        load(('y1', 0), (y1_hbm.at[groups[0]], y1.at[groups[0]]))
        for j in range(n_blk):
            blk = pl.ds(j * 256, 256)
            load(('w1', j), (w1_hbm.at[:, blk], w1.at[:, blk]))
        for j, cols in enumerate((lo, hi)):
            load(('w2', j), (w2_hbm.at[:, cols], w2.at[:, cols]))
        for g in range(1, N_GROUPS):
            load(('y1', g), (y1_hbm.at[groups[g]], y1.at[groups[g]]))

    def load_rest():
        load(('dy2',), (dy2_hbm, dy2))
        load(('y2',), *((y2_hbm.at[piece_rows(c, chip)], y2_own.at[own_rows(c)]) for c in range(N_CHUNKS)))
        load(('dy1',), *((dy1_hbm.at[piece_rows(c, chip)], dy1_own.at[own_rows(c)]) for c in range(N_CHUNKS)))
        load(('wq',), (wq_hbm, wq_raw))
        load(('wk',), (wk_hbm, wqkv.at[:, pl.ds(qdim, head_dim)]))
        load(('wv',), (wv_hbm, wqkv.at[:, pl.ds(qdim + head_dim, head_dim)]))
        load(('wo',), (wo_hbm, wo))

    def shared(a, c):
        return a % 2 * N_CHUNKS + c

    def msg(a, c, i):
        rows_own, rows_r, rows_l, rows_o = (piece_rows(c, x) for x in (chip, chip_r, chip_l, chip_o))
        u = a * N_CHUNKS + c
        slot = pl.ds(u * piece, piece)
        pa, oa = part.at[a], full[a]
        if i == 0:
            src, dst, dev = pa.at[half_rows(c, 1 - core), lo], d2d.at[pl.ds(u * half, half), lo], partner
        elif i == 12:
            src, dst, dev = pa.at[half_rows(c, 1 - core), hi], d2d.at[pl.ds(u * half, half), hi], partner
        elif i == 1:
            src, dst, dev = pa.at[rows_o, lo], ring1.at[0, slot], right
        elif i == 2:
            src, dst, dev = pa.at[rows_o, hi], ring1.at[1, slot], left
        elif i == 3:
            src, dst, dev = pa.at[rows_r, hi], ring2.at[0, slot, hi], right
        elif i == 4:
            src, dst, dev = pa.at[rows_l, lo], ring2.at[1, slot, lo], left
        elif i == 5:
            src, dst, dev = pa.at[rows_r, lo], ring2.at[0, slot, lo], right
        elif i == 6:
            src, dst, dev = pa.at[rows_l, hi], ring2.at[1, slot, hi], left
        elif i == 7:
            src, dst, dev = oa.at[rows_own], oa.at[rows_own], right
        elif i == 8:
            src, dst, dev = oa.at[rows_own], oa.at[rows_own], left
        elif i == 9:
            src, dst, dev = oa.at[rows_l, lo], oa.at[rows_l, lo], right
        elif i == 10:
            src, dst, dev = oa.at[rows_r, hi], oa.at[rows_r, hi], left
        else:
            rows = {11: rows_own, 13: rows_l, 14: rows_r, 15: rows_o}[i]
            src, dst, dev = oa.at[rows], oa.at[rows], partner
        return pltpu.make_async_remote_copy(src, dst, send_sem.at[i], recv_sem.at[RECV_SLOT[i], shared(a, c)],
                                            device_id={'tp': dev}, device_id_type=MESH)

    def send(a, c, *ids):
        for i in ids:
            msg(a, c, i).start()

    def recv(a, c, *slots):
        u = pl.ds((a * N_CHUNKS + c) * piece, piece)
        own = full[a].at[piece_rows(c, chip)]
        pair = pl.ds((a * N_CHUNKS + c) * half, half)
        whole = (d2d.at[pair, lo], ring1.at[0, u], ring1.at[1, u], ring2.at[:, u],
                 own, own, own, full[a].at[half_rows(c, core)], d2d.at[pair, hi])
        for s in slots:
            pltpu.make_async_copy(whole[s], whole[s], recv_sem.at[s, shared(a, c)]).wait()

    state = {'met': False}

    def met():
        if not state['met']:
            pl.semaphore_wait(barrier, 3)
            state['met'] = True

    def f0a(a, c):
        met()
        send(a, c, 0)

    def f0b(a, c):
        met()
        send(a, c, 12)

    def add_pair(a, c, cols):
        rows = half_rows(c, core)
        part[a, rows, cols] = part[a, rows, cols] + d2d[pl.ds((a * N_CHUNKS + c) * half, half), cols]

    def f1a(a, c):
        recv(a, c, 0)
        add_pair(a, c, lo)
        send(a, c, 1, 4)

    def f1b(a, c):
        recv(a, c, 8)
        add_pair(a, c, hi)
        send(a, c, 2, 3)

    def f2r(a, c):
        recv(a, c, 1)
        rows = piece_rows(c, chip_r)
        part[a, rows, lo] = part[a, rows, lo] + ring1[0, pl.ds((a * N_CHUNKS + c) * piece, piece)]
        send(a, c, 5)

    def f2l(a, c):
        recv(a, c, 2)
        rows = piece_rows(c, chip_l)
        part[a, rows, hi] = part[a, rows, hi] + ring1[1, pl.ds((a * N_CHUNKS + c) * piece, piece)]
        send(a, c, 6)

    def f3(a, c):
        recv(a, c, 3)
        rows = piece_rows(c, chip)
        slot = pl.ds((a * N_CHUNKS + c) * piece, piece)
        total = part[a, rows] + ring2[0, slot] + ring2[1, slot]
        if a == 0:
            arrived(('y2',))
            out = y2_own[own_rows(c)] - total
        elif a == 1:
            arrived(('dy1',))
            out = dy1_own[own_rows(c)] + rms_back(y1[rows], total)
        elif a == 2:
            out = y1[rows] - total
        else:
            out = dy2[rows] + rms_back(x2[rows], total)
        full[a][rows] = out
        send(a, c, 7, 8, 11)

    def f4r(a, c):
        recv(a, c, 4)
        send(a, c, 9, 13)

    def f4l(a, c):
        recv(a, c, 5)
        send(a, c, 10, 14)

    def f5(a, c):
        recv(a, c, 6)
        send(a, c, 15)

    def f6(a, c):
        recv(a, c, 7)

    group = tokens // N_GROUPS

    def group_rows(g):
        return pl.ds(g * group, group)

    def g1(g):
        rows = group_rows(g)
        arrived(('y1', g))
        y_val = y1[rows]
        ng[rows] = (y_val * inv_rms(y_val)).astype(BF16)
        for j in range(n_blk):
            cols = pl.ds(j * 256, 256)
            arrived(('w1', j))
            pre = mm(ng[rows], w1[:, cols])
            th = jnp.tanh(GELU_C * (pre + GELU_A * (pre * pre * pre)))
            act[rows, cols] = (0.5 * pre * (1.0 + th)).astype(BF16)
            dact[rows, cols] = 0.5 * (1.0 + th) + (0.5 * pre) * (1.0 - th * th) * (
                GELU_C * (1.0 + (3.0 * GELU_A) * (pre * pre)))

    def g2(g, j):
        rows, cols = group_rows(g), (lo, hi)[j]
        arrived(('w2', j))
        if g == 0 and j == 1:
            load_rest()
        part[0, rows, cols] = mm(act[rows], w2[:, cols])

    def g3(j):
        arrived(('dy2',))
        cols = pl.ds(j * (ff // 2), ff // 2)
        if j == 0:
            dyb[...] = dy2[...].astype(BF16)
        dpre[:, cols] = (dact[:, cols] * mm_nt(dyb[...], w2[cols])).astype(BF16)

    def g4(j):
        cols = (lo, hi)[j]
        part[1, :, cols] = mm_nt(dpre[...], w1[cols])

    def prep():
        arrived(('wq',))
        wq_f[...] = wq_raw[...].astype(F32)
        for h in range(n_heads):
            wqkv[:, pl.ds(h * head_dim, head_dim)] = wq_f[pl.ds(h, width, stride=n_heads)].astype(BF16)

    def atf(g):
        rows = group_rows(g)
        arrived(('wk',), ('wv',))
        x_val = x2[rows]
        nf[rows] = (x_val * inv_rms(x_val)).astype(BF16)
        qkv[rows] = mm(nf[rows], wqkv[...]).astype(BF16)
        key = qkv[rows, pl.ds(qdim, head_dim)]
        val = qkv[rows, pl.ds(qdim + head_dim, head_dim)]
        n_seqs = group // seq_len
        row_pos = lax.broadcasted_iota(jnp.int32, (group, group), 0)
        col_pos = lax.broadcasted_iota(jnp.int32, (group, group), 1)
        visible = jnp.zeros((group, group), jnp.bool_)
        for s in range(n_seqs):
            base = s * seq_len
            stop = base + lens_ref[g * n_seqs + s]
            visible = visible | ((row_pos >= base) & (row_pos < base + seq_len)
                                 & (col_pos >= base) & (col_pos < stop) & (col_pos <= row_pos))
        for h in range(n_heads):
            cols = pl.ds(h * head_dim, head_dim)
            scores = mm_nt(qkv[rows, cols], key) * (head_dim ** -0.5)
            scores = jnp.where(visible, scores, MASK_VALUE)
            exps = jnp.exp(scores - jnp.max(scores, axis=-1, keepdims=True))
            probs = exps / jnp.sum(exps, axis=-1, keepdims=True)
            prob[h, rows] = probs
            attn[rows, cols] = mm(probs.astype(BF16), val).astype(BF16)

    def ato(g, j):
        rows, cols = group_rows(g), (lo, hi)[j]
        arrived(('wo',))
        part[2, rows, cols] = mm(attn[rows], wo[:, cols])

    def atb(g):
        rows = group_rows(g)
        d_attn = mm_nt(dx1[rows].astype(BF16), wo[...]).astype(BF16)
        key = qkv[rows, pl.ds(qdim, head_dim)]
        val = qkv[rows, pl.ds(qdim + head_dim, head_dim)]
        d_key = jnp.zeros((group, head_dim), F32)
        d_val = jnp.zeros((group, head_dim), F32)
        for h in range(n_heads):
            cols = pl.ds(h * head_dim, head_dim)
            d_head = d_attn[:, h * head_dim:(h + 1) * head_dim]
            probs = prob[h, rows]
            d_probs = mm_nt(d_head, val)
            d_scores = probs * (d_probs - jnp.sum(probs * d_probs, axis=-1, keepdims=True)) * (head_dim ** -0.5)
            d_scores = d_scores.astype(BF16)
            dqkv[rows, cols] = mm(d_scores, key).astype(BF16)
            d_key = d_key + mm_tn(d_scores, qkv[rows, cols])
            d_val = d_val + mm_tn(probs.astype(BF16), d_head)
        dqkv[rows, pl.ds(qdim, head_dim)] = d_key.astype(BF16)
        dqkv[rows, pl.ds(qdim + head_dim, head_dim)] = d_val.astype(BF16)

    def atg(g, j):
        rows, cols = group_rows(g), (lo, hi)[j]
        part[3, rows, cols] = mm_nt(dqkv[rows], wqkv[cols])

    steps = {'F0A': f0a, 'F0B': f0b, 'F1A': f1a, 'F1B': f1b, 'F2R': f2r, 'F2L': f2l, 'F3': f3, 'F4R': f4r, 'F4L': f4l, 'F5': f5, 'F6': f6,
             'G1': g1, 'G2': g2, 'G3': g3, 'G4': g4, 'PREP': prep, 'ATF': atf, 'ATO': ato, 'ATB': atb, 'ATG': atg}
    load_first()
    for name, *where in plan_order():
        steps[name](*where)
    sent = ((d2d.at[:, lo],) + (ring1.at[0],) * 6 + (ring2.at[0],) * 2 + (ring1.at[0],) * 2
            + (ring2.at[0], d2d.at[:, hi]) + (ring2.at[0],) * 3)
    for i in range(N_MSGS):
        pltpu.make_async_copy(sent[i], sent[i], send_sem.at[i]).wait()


def block_call(n_tp, seq_lens, y_one, y_two, dy_one, dy_two, w_query, w_key, w_value, w_out, w_up, w_down):
    n_batch, seq_len, width = y_one.shape
    tokens = n_batch * seq_len
    n_heads, head_dim = w_query.shape[1], w_query.shape[2]
    ff = w_up.shape[1]
    qdim = n_heads * head_dim
    qkv_dim = qdim + 2 * head_dim
    units = N_SUMS * N_CHUNKS
    half = tokens // N_CHUNKS // 2
    piece = half // (n_tp // 2)
    acts = tuple(v.reshape(tokens, width) for v in (y_one, y_two, dy_one, dy_two))
    weights = (w_query.reshape(width * n_heads, head_dim), w_key.reshape(width, head_dim), w_value.reshape(width, head_dim),
               w_out.reshape(qdim, width), w_up, w_down)
    vm = pltpu.VMEM
    out_shape = [vm((tokens, width), F32)] * 4 + [
        vm((tokens, width), BF16), vm((tokens, width), BF16), vm((tokens, ff), BF16), vm((tokens, ff), BF16),
        vm((tokens, qdim), BF16), vm((tokens, qkv_dim), BF16), vm((tokens, width), BF16)]
    scratch = [
        vm((width, ff), BF16), vm((ff, width), BF16), vm((width, qkv_dim), BF16), vm((qdim, width), BF16),
        vm((width * n_heads, head_dim), BF16), vm((width * n_heads, head_dim), F32),
        vm((tokens, width), F32), vm((tokens, width), F32),
        vm((N_CHUNKS * piece, width), F32), vm((N_CHUNKS * piece, width), F32),
        vm((tokens, ff), F32), vm((tokens, qkv_dim), BF16), vm((n_heads, tokens, tokens // N_GROUPS), F32),
        vm((N_SUMS, tokens, width), F32), vm((units * half, width), F32),
        vm((2, units * piece, width // 2), F32), vm((2, units * piece, width), F32),
        pltpu.SemaphoreType.DMA((16,)), pltpu.SemaphoreType.DMA((N_MSGS,)), pltpu.SemaphoreType.DMA((9, units // 2)),
    ]
    return pl.pallas_call(
        functools.partial(block_kernel, n_tp, head_dim, seq_len),
        out_shape=out_shape,
        in_specs=[pl.BlockSpec(memory_space=pltpu.SMEM)] + [ANY] * 10,
        out_specs=[pl.BlockSpec(memory_space=pltpu.VMEM)] * len(out_shape),
        scratch_shapes=scratch,
        name='block_back',
        compiler_params=pltpu.CompilerParams(collective_id=0, has_side_effects=True,
                                             vmem_limit_bytes=46 * 1024 * 1024),
        cost_estimate=pl.CostEstimate(flops=10 ** 10, bytes_accessed=3 * 10 ** 7, transcendentals=10 ** 6),
    )(seq_lens, *acts, *weights)


def grads_kernel(head_dim, n_blk,
                 x2, dx1, x1, dx2, ng, nf, act, dpre, attn, dqkv, e_val,
                 x2_out, dx1_out, x1_out, dx2_out, dwq_out, dwk_out, dwv_out, dwo_out, dw1_out, dw2_out,
                 c_val, dwq, dwk, dwv, dwo, dw1, dw2, out_sem):
    outs = []

    def store(src, dst):
        outs.append(pltpu.make_async_copy(src, dst, out_sem.at[len(outs)]))
        outs[-1].start()

    store(x2, x2_out)
    store(dx1, dx1_out)
    width, ff = dw1.shape
    qdim = attn.shape[1]
    n_heads = qdim // head_dim
    rows2, rows1 = ff // n_blk, width // n_blk
    for j in range(n_blk):
        rows = pl.ds(j * rows2, rows2)
        dw2[rows] = mm_tn(act[:, rows], e_val[...])
        store(dw2.at[rows], dw2_out.at[rows])
    for j in range(n_blk):
        rows = pl.ds(j * rows1, rows1)
        dw1[rows] = mm_tn(ng[:, rows], dpre[...])
        store(dw1.at[rows], dw1_out.at[rows])
    store(x1, x1_out)
    store(dx2, dx2_out)
    c_val[...] = dx1[...].astype(BF16)
    for h in range(n_heads):
        rows = pl.ds(h * head_dim, head_dim)
        dwo[rows] = mm_tn(attn[:, rows], c_val[...])
        store(dwo.at[rows], dwo_out.at[rows])
    for j in range(n_blk // 2):
        step = width // (n_blk // 2)
        rows = pl.ds(j * step, step)
        grad = mm_tn(nf[:, rows], dqkv[...])
        for h in range(n_heads):
            dwq[pl.ds(j * step * n_heads + h, step, stride=n_heads)] = grad[:, h * head_dim:(h + 1) * head_dim]
        dwk[rows] = grad[:, qdim:qdim + head_dim]
        dwv[rows] = grad[:, qdim + head_dim:]
        rows_q = pl.ds(j * step * n_heads, step * n_heads)
        store(dwq.at[rows_q], dwq_out.at[rows_q])
        store(dwk.at[rows], dwk_out.at[rows])
        store(dwv.at[rows], dwv_out.at[rows])
    for copy in outs:
        copy.wait()


def grads_call(n_heads, head_dim, *saved):
    tokens, width = saved[0].shape
    ff, qdim = saved[6].shape[1], n_heads * head_dim
    sds, vm = jax.ShapeDtypeStruct, pltpu.VMEM
    dw_shapes = [(width * n_heads, head_dim), (width, head_dim), (width, head_dim), (qdim, width), (width, ff), (ff, width)]
    scratch = [vm((tokens, width), BF16)] + [vm(s, F32) for s in dw_shapes] + [pltpu.SemaphoreType.DMA((40,))]
    return pl.pallas_call(
        functools.partial(grads_kernel, head_dim, 8),
        out_shape=[sds((tokens, width), F32)] * 4 + [sds(s, F32) for s in dw_shapes],
        in_specs=[pl.BlockSpec(memory_space=pltpu.VMEM)] * len(saved),
        out_specs=[ANY] * 10,
        scratch_shapes=scratch,
        name='weight_grads',
        compiler_params=pltpu.CompilerParams(vmem_limit_bytes=34 * 1024 * 1024),
        cost_estimate=pl.CostEstimate(flops=4 * 10 ** 9, bytes_accessed=4 * 10 ** 7, transcendentals=0),
    )(*saved)


def solution(mesh):
    n_tp = mesh.shape['tp']
    act_spec = P('dp', None, None)
    w_specs = (P(None, None, 'tp', None), P(None, None, 'tp', None), P(None, None, 'tp', None),
               P(None, 'tp', None, None), P(None, None, 'tp'), P(None, 'tp', None))
    g_specs = (P('dp', None, 'tp', None), P('dp', None, 'tp', None), P('dp', None, 'tp', None),
               P('dp', 'tp', None, None), P('dp', None, 'tp'), P('dp', 'tp', None))

    def local_fn(y_one, y_two, dy_one, dy_two, seq_lens, w_query, w_key, w_value, w_out, w_up, w_down):
        n_heads, head_dim = w_query.shape[2], w_query.shape[3]
        ws = tuple(w[0] for w in (w_query, w_key, w_value, w_out, w_up, w_down))
        saved = block_call(n_tp, seq_lens, y_one, y_two, dy_one, dy_two, *ws)
        res = grads_call(n_heads, head_dim, *saved)
        dw = tuple(g.reshape((1,) + w.shape) for g, w in zip(res[4:], ws))
        return tuple(v.reshape(y_one.shape) for v in (res[2], res[0], res[1], res[3])) + dw

    return jax.shard_map(local_fn, mesh=mesh,
                         in_specs=(act_spec,) * 4 + (P('dp'),) + w_specs,
                         out_specs=(act_spec,) * 4 + g_specs,
                         check_vma=False)
```

```python
import functools
import jax
import jax.numpy as jnp
from jax import lax
from jax.experimental import pallas as pl
from jax.experimental.pallas import tpu as pltpu
from jax.sharding import PartitionSpec as P

F32 = jnp.float32
BF16 = jnp.bfloat16
EPS = 1e-5
MASK_VALUE = -1e30
GELU_C = 0.7978845608028654
GELU_A = 0.044715
MESH = pl.DeviceIdType.MESH
ANY = pl.BlockSpec(memory_space=pl.ANY)

N_CHUNKS = 4
N_GROUPS = 2
N_SUMS = 4
N_MSGS = 16
RECV_SLOT = (0, 1, 2, 3, 3, 3, 3, 4, 5, 6, 6, 7, 8, 7, 7, 7)

LOAD_US = 4.0
STEP_US = {'G1': 0.7, 'G2': 0.4, 'G3': 0.6, 'G4': 0.5, 'PREP': 0.4, 'ATF': 1.2, 'ATO': 0.2, 'ATB': 1.5, 'ATG': 0.5}
SUM_US = {'F0A': 0.03, 'F0B': 0.03, 'F1A': 0.1, 'F1B': 0.1, 'F2R': 0.05, 'F2L': 0.05, 'F3': 0.25, 'F4R': 0.03,
          'F4L': 0.03, 'F5': 0.03, 'F6': 0.03}
SENDS = {'F0A': (0,), 'F0B': (12,), 'F1A': (1, 4), 'F1B': (2, 3), 'F2R': (5,), 'F2L': (6,), 'F3': (7, 8, 11),
         'F4R': (9, 13), 'F4L': (10, 14), 'F5': (15,)}
RECVS = {'F1A': (0,), 'F1B': (12,), 'F2R': (1,), 'F2L': (2,), 'F3': (3, 4, 5, 6), 'F4R': (7,), 'F4L': (8,), 'F5': (9, 10),
         'F6': (11, 13, 14, 15)}
AFTER = {'F1A': ('F0A',), 'F1B': ('F0B',), 'F2R': ('F1A',), 'F2L': ('F1B',), 'F3': ('F2R', 'F2L'), 'F4R': ('F3',),
         'F4L': ('F3',), 'F5': ('F4R', 'F4L'), 'F6': ('F5',)}
MSG_US = ((0.8, 1.1),) + ((2.8, 2.17),) * 6 + ((5.6, 2.17),) * 2 + ((2.8, 2.17),) * 2 + ((0.4, 1.1), (0.8, 1.1)) + ((0.4, 1.1),) * 3
SAME_CHIP = (0, 11, 12, 13, 14, 15)
RANK = ('G1', 'G2', 'ATF', 'ATO', 'ATB', 'ATG', 'G3', 'G4', 'PREP')
BACKLOG_US = (8.7, 4.2, 2.5, 11.5)
STEP_RANK = {'F0A': 5.4, 'F0B': -2.2, 'F1A': -0.2, 'F1B': -7.9, 'F2R': 5.1, 'F2L': 1.2, 'F3': 2.0, 'F4R': -3.8, 'F4L': -1.6, 'F5': -8.6, 'F6': 1.8}
SUM_RANK = (2.9, 6.4, 2.0, 13.4)
CHUNK_RANK = 4.27


def plan_order():
    per = N_CHUNKS // N_GROUPS
    todo = {}

    def add(key, needs, sends=()):
        todo[key] = (needs, STEP_US[key[0]] if key[0] in STEP_US else SUM_US[key[0]], sends)

    for g in range(N_GROUPS):
        chunks = range(g * per, (g + 1) * per)
        add(('G1', g), [('G2', g - 1, 1)] if g else [])
        add(('ATF', g), [('F6', 0, c) for c in chunks] + [('PREP',)])
        add(('ATB', g), [('F6', 1, c) for c in chunks] + [('ATF', g)])
        for j in range(2):
            add(('G2', g, j), [('G1', g)])
            add(('ATO', g, j), [('ATF', g)])
            add(('ATG', g, j), [('ATB', g)])
    for j in range(2):
        add(('G3', j), [('G1', g) for g in range(N_GROUPS)])
        add(('G4', j), [('G3', 0), ('G3', 1)])
    add(('PREP',), [('G4', 0), ('G4', 1)])
    for c in range(N_CHUNKS):
        g = c // per
        for a in range(N_SUMS):
            for name in SUM_US:
                needs = [(p, a, c) for p in AFTER.get(name, ())] + [(i, a, c) for i in RECVS.get(name, ())]
                if name in ('F0A', 'F0B'):
                    j = int(name == 'F0B')
                    needs.append((('G2', g, j), ('G4', j), ('ATO', g, j), ('ATG', g, j))[a])
                add((name, a, c), needs, SENDS.get(name, ()))

    def rank(key):
        if key[0] in STEP_US:
            return (1, RANK.index(key[0])) + key[1:]
        return (0, STEP_RANK[key[0]] + SUM_RANK[key[1]] + CHUNK_RANK * key[2])

    now, order, done, free = LOAD_US, [], {}, {}
    while todo:
        ready = {}
        for key, (needs, _, sends) in todo.items():
            if all(n in done for n in needs):
                queue = max([free.get(1 + i % 2, 0.0) for i in sends if i not in SAME_CHIP], default=0.0)
                ready[key] = max([done[n] for n in needs] + [queue - (BACKLOG_US[key[1]] if sends else 0.0)])
        now = max(now, min(ready.values()))
        key = min((k for k, at in ready.items() if at <= now), key=rank)
        _, cost, sends = todo.pop(key)
        now += cost
        done[key] = now
        order.append(key)
        for i in sends:
            link = 0 if i in SAME_CHIP else 1 + i % 2
            wire, delay = MSG_US[i]
            start = max(now, free.get(link, 0.0))
            free[link] = start + wire / N_CHUNKS
            done[(i,) + key[1:]] = free[link] + delay
    return order


def mm(lhs, rhs):
    return jnp.dot(lhs, rhs, preferred_element_type=F32)


def mm_nt(lhs, rhs):
    return lax.dot_general(lhs, rhs, (((1,), (1,)), ((), ())), preferred_element_type=F32)


def mm_tn(lhs, rhs):
    return lax.dot_general(lhs, rhs, (((0,), (0,)), ((), ())), preferred_element_type=F32)


def inv_rms(x_val):
    return lax.rsqrt(jnp.mean(x_val * x_val, axis=-1, keepdims=True) + EPS)


def rms_back(x_val, grad_norm):
    inv = inv_rms(x_val)
    normed = x_val * inv
    return inv * (grad_norm - normed * jnp.mean(grad_norm * normed, axis=-1, keepdims=True))


def block_kernel(n_tp, head_dim, seq_len,
                 lens_ref, y1_hbm, y2_hbm, dy1_hbm, dy2_hbm, wq_hbm, wk_hbm, wv_hbm, wo_hbm, w1_hbm, w2_hbm,
                 x2, dx1, x1, dx2, ng, nf, act, dpre, attn, dqkv, dyb,
                 w1, w2, wqkv, wo, wq_raw, wq_f, y1, dy2, y2_own, dy1_own, dact, qkv, prob,
                 part, d2d, ring1, ring2,
                 load_sem, send_sem, recv_sem):
    full = (x2, dx1, x1, dx2)
    tokens, width = y1.shape
    ff = w1.shape[1]
    qdim = attn.shape[1]
    n_heads = qdim // head_dim
    chunk = tokens // N_CHUNKS
    half = chunk // 2
    piece = half // (n_tp // 2)
    hw = width // 2
    n_chips = n_tp // 2

    me = lax.axis_index('tp')
    core = lax.rem(me, 2)
    chip = lax.div(me, 2)
    partner = me + 1 - 2 * core
    right = lax.rem(me + 2, n_tp)
    left = lax.rem(me + n_tp - 2, n_tp)
    chip_r = lax.rem(chip + 1, n_chips)
    chip_l = lax.rem(chip + n_chips - 1, n_chips)
    chip_o = lax.rem(chip + 2, n_chips)

    def half_rows(c, k):
        return pl.ds(pl.multiple_of(c * chunk + k * half, half), half)

    def piece_rows(c, x):
        return pl.ds(pl.multiple_of(c * chunk + core * half + x * piece, piece), piece)

    def own_rows(c):
        return pl.ds(c * piece, piece)

    lo, hi = pl.ds(0, hw), pl.ds(hw, hw)

    barrier = pltpu.get_barrier_semaphore()
    for dev in (partner, left, right):
        pl.semaphore_signal(barrier, inc=1, device_id={'tp': dev}, device_id_type=MESH)

    loads = {}

    def arrived(*names):
        for name in names:
            if name in loads:
                loads.pop(name).wait()

    n_blk = ff // 256

    free_sems = list(range(16))

    def load(name, *copies):
        sem = load_sem.at[free_sems.pop(0)]
        for src, dst in copies:
            pltpu.make_async_copy(src, dst, sem).start()
        whole = copies[0][1] if len(copies) == 1 else {'y2': y2_own, 'dy1': dy1_own}[name[0]]
        loads[name] = pltpu.make_async_copy(whole, whole, sem)

    def load_first():
        groups = [pl.ds(g * (tokens // N_GROUPS), tokens // N_GROUPS) for g in range(N_GROUPS)]
        load(('y1', 0), (y1_hbm.at[groups[0]], y1.at[groups[0]]))
        for j in range(n_blk):
            blk = pl.ds(j * 256, 256)
            load(('w1', j), (w1_hbm.at[:, blk], w1.at[:, blk]))
        for j, cols in enumerate((lo, hi)):
            load(('w2', j), (w2_hbm.at[:, cols], w2.at[:, cols]))
        for g in range(1, N_GROUPS):
            load(('y1', g), (y1_hbm.at[groups[g]], y1.at[groups[g]]))

    def load_rest():
        load(('dy2',), (dy2_hbm, dy2))
        load(('y2',), *((y2_hbm.at[piece_rows(c, chip)], y2_own.at[own_rows(c)]) for c in range(N_CHUNKS)))
        load(('dy1',), *((dy1_hbm.at[piece_rows(c, chip)], dy1_own.at[own_rows(c)]) for c in range(N_CHUNKS)))
        load(('wq',), (wq_hbm, wq_raw))
        load(('wk',), (wk_hbm, wqkv.at[:, pl.ds(qdim, head_dim)]))
        load(('wv',), (wv_hbm, wqkv.at[:, pl.ds(qdim + head_dim, head_dim)]))
        load(('wo',), (wo_hbm, wo))

    def shared(a, c):
        return a % 2 * N_CHUNKS + c

    def msg(a, c, i):
        rows_own, rows_r, rows_l, rows_o = (piece_rows(c, x) for x in (chip, chip_r, chip_l, chip_o))
        u = a * N_CHUNKS + c
        slot = pl.ds(u * piece, piece)
        pa, oa = part.at[a], full[a]
        if i == 0:
            src, dst, dev = pa.at[half_rows(c, 1 - core), lo], d2d.at[pl.ds(u * half, half), lo], partner
        elif i == 12:
            src, dst, dev = pa.at[half_rows(c, 1 - core), hi], d2d.at[pl.ds(u * half, half), hi], partner
        elif i == 1:
            src, dst, dev = pa.at[rows_o, lo], ring1.at[0, slot], right
        elif i == 2:
            src, dst, dev = pa.at[rows_o, hi], ring1.at[1, slot], left
        elif i == 3:
            src, dst, dev = pa.at[rows_r, hi], ring2.at[0, slot, hi], right
        elif i == 4:
            src, dst, dev = pa.at[rows_l, lo], ring2.at[1, slot, lo], left
        elif i == 5:
            src, dst, dev = pa.at[rows_r, lo], ring2.at[0, slot, lo], right
        elif i == 6:
            src, dst, dev = pa.at[rows_l, hi], ring2.at[1, slot, hi], left
        elif i == 7:
            src, dst, dev = oa.at[rows_own], oa.at[rows_own], right
        elif i == 8:
            src, dst, dev = oa.at[rows_own], oa.at[rows_own], left
        elif i == 9:
            src, dst, dev = oa.at[rows_l, lo], oa.at[rows_l, lo], right
        elif i == 10:
            src, dst, dev = oa.at[rows_r, hi], oa.at[rows_r, hi], left
        else:
            rows = {11: rows_own, 13: rows_l, 14: rows_r, 15: rows_o}[i]
            src, dst, dev = oa.at[rows], oa.at[rows], partner
        return pltpu.make_async_remote_copy(src, dst, send_sem.at[i], recv_sem.at[RECV_SLOT[i], shared(a, c)],
                                            device_id={'tp': dev}, device_id_type=MESH)

    def send(a, c, *ids):
        for i in ids:
            msg(a, c, i).start()

    def recv(a, c, *slots):
        u = pl.ds((a * N_CHUNKS + c) * piece, piece)
        own = full[a].at[piece_rows(c, chip)]
        pair = pl.ds((a * N_CHUNKS + c) * half, half)
        whole = (d2d.at[pair, lo], ring1.at[0, u], ring1.at[1, u], ring2.at[:, u],
                 own, own, own, full[a].at[half_rows(c, core)], d2d.at[pair, hi])
        for s in slots:
            pltpu.make_async_copy(whole[s], whole[s], recv_sem.at[s, shared(a, c)]).wait()

    state = {'met': False}

    def met():
        if not state['met']:
            pl.semaphore_wait(barrier, 3)
            state['met'] = True

    def f0a(a, c):
        met()
        send(a, c, 0)

    def f0b(a, c):
        met()
        send(a, c, 12)

    def add_pair(a, c, cols):
        rows = half_rows(c, core)
        part[a, rows, cols] = part[a, rows, cols] + d2d[pl.ds((a * N_CHUNKS + c) * half, half), cols]

    def f1a(a, c):
        recv(a, c, 0)
        add_pair(a, c, lo)
        send(a, c, 1, 4)

    def f1b(a, c):
        recv(a, c, 8)
        add_pair(a, c, hi)
        send(a, c, 2, 3)

    def f2r(a, c):
        recv(a, c, 1)
        rows = piece_rows(c, chip_r)
        part[a, rows, lo] = part[a, rows, lo] + ring1[0, pl.ds((a * N_CHUNKS + c) * piece, piece)]
        send(a, c, 5)

    def f2l(a, c):
        recv(a, c, 2)
        rows = piece_rows(c, chip_l)
        part[a, rows, hi] = part[a, rows, hi] + ring1[1, pl.ds((a * N_CHUNKS + c) * piece, piece)]
        send(a, c, 6)

    def f3(a, c):
        recv(a, c, 3)
        rows = piece_rows(c, chip)
        slot = pl.ds((a * N_CHUNKS + c) * piece, piece)
        total = part[a, rows] + ring2[0, slot] + ring2[1, slot]
        if a == 0:
            arrived(('y2',))
            out = y2_own[own_rows(c)] - total
        elif a == 1:
            arrived(('dy1',))
            out = dy1_own[own_rows(c)] + rms_back(y1[rows], total)
        elif a == 2:
            out = y1[rows] - total
        else:
            out = dy2[rows] + rms_back(x2[rows], total)
        full[a][rows] = out
        send(a, c, 7, 8, 11)

    def f4r(a, c):
        recv(a, c, 4)
        send(a, c, 9, 13)

    def f4l(a, c):
        recv(a, c, 5)
        send(a, c, 10, 14)

    def f5(a, c):
        recv(a, c, 6)
        send(a, c, 15)

    def f6(a, c):
        recv(a, c, 7)

    group = tokens // N_GROUPS

    def group_rows(g):
        return pl.ds(g * group, group)

    def g1(g):
        rows = group_rows(g)
        arrived(('y1', g))
        y_val = y1[rows]
        ng[rows] = (y_val * inv_rms(y_val)).astype(BF16)
        for j in range(n_blk):
            cols = pl.ds(j * 256, 256)
            arrived(('w1', j))
            pre = mm(ng[rows], w1[:, cols])
            th = jnp.tanh(GELU_C * (pre + GELU_A * (pre * pre * pre)))
            act[rows, cols] = (0.5 * pre * (1.0 + th)).astype(BF16)
            dact[rows, cols] = 0.5 * (1.0 + th) + (0.5 * pre) * (1.0 - th * th) * (
                GELU_C * (1.0 + (3.0 * GELU_A) * (pre * pre)))

    def g2(g, j):
        rows, cols = group_rows(g), (lo, hi)[j]
        arrived(('w2', j))
        if g == 0 and j == 1:
            load_rest()
        part[0, rows, cols] = mm(act[rows], w2[:, cols])

    def g3(j):
        arrived(('dy2',))
        cols = pl.ds(j * (ff // 2), ff // 2)
        if j == 0:
            dyb[...] = dy2[...].astype(BF16)
        dpre[:, cols] = (dact[:, cols] * mm_nt(dyb[...], w2[cols])).astype(BF16)

    def g4(j):
        cols = (lo, hi)[j]
        part[1, :, cols] = mm_nt(dpre[...], w1[cols])

    def prep():
        arrived(('wq',))
        wq_f[...] = wq_raw[...].astype(F32)
        for h in range(n_heads):
            wqkv[:, pl.ds(h * head_dim, head_dim)] = wq_f[pl.ds(h, width, stride=n_heads)].astype(BF16)

    def atf(g):
        rows = group_rows(g)
        arrived(('wk',), ('wv',))
        x_val = x2[rows]
        nf[rows] = (x_val * inv_rms(x_val)).astype(BF16)
        qkv[rows] = mm(nf[rows], wqkv[...]).astype(BF16)
        key = qkv[rows, pl.ds(qdim, head_dim)]
        val = qkv[rows, pl.ds(qdim + head_dim, head_dim)]
        n_seqs = group // seq_len
        row_pos = lax.broadcasted_iota(jnp.int32, (group, group), 0)
        col_pos = lax.broadcasted_iota(jnp.int32, (group, group), 1)
        visible = jnp.zeros((group, group), jnp.bool_)
        for s in range(n_seqs):
            base = s * seq_len
            stop = base + lens_ref[g * n_seqs + s]
            visible = visible | ((row_pos >= base) & (row_pos < base + seq_len)
                                 & (col_pos >= base) & (col_pos < stop) & (col_pos <= row_pos))
        for h in range(n_heads):
            cols = pl.ds(h * head_dim, head_dim)
            scores = mm_nt(qkv[rows, cols], key) * (head_dim ** -0.5)
            scores = jnp.where(visible, scores, MASK_VALUE)
            exps = jnp.exp(scores - jnp.max(scores, axis=-1, keepdims=True))
            probs = exps / jnp.sum(exps, axis=-1, keepdims=True)
            prob[h, rows] = probs
            attn[rows, cols] = mm(probs.astype(BF16), val).astype(BF16)

    def ato(g, j):
        rows, cols = group_rows(g), (lo, hi)[j]
        arrived(('wo',))
        part[2, rows, cols] = mm(attn[rows], wo[:, cols])

    def atb(g):
        rows = group_rows(g)
        d_attn = mm_nt(dx1[rows].astype(BF16), wo[...]).astype(BF16)
        key = qkv[rows, pl.ds(qdim, head_dim)]
        val = qkv[rows, pl.ds(qdim + head_dim, head_dim)]
        d_key = jnp.zeros((group, head_dim), F32)
        d_val = jnp.zeros((group, head_dim), F32)
        for h in range(n_heads):
            cols = pl.ds(h * head_dim, head_dim)
            d_head = d_attn[:, h * head_dim:(h + 1) * head_dim]
            probs = prob[h, rows]
            d_probs = mm_nt(d_head, val)
            d_scores = probs * (d_probs - jnp.sum(probs * d_probs, axis=-1, keepdims=True)) * (head_dim ** -0.5)
            d_scores = d_scores.astype(BF16)
            dqkv[rows, cols] = mm(d_scores, key).astype(BF16)
            d_key = d_key + mm_tn(d_scores, qkv[rows, cols])
            d_val = d_val + mm_tn(probs.astype(BF16), d_head)
        dqkv[rows, pl.ds(qdim, head_dim)] = d_key.astype(BF16)
        dqkv[rows, pl.ds(qdim + head_dim, head_dim)] = d_val.astype(BF16)

    def atg(g, j):
        rows, cols = group_rows(g), (lo, hi)[j]
        part[3, rows, cols] = mm_nt(dqkv[rows], wqkv[cols])

    steps = {'F0A': f0a, 'F0B': f0b, 'F1A': f1a, 'F1B': f1b, 'F2R': f2r, 'F2L': f2l, 'F3': f3, 'F4R': f4r, 'F4L': f4l, 'F5': f5, 'F6': f6,
             'G1': g1, 'G2': g2, 'G3': g3, 'G4': g4, 'PREP': prep, 'ATF': atf, 'ATO': ato, 'ATB': atb, 'ATG': atg}
    load_first()
    for name, *where in plan_order():
        steps[name](*where)
    sent = ((d2d.at[:, lo],) + (ring1.at[0],) * 6 + (ring2.at[0],) * 2 + (ring1.at[0],) * 2
            + (ring2.at[0], d2d.at[:, hi]) + (ring2.at[0],) * 3)
    for i in range(N_MSGS):
        pltpu.make_async_copy(sent[i], sent[i], send_sem.at[i]).wait()


def block_call(n_tp, seq_lens, y_one, y_two, dy_one, dy_two, w_query, w_key, w_value, w_out, w_up, w_down):
    n_batch, seq_len, width = y_one.shape
    tokens = n_batch * seq_len
    n_heads, head_dim = w_query.shape[1], w_query.shape[2]
    ff = w_up.shape[1]
    qdim = n_heads * head_dim
    qkv_dim = qdim + 2 * head_dim
    units = N_SUMS * N_CHUNKS
    half = tokens // N_CHUNKS // 2
    piece = half // (n_tp // 2)
    acts = tuple(v.reshape(tokens, width) for v in (y_one, y_two, dy_one, dy_two))
    weights = (w_query.reshape(width * n_heads, head_dim), w_key.reshape(width, head_dim), w_value.reshape(width, head_dim),
               w_out.reshape(qdim, width), w_up, w_down)
    vm = pltpu.VMEM
    out_shape = [vm((tokens, width), F32)] * 4 + [
        vm((tokens, width), BF16), vm((tokens, width), BF16), vm((tokens, ff), BF16), vm((tokens, ff), BF16),
        vm((tokens, qdim), BF16), vm((tokens, qkv_dim), BF16), vm((tokens, width), BF16)]
    scratch = [
        vm((width, ff), BF16), vm((ff, width), BF16), vm((width, qkv_dim), BF16), vm((qdim, width), BF16),
        vm((width * n_heads, head_dim), BF16), vm((width * n_heads, head_dim), F32),
        vm((tokens, width), F32), vm((tokens, width), F32),
        vm((N_CHUNKS * piece, width), F32), vm((N_CHUNKS * piece, width), F32),
        vm((tokens, ff), F32), vm((tokens, qkv_dim), BF16), vm((n_heads, tokens, tokens // N_GROUPS), F32),
        vm((N_SUMS, tokens, width), F32), vm((units * half, width), F32),
        vm((2, units * piece, width // 2), F32), vm((2, units * piece, width), F32),
        pltpu.SemaphoreType.DMA((16,)), pltpu.SemaphoreType.DMA((N_MSGS,)), pltpu.SemaphoreType.DMA((9, units // 2)),
    ]
    return pl.pallas_call(
        functools.partial(block_kernel, n_tp, head_dim, seq_len),
        out_shape=out_shape,
        in_specs=[pl.BlockSpec(memory_space=pltpu.SMEM)] + [ANY] * 10,
        out_specs=[pl.BlockSpec(memory_space=pltpu.VMEM)] * len(out_shape),
        scratch_shapes=scratch,
        name='block_back',
        compiler_params=pltpu.CompilerParams(collective_id=0, has_side_effects=True,
                                             vmem_limit_bytes=46 * 1024 * 1024),
        cost_estimate=pl.CostEstimate(flops=10 ** 10, bytes_accessed=3 * 10 ** 7, transcendentals=10 ** 6),
    )(seq_lens, *acts, *weights)


def grads_kernel(head_dim, n_blk,
                 x2, dx1, x1, dx2, ng, nf, act, dpre, attn, dqkv, e_val,
                 x2_out, dx1_out, x1_out, dx2_out, dwq_out, dwk_out, dwv_out, dwo_out, dw1_out, dw2_out,
                 c_val, dwq, dwk, dwv, dwo, dw1, dw2, out_sem):
    outs = []

    def store(src, dst):
        outs.append(pltpu.make_async_copy(src, dst, out_sem.at[len(outs)]))
        outs[-1].start()

    store(x2, x2_out)
    store(dx1, dx1_out)
    width, ff = dw1.shape
    qdim = attn.shape[1]
    n_heads = qdim // head_dim
    rows2, rows1 = ff // n_blk, width // n_blk
    for j in range(n_blk):
        rows = pl.ds(j * rows2, rows2)
        dw2[rows] = mm_tn(act[:, rows], e_val[...])
        store(dw2.at[rows], dw2_out.at[rows])
    for j in range(n_blk):
        rows = pl.ds(j * rows1, rows1)
        dw1[rows] = mm_tn(ng[:, rows], dpre[...])
        store(dw1.at[rows], dw1_out.at[rows])
    store(x1, x1_out)
    store(dx2, dx2_out)
    c_val[...] = dx1[...].astype(BF16)
    for h in range(n_heads):
        rows = pl.ds(h * head_dim, head_dim)
        dwo[rows] = mm_tn(attn[:, rows], c_val[...])
        store(dwo.at[rows], dwo_out.at[rows])
    for j in range(n_blk // 2):
        step = width // (n_blk // 2)
        rows = pl.ds(j * step, step)
        grad = mm_tn(nf[:, rows], dqkv[...])
        for h in range(n_heads):
            dwq[pl.ds(j * step * n_heads + h, step, stride=n_heads)] = grad[:, h * head_dim:(h + 1) * head_dim]
        dwk[rows] = grad[:, qdim:qdim + head_dim]
        dwv[rows] = grad[:, qdim + head_dim:]
        rows_q = pl.ds(j * step * n_heads, step * n_heads)
        store(dwq.at[rows_q], dwq_out.at[rows_q])
        store(dwk.at[rows], dwk_out.at[rows])
        store(dwv.at[rows], dwv_out.at[rows])
    for copy in outs:
        copy.wait()


def grads_call(n_heads, head_dim, *saved):
    tokens, width = saved[0].shape
    ff, qdim = saved[6].shape[1], n_heads * head_dim
    sds, vm = jax.ShapeDtypeStruct, pltpu.VMEM
    dw_shapes = [(width * n_heads, head_dim), (width, head_dim), (width, head_dim), (qdim, width), (width, ff), (ff, width)]
    scratch = [vm((tokens, width), BF16)] + [vm(s, F32) for s in dw_shapes] + [pltpu.SemaphoreType.DMA((40,))]
    return pl.pallas_call(
        functools.partial(grads_kernel, head_dim, 8),
        out_shape=[sds((tokens, width), F32)] * 4 + [sds(s, F32) for s in dw_shapes],
        in_specs=[pl.BlockSpec(memory_space=pltpu.VMEM)] * len(saved),
        out_specs=[ANY] * 10,
        scratch_shapes=scratch,
        name='weight_grads',
        compiler_params=pltpu.CompilerParams(vmem_limit_bytes=34 * 1024 * 1024),
        cost_estimate=pl.CostEstimate(flops=4 * 10 ** 9, bytes_accessed=4 * 10 ** 7, transcendentals=0),
    )(*saved)


def solution(mesh):
    n_tp = mesh.shape['tp']
    act_spec = P('dp', None, None)
    w_specs = (P(None, None, 'tp', None), P(None, None, 'tp', None), P(None, None, 'tp', None),
               P(None, 'tp', None, None), P(None, None, 'tp'), P(None, 'tp', None))
    g_specs = (P('dp', None, 'tp', None), P('dp', None, 'tp', None), P('dp', None, 'tp', None),
               P('dp', 'tp', None, None), P('dp', None, 'tp'), P('dp', 'tp', None))

    def local_fn(y_one, y_two, dy_one, dy_two, seq_lens, w_query, w_key, w_value, w_out, w_up, w_down):
        n_heads, head_dim = w_query.shape[2], w_query.shape[3]
        ws = tuple(w[0] for w in (w_query, w_key, w_value, w_out, w_up, w_down))
        saved = block_call(n_tp, seq_lens, y_one, y_two, dy_one, dy_two, *ws)
        res = grads_call(n_heads, head_dim, *saved)
        dw = tuple(g.reshape((1,) + w.shape) for g, w in zip(res[4:], ws))
        return tuple(v.reshape(y_one.shape) for v in (res[2], res[0], res[1], res[3])) + dw

    return jax.shard_map(local_fn, mesh=mesh,
                         in_specs=(act_spec,) * 4 + (P('dp'),) + w_specs,
                         out_specs=(act_spec,) * 4 + g_specs,
                         check_vma=False)
```

```python
import functools
import jax
import jax.numpy as jnp
from jax import lax
from jax.experimental import pallas as pl
from jax.experimental.pallas import tpu as pltpu
from jax.sharding import PartitionSpec as P

F32 = jnp.float32
BF16 = jnp.bfloat16
EPS = 1e-5
MASK_VALUE = -1e30
GELU_C = 0.7978845608028654
GELU_A = 0.044715
MESH = pl.DeviceIdType.MESH
ANY = pl.BlockSpec(memory_space=pl.ANY)

N_CHUNKS = 4
N_GROUPS = 2
N_SUMS = 4
N_MSGS = 16
SEND_SLOT = (0, 0, 0, 0, 0, 0, 0, 1, 1, 0, 0, 1, 0, 1, 1, 1)
RECV_SLOT = (0, 1, 2, 3, 3, 3, 3, 4, 5, 6, 6, 7, 8, 7, 7, 7)

LOAD_US = 4.0
STEP_US = {'G1': 0.7, 'G2': 0.4, 'G3': 0.6, 'G4': 0.5, 'PREP': 0.4, 'ATF': 1.2, 'ATO': 0.2, 'ATB': 1.5, 'ATG': 0.5}
SUM_US = {'F0A': 0.03, 'F0B': 0.03, 'F1A': 0.1, 'F1B': 0.1, 'F2R': 0.05, 'F2L': 0.05, 'F3': 0.25, 'F4R': 0.03,
          'F4L': 0.03, 'F5': 0.03, 'F6': 0.03}
SENDS = {'F0A': (0,), 'F0B': (12,), 'F1A': (1, 4), 'F1B': (2, 3), 'F2R': (5,), 'F2L': (6,), 'F3': (7, 8, 11),
         'F4R': (9, 13), 'F4L': (10, 14), 'F5': (15,)}
RECVS = {'F1A': (0,), 'F1B': (12,), 'F2R': (1,), 'F2L': (2,), 'F3': (3, 4, 5, 6), 'F4R': (7,), 'F4L': (8,), 'F5': (9, 10),
         'F6': (11, 13, 14, 15)}
AFTER = {'F1A': ('F0A',), 'F1B': ('F0B',), 'F2R': ('F1A',), 'F2L': ('F1B',), 'F3': ('F2R', 'F2L'), 'F4R': ('F3',),
         'F4L': ('F3',), 'F5': ('F4R', 'F4L'), 'F6': ('F5',)}
MSG_US = ((0.8, 1.1),) + ((2.8, 2.17),) * 6 + ((5.6, 2.17),) * 2 + ((2.8, 2.17),) * 2 + ((0.4, 1.1), (0.8, 1.1)) + ((0.4, 1.1),) * 3
SAME_CHIP = (0, 11, 12, 13, 14, 15)
RANK = ('G1', 'G2', 'ATF', 'ATO', 'ATB', 'ATG', 'G3', 'G4', 'PREP')
BACKLOG_US = (8.7, 4.2, 2.5, 11.5)
STEP_RANK = {'F0A': 5.4, 'F0B': -2.2, 'F1A': -0.2, 'F1B': -7.9, 'F2R': 5.1, 'F2L': 1.2, 'F3': 2.0, 'F4R': -3.8, 'F4L': -1.6, 'F5': -8.6, 'F6': 1.8}
SUM_RANK = (2.9, 6.4, 2.0, 13.4)
CHUNK_RANK = 4.27


def plan_order():
    per = N_CHUNKS // N_GROUPS
    todo = {}

    def add(key, needs, sends=()):
        todo[key] = (needs, STEP_US[key[0]] if key[0] in STEP_US else SUM_US[key[0]], sends)

    for g in range(N_GROUPS):
        chunks = range(g * per, (g + 1) * per)
        add(('G1', g), [('G2', g - 1, 1)] if g else [])
        add(('ATF', g), [('F6', 0, c) for c in chunks] + [('PREP',)])
        add(('ATB', g), [('F6', 1, c) for c in chunks] + [('ATF', g)])
        for j in range(2):
            add(('G2', g, j), [('G1', g)])
            add(('ATO', g, j), [('ATF', g)])
            add(('ATG', g, j), [('ATB', g)])
    for j in range(2):
        add(('G3', j), [('G1', g) for g in range(N_GROUPS)])
        add(('G4', j), [('G3', 0), ('G3', 1)])
    add(('PREP',), [('G4', 0), ('G4', 1)])
    for c in range(N_CHUNKS):
        g = c // per
        for a in range(N_SUMS):
            for name in SUM_US:
                needs = [(p, a, c) for p in AFTER.get(name, ())] + [(i, a, c) for i in RECVS.get(name, ())]
                if name in ('F0A', 'F0B'):
                    j = int(name == 'F0B')
                    needs.append((('G2', g, j), ('G4', j), ('ATO', g, j), ('ATG', g, j))[a])
                add((name, a, c), needs, SENDS.get(name, ()))

    def rank(key):
        if key[0] in STEP_US:
            return (1, RANK.index(key[0])) + key[1:]
        return (0, STEP_RANK[key[0]] + SUM_RANK[key[1]] + CHUNK_RANK * key[2])

    now, order, done, free = LOAD_US, [], {}, {}
    while todo:
        ready = {}
        for key, (needs, _, sends) in todo.items():
            if all(n in done for n in needs):
                queue = max([free.get(1 + i % 2, 0.0) for i in sends if i not in SAME_CHIP], default=0.0)
                ready[key] = max([done[n] for n in needs] + [queue - (BACKLOG_US[key[1]] if sends else 0.0)])
        now = max(now, min(ready.values()))
        key = min((k for k, at in ready.items() if at <= now), key=rank)
        _, cost, sends = todo.pop(key)
        now += cost
        done[key] = now
        order.append(key)
        for i in sends:
            link = 0 if i in SAME_CHIP else 1 + i % 2
            wire, delay = MSG_US[i]
            start = max(now, free.get(link, 0.0))
            free[link] = start + wire / N_CHUNKS
            done[(i,) + key[1:]] = free[link] + delay
    return order


def mm(lhs, rhs):
    return jnp.dot(lhs, rhs, preferred_element_type=F32)


def mm_nt(lhs, rhs):
    return lax.dot_general(lhs, rhs, (((1,), (1,)), ((), ())), preferred_element_type=F32)


def mm_tn(lhs, rhs):
    return lax.dot_general(lhs, rhs, (((0,), (0,)), ((), ())), preferred_element_type=F32)


def inv_rms(x_val):
    return lax.rsqrt(jnp.mean(x_val * x_val, axis=-1, keepdims=True) + EPS)


def rms_back(x_val, grad_norm):
    inv = inv_rms(x_val)
    normed = x_val * inv
    return inv * (grad_norm - normed * jnp.mean(grad_norm * normed, axis=-1, keepdims=True))


def block_kernel(n_tp, head_dim, seq_len,
                 lens_hbm, y1_hbm, y2_hbm, dy1_hbm, dy2_hbm, wq_hbm, wk_hbm, wv_hbm, wo_hbm, w1_hbm, w2_hbm,
                 x2, dx1, x1, dx2, ng, nf, act, dpre, attn, dqkv, dyb,
                 w1, w2, wqkv, wo, wq_raw, wq_f, y1, dy2, y2_own, dy1_own, dact, qkv, prob,
                 part, d2d, ring1, ring2,
                 lens, load_sem, send_sem, recv_sem):
    full = (x2, dx1, x1, dx2)
    tokens, width = y1.shape
    ff = w1.shape[1]
    qdim = attn.shape[1]
    n_heads = qdim // head_dim
    chunk = tokens // N_CHUNKS
    half = chunk // 2
    piece = half // (n_tp // 2)
    hw = width // 2
    n_chips = n_tp // 2

    me = lax.axis_index('tp')
    core = lax.rem(me, 2)
    chip = lax.div(me, 2)
    partner = me + 1 - 2 * core
    right = lax.rem(me + 2, n_tp)
    left = lax.rem(me + n_tp - 2, n_tp)
    chip_r = lax.rem(chip + 1, n_chips)
    chip_l = lax.rem(chip + n_chips - 1, n_chips)
    chip_o = lax.rem(chip + 2, n_chips)

    def half_rows(c, k):
        return pl.ds(pl.multiple_of(c * chunk + k * half, half), half)

    def piece_rows(c, x):
        return pl.ds(pl.multiple_of(c * chunk + core * half + x * piece, piece), piece)

    def own_rows(c):
        return pl.ds(c * piece, piece)

    lo, hi = pl.ds(0, hw), pl.ds(hw, hw)

    barrier = pltpu.get_barrier_semaphore()
    for dev in (partner, left, right):
        pl.semaphore_signal(barrier, inc=1, device_id={'tp': dev}, device_id_type=MESH)

    loads = {}

    def arrived(*names):
        for name in names:
            if name in loads:
                loads.pop(name).wait()

    n_blk = ff // 512

    free_sems = list(range(14))

    def load(name, *copies):
        sem = load_sem.at[free_sems.pop(0)]
        for src, dst in copies:
            pltpu.make_async_copy(src, dst, sem).start()
        whole = copies[0][1] if len(copies) == 1 else {'y2': y2_own, 'dy1': dy1_own}[name[0]]
        loads[name] = pltpu.make_async_copy(whole, whole, sem)

    def load_first():
        groups = [pl.ds(g * (tokens // N_GROUPS), tokens // N_GROUPS) for g in range(N_GROUPS)]
        load(('y1', 0), (y1_hbm.at[groups[0]], y1.at[groups[0]]))
        for j in range(n_blk):
            blk = pl.ds(j * 512, 512)
            load(('w1', j), (w1_hbm.at[:, blk], w1.at[:, blk]))
        for j, cols in enumerate((lo, hi)):
            load(('w2', j), (w2_hbm.at[:, cols], w2.at[:, cols]))
        for g in range(1, N_GROUPS):
            load(('y1', g), (y1_hbm.at[groups[g]], y1.at[groups[g]]))

    def load_rest():
        load(('dy2',), (dy2_hbm, dy2))
        load(('y2',), *((y2_hbm.at[piece_rows(c, chip)], y2_own.at[own_rows(c)]) for c in range(N_CHUNKS)))
        load(('dy1',), *((dy1_hbm.at[piece_rows(c, chip)], dy1_own.at[own_rows(c)]) for c in range(N_CHUNKS)))
        load(('wq',), (wq_hbm, wq_raw))
        load(('wk',), (wk_hbm, wqkv.at[:, pl.ds(qdim, head_dim)]))
        load(('wv',), (wv_hbm, wqkv.at[:, pl.ds(qdim + head_dim, head_dim)]))
        load(('wo',), (wo_hbm, wo))
        load(('lens',), (lens_hbm, lens))

    def shared(a, c):
        return a % 2 * N_CHUNKS + c

    def msg(a, c, i):
        rows_own, rows_r, rows_l, rows_o = (piece_rows(c, x) for x in (chip, chip_r, chip_l, chip_o))
        u = a * N_CHUNKS + c
        slot = pl.ds(u * piece, piece)
        pa, oa = part.at[a], full[a]
        if i == 0:
            src, dst, dev = pa.at[half_rows(c, 1 - core), lo], d2d.at[pl.ds(u * half, half), lo], partner
        elif i == 12:
            src, dst, dev = pa.at[half_rows(c, 1 - core), hi], d2d.at[pl.ds(u * half, half), hi], partner
        elif i == 1:
            src, dst, dev = pa.at[rows_o, lo], ring1.at[0, slot], right
        elif i == 2:
            src, dst, dev = pa.at[rows_o, hi], ring1.at[1, slot], left
        elif i == 3:
            src, dst, dev = pa.at[rows_r, hi], ring2.at[0, slot, hi], right
        elif i == 4:
            src, dst, dev = pa.at[rows_l, lo], ring2.at[1, slot, lo], left
        elif i == 5:
            src, dst, dev = pa.at[rows_r, lo], ring2.at[0, slot, lo], right
        elif i == 6:
            src, dst, dev = pa.at[rows_l, hi], ring2.at[1, slot, hi], left
        elif i == 7:
            src, dst, dev = oa.at[rows_own], oa.at[rows_own], right
        elif i == 8:
            src, dst, dev = oa.at[rows_own], oa.at[rows_own], left
        elif i == 9:
            src, dst, dev = oa.at[rows_l, lo], oa.at[rows_l, lo], right
        elif i == 10:
            src, dst, dev = oa.at[rows_r, hi], oa.at[rows_r, hi], left
        else:
            rows = {11: rows_own, 13: rows_l, 14: rows_r, 15: rows_o}[i]
            src, dst, dev = oa.at[rows], oa.at[rows], partner
        return pltpu.make_async_remote_copy(src, dst, send_sem.at[SEND_SLOT[i]], recv_sem.at[RECV_SLOT[i], shared(a, c)],
                                            device_id={'tp': dev}, device_id_type=MESH)

    def send(a, c, *ids):
        for i in ids:
            msg(a, c, i).start()

    def recv(a, c, *slots):
        u = pl.ds((a * N_CHUNKS + c) * piece, piece)
        own = full[a].at[piece_rows(c, chip)]
        pair = pl.ds((a * N_CHUNKS + c) * half, half)
        whole = (d2d.at[pair, lo], ring1.at[0, u], ring1.at[1, u], ring2.at[:, u],
                 own, own, own, full[a].at[half_rows(c, core)], d2d.at[pair, hi])
        for s in slots:
            pltpu.make_async_copy(whole[s], whole[s], recv_sem.at[s, shared(a, c)]).wait()

    state = {'met': False}

    def met():
        if not state['met']:
            pl.semaphore_wait(barrier, 3)
            state['met'] = True

    def f0a(a, c):
        met()
        send(a, c, 0)

    def f0b(a, c):
        met()
        send(a, c, 12)

    def add_pair(a, c, cols):
        rows = half_rows(c, core)
        part[a, rows, cols] = part[a, rows, cols] + d2d[pl.ds((a * N_CHUNKS + c) * half, half), cols]

    def f1a(a, c):
        recv(a, c, 0)
        add_pair(a, c, lo)
        send(a, c, 1, 4)

    def f1b(a, c):
        recv(a, c, 8)
        add_pair(a, c, hi)
        send(a, c, 2, 3)

    def f2r(a, c):
        recv(a, c, 1)
        rows = piece_rows(c, chip_r)
        part[a, rows, lo] = part[a, rows, lo] + ring1[0, pl.ds((a * N_CHUNKS + c) * piece, piece)]
        send(a, c, 5)

    def f2l(a, c):
        recv(a, c, 2)
        rows = piece_rows(c, chip_l)
        part[a, rows, hi] = part[a, rows, hi] + ring1[1, pl.ds((a * N_CHUNKS + c) * piece, piece)]
        send(a, c, 6)

    def f3(a, c):
        recv(a, c, 3)
        rows = piece_rows(c, chip)
        slot = pl.ds((a * N_CHUNKS + c) * piece, piece)
        total = part[a, rows] + ring2[0, slot] + ring2[1, slot]
        if a == 0:
            arrived(('y2',))
            out = y2_own[own_rows(c)] - total
        elif a == 1:
            arrived(('dy1',))
            out = dy1_own[own_rows(c)] + rms_back(y1[rows], total)
        elif a == 2:
            out = y1[rows] - total
        else:
            out = dy2[rows] + rms_back(x2[rows], total)
        full[a][rows] = out
        send(a, c, 7, 8, 11)

    def f4r(a, c):
        recv(a, c, 4)
        send(a, c, 9, 13)

    def f4l(a, c):
        recv(a, c, 5)
        send(a, c, 10, 14)

    def f5(a, c):
        recv(a, c, 6)
        send(a, c, 15)

    def f6(a, c):
        recv(a, c, 7)

    group = tokens // N_GROUPS

    def group_rows(g):
        return pl.ds(g * group, group)

    def g1(g):
        rows = group_rows(g)
        arrived(('y1', g))
        y_val = y1[rows]
        ng[rows] = (y_val * inv_rms(y_val)).astype(BF16)
        for j in range(n_blk):
            cols = pl.ds(j * 512, 512)
            arrived(('w1', j))
            pre = mm(ng[rows], w1[:, cols])
            th = jnp.tanh(GELU_C * (pre + GELU_A * (pre * pre * pre)))
            act[rows, cols] = (0.5 * pre * (1.0 + th)).astype(BF16)
            dact[rows, cols] = 0.5 * (1.0 + th) + (0.5 * pre) * (1.0 - th * th) * (
                GELU_C * (1.0 + (3.0 * GELU_A) * (pre * pre)))

    def g2(g, j):
        rows, cols = group_rows(g), (lo, hi)[j]
        arrived(('w2', j))
        if g == 0 and j == 1:
            load_rest()
        part[0, rows, cols] = mm(act[rows], w2[:, cols])

    def g3(j):
        arrived(('dy2',))
        cols = pl.ds(j * (ff // 2), ff // 2)
        if j == 0:
            dyb[...] = dy2[...].astype(BF16)
        dpre[:, cols] = (dact[:, cols] * mm_nt(dyb[...], w2[cols])).astype(BF16)

    def g4(j):
        cols = (lo, hi)[j]
        part[1, :, cols] = mm_nt(dpre[...], w1[cols])

    def prep():
        arrived(('wq',))
        wq_f[...] = wq_raw[...].astype(F32)
        for h in range(n_heads):
            wqkv[:, pl.ds(h * head_dim, head_dim)] = wq_f[pl.ds(h, width, stride=n_heads)].astype(BF16)

    def atf(g):
        rows = group_rows(g)
        arrived(('wk',), ('wv',), ('lens',))
        x_val = x2[rows]
        nf[rows] = (x_val * inv_rms(x_val)).astype(BF16)
        qkv[rows] = mm(nf[rows], wqkv[...]).astype(BF16)
        key = qkv[rows, pl.ds(qdim, head_dim)]
        val = qkv[rows, pl.ds(qdim + head_dim, head_dim)]
        n_seqs = group // seq_len
        row_pos = lax.broadcasted_iota(jnp.int32, (group, group), 0)
        col_pos = lax.broadcasted_iota(jnp.int32, (group, group), 1)
        visible = jnp.zeros((group, group), jnp.bool_)
        for s in range(n_seqs):
            base = s * seq_len
            stop = base + lens[g * n_seqs + s]
            visible = visible | ((row_pos >= base) & (row_pos < base + seq_len)
                                 & (col_pos >= base) & (col_pos < stop) & (col_pos <= row_pos))
        for h in range(n_heads):
            cols = pl.ds(h * head_dim, head_dim)
            scores = mm_nt(qkv[rows, cols], key) * (head_dim ** -0.5)
            scores = jnp.where(visible, scores, MASK_VALUE)
            exps = jnp.exp(scores - jnp.max(scores, axis=-1, keepdims=True))
            probs = exps / jnp.sum(exps, axis=-1, keepdims=True)
            prob[h, rows] = probs
            attn[rows, cols] = mm(probs.astype(BF16), val).astype(BF16)

    def ato(g, j):
        rows, cols = group_rows(g), (lo, hi)[j]
        arrived(('wo',))
        part[2, rows, cols] = mm(attn[rows], wo[:, cols])

    def atb(g):
        rows = group_rows(g)
        d_attn = mm_nt(dx1[rows].astype(BF16), wo[...]).astype(BF16)
        key = qkv[rows, pl.ds(qdim, head_dim)]
        val = qkv[rows, pl.ds(qdim + head_dim, head_dim)]
        d_key = jnp.zeros((group, head_dim), F32)
        d_val = jnp.zeros((group, head_dim), F32)
        for h in range(n_heads):
            cols = pl.ds(h * head_dim, head_dim)
            d_head = d_attn[:, h * head_dim:(h + 1) * head_dim]
            probs = prob[h, rows]
            d_probs = mm_nt(d_head, val)
            d_scores = probs * (d_probs - jnp.sum(probs * d_probs, axis=-1, keepdims=True)) * (head_dim ** -0.5)
            d_scores = d_scores.astype(BF16)
            dqkv[rows, cols] = mm(d_scores, key).astype(BF16)
            d_key = d_key + mm_tn(d_scores, qkv[rows, cols])
            d_val = d_val + mm_tn(probs.astype(BF16), d_head)
        dqkv[rows, pl.ds(qdim, head_dim)] = d_key.astype(BF16)
        dqkv[rows, pl.ds(qdim + head_dim, head_dim)] = d_val.astype(BF16)

    def atg(g, j):
        rows, cols = group_rows(g), (lo, hi)[j]
        part[3, rows, cols] = mm_nt(dqkv[rows], wqkv[cols])

    steps = {'F0A': f0a, 'F0B': f0b, 'F1A': f1a, 'F1B': f1b, 'F2R': f2r, 'F2L': f2l, 'F3': f3, 'F4R': f4r, 'F4L': f4l, 'F5': f5, 'F6': f6,
             'G1': g1, 'G2': g2, 'G3': g3, 'G4': g4, 'PREP': prep, 'ATF': atf, 'ATO': ato, 'ATB': atb, 'ATG': atg}
    load_first()
    for name, *where in plan_order():
        steps[name](*where)
    for i, sent in enumerate((part, part.at[pl.ds(0, 3)])):
        pltpu.make_async_copy(sent, sent, send_sem.at[i]).wait()


def block_call(n_tp, seq_lens, y_one, y_two, dy_one, dy_two, w_query, w_key, w_value, w_out, w_up, w_down):
    n_batch, seq_len, width = y_one.shape
    tokens = n_batch * seq_len
    n_heads, head_dim = w_query.shape[1], w_query.shape[2]
    ff = w_up.shape[1]
    qdim = n_heads * head_dim
    qkv_dim = qdim + 2 * head_dim
    units = N_SUMS * N_CHUNKS
    half = tokens // N_CHUNKS // 2
    piece = half // (n_tp // 2)
    acts = tuple(v.reshape(tokens, width) for v in (y_one, y_two, dy_one, dy_two))
    weights = (w_query.reshape(width * n_heads, head_dim), w_key.reshape(width, head_dim), w_value.reshape(width, head_dim),
               w_out.reshape(qdim, width), w_up, w_down)
    vm = pltpu.VMEM
    out_shape = [vm((tokens, width), F32)] * 4 + [
        vm((tokens, width), BF16), vm((tokens, width), BF16), vm((tokens, ff), BF16), vm((tokens, ff), BF16),
        vm((tokens, qdim), BF16), vm((tokens, qkv_dim), BF16), vm((tokens, width), BF16)]
    scratch = [
        vm((width, ff), BF16), vm((ff, width), BF16), vm((width, qkv_dim), BF16), vm((qdim, width), BF16),
        vm((width * n_heads, head_dim), BF16), vm((width * n_heads, head_dim), F32),
        vm((tokens, width), F32), vm((tokens, width), F32),
        vm((N_CHUNKS * piece, width), F32), vm((N_CHUNKS * piece, width), F32),
        vm((tokens, ff), F32), vm((tokens, qkv_dim), BF16), vm((n_heads, tokens, tokens // N_GROUPS), F32),
        vm((N_SUMS, tokens, width), F32), vm((units * half, width), F32),
        vm((2, units * piece, width // 2), F32), vm((2, units * piece, width), F32),
        pltpu.SMEM((n_batch,), jnp.int32), pltpu.SemaphoreType.DMA((14,)), pltpu.SemaphoreType.DMA((2,)), pltpu.SemaphoreType.DMA((9, units // 2)),
    ]
    return pl.pallas_call(
        functools.partial(block_kernel, n_tp, head_dim, seq_len),
        out_shape=out_shape,
        in_specs=[ANY] * 11,
        out_specs=[pl.BlockSpec(memory_space=pltpu.VMEM)] * len(out_shape),
        scratch_shapes=scratch,
        name='block_back',
        compiler_params=pltpu.CompilerParams(collective_id=0, has_side_effects=True,
                                             vmem_limit_bytes=46 * 1024 * 1024),
        cost_estimate=pl.CostEstimate(flops=10 ** 10, bytes_accessed=3 * 10 ** 7, transcendentals=10 ** 6),
    )(seq_lens, *acts, *weights)


def grads_kernel(head_dim, n_blk,
                 x2, dx1, x1, dx2, ng, nf, act, dpre, attn, dqkv, e_val,
                 x2_out, dx1_out, x1_out, dx2_out, dwq_out, dwk_out, dwv_out, dwo_out, dw1_out, dw2_out,
                 c_val, dwq, dwk, dwv, dwo, dw1, dw2, out_sem):
    pairs = ((x2, x2_out), (dx1, dx1_out), (x1, x1_out), (dx2, dx2_out), (dw2, dw2_out), (dw1, dw1_out),
             (dwo, dwo_out), (dwq, dwq_out), (dwk, dwk_out), (dwv, dwv_out))

    def store(i, rows=None):
        src, dst = pairs[i] if rows is None else (ref.at[rows] for ref in pairs[i])
        pltpu.make_async_copy(src, dst, out_sem.at[i]).start()

    store(0)
    store(1)
    width, ff = dw1.shape
    qdim = attn.shape[1]
    n_heads = qdim // head_dim
    rows2, rows1 = ff // n_blk, width // n_blk
    for j in range(n_blk):
        rows = pl.ds(j * rows2, rows2)
        dw2[rows] = mm_tn(act[:, rows], e_val[...])
        store(4, rows)
    for j in range(n_blk):
        rows = pl.ds(j * rows1, rows1)
        dw1[rows] = mm_tn(ng[:, rows], dpre[...])
        store(5, rows)
    store(2)
    store(3)
    c_val[...] = dx1[...].astype(BF16)
    for h in range(n_heads):
        rows = pl.ds(h * head_dim, head_dim)
        dwo[rows] = mm_tn(attn[:, rows], c_val[...])
        store(6, rows)
    for j in range(n_blk // 2):
        step = width // (n_blk // 2)
        rows = pl.ds(j * step, step)
        grad = mm_tn(nf[:, rows], dqkv[...])
        for h in range(n_heads):
            dwq[pl.ds(j * step * n_heads + h, step, stride=n_heads)] = grad[:, h * head_dim:(h + 1) * head_dim]
        dwk[rows] = grad[:, qdim:qdim + head_dim]
        dwv[rows] = grad[:, qdim + head_dim:]
        rows_q = pl.ds(j * step * n_heads, step * n_heads)
        store(7, rows_q)
        store(8, rows)
        store(9, rows)
    for i, (src, dst) in enumerate(pairs):
        pltpu.make_async_copy(src, dst, out_sem.at[i]).wait()


def grads_call(n_heads, head_dim, *saved):
    tokens, width = saved[0].shape
    ff, qdim = saved[6].shape[1], n_heads * head_dim
    sds, vm = jax.ShapeDtypeStruct, pltpu.VMEM
    dw_shapes = [(width * n_heads, head_dim), (width, head_dim), (width, head_dim), (qdim, width), (width, ff), (ff, width)]
    scratch = [vm((tokens, width), BF16)] + [vm(s, F32) for s in dw_shapes] + [pltpu.SemaphoreType.DMA((10,))]
    return pl.pallas_call(
        functools.partial(grads_kernel, head_dim, 8),
        out_shape=[sds((tokens, width), F32)] * 4 + [sds(s, F32) for s in dw_shapes],
        in_specs=[pl.BlockSpec(memory_space=pltpu.VMEM)] * len(saved),
        out_specs=[ANY] * 10,
        scratch_shapes=scratch,
        name='weight_grads',
        compiler_params=pltpu.CompilerParams(vmem_limit_bytes=34 * 1024 * 1024),
        cost_estimate=pl.CostEstimate(flops=4 * 10 ** 9, bytes_accessed=4 * 10 ** 7, transcendentals=0),
    )(*saved)


def solution(mesh):
    n_tp = mesh.shape['tp']
    act_spec = P('dp', None, None)
    w_specs = (P(None, None, 'tp', None), P(None, None, 'tp', None), P(None, None, 'tp', None),
               P(None, 'tp', None, None), P(None, None, 'tp'), P(None, 'tp', None))
    g_specs = (P('dp', None, 'tp', None), P('dp', None, 'tp', None), P('dp', None, 'tp', None),
               P('dp', 'tp', None, None), P('dp', None, 'tp'), P('dp', 'tp', None))

    def local_fn(y_one, y_two, dy_one, dy_two, seq_lens, w_query, w_key, w_value, w_out, w_up, w_down):
        n_heads, head_dim = w_query.shape[2], w_query.shape[3]
        ws = tuple(w[0] for w in (w_query, w_key, w_value, w_out, w_up, w_down))
        saved = block_call(n_tp, seq_lens, y_one, y_two, dy_one, dy_two, *ws)
        res = grads_call(n_heads, head_dim, *saved)
        dw = tuple(g.reshape((1,) + w.shape) for g, w in zip(res[4:], ws))
        return tuple(v.reshape(y_one.shape) for v in (res[2], res[0], res[1], res[3])) + dw

    return jax.shard_map(local_fn, mesh=mesh,
                         in_specs=(act_spec,) * 4 + (P('dp'),) + w_specs,
                         out_specs=(act_spec,) * 4 + g_specs,
                         check_vma=False)
```

```python
import functools
import jax
import jax.numpy as jnp
from jax import lax
from jax.experimental import pallas as pl
from jax.experimental.pallas import tpu as pltpu
from jax.sharding import PartitionSpec as P

F32 = jnp.float32
BF16 = jnp.bfloat16
EPS = 1e-5
MASK_VALUE = -1e30
GELU_C = 0.7978845608028654
GELU_A = 0.044715
MESH = pl.DeviceIdType.MESH
ANY = pl.BlockSpec(memory_space=pl.ANY)

N_CHUNKS = 4
N_GROUPS = 2
N_SUMS = 4
N_MSGS = 16
SEND_SLOT = (0, 0, 0, 0, 0, 0, 0, 1, 1, 0, 0, 1, 0, 1, 1, 1)
RECV_SLOT = (0, 1, 2, 3, 3, 3, 3, 4, 5, 6, 6, 7, 8, 7, 7, 7)

LOAD_US = 4.0
STEP_US = {'G1': 0.7, 'G2': 0.4, 'G3': 0.6, 'G4': 0.5, 'PREP': 0.4, 'ATF': 1.2, 'ATO': 0.2, 'ATB': 1.5, 'ATG': 0.5}
SUM_US = {'F0A': 0.03, 'F0B': 0.03, 'F1A': 0.1, 'F1B': 0.1, 'F2R': 0.05, 'F2L': 0.05, 'F3': 0.25, 'F4R': 0.03,
          'F4L': 0.03, 'F5': 0.03, 'F6': 0.03}
SENDS = {'F0A': (0,), 'F0B': (12,), 'F1A': (1, 4), 'F1B': (2, 3), 'F2R': (5,), 'F2L': (6,), 'F3': (7, 8, 11),
         'F4R': (9, 13), 'F4L': (10, 14), 'F5': (15,)}
RECVS = {'F1A': (0,), 'F1B': (12,), 'F2R': (1,), 'F2L': (2,), 'F3': (3, 4, 5, 6), 'F4R': (7,), 'F4L': (8,), 'F5': (9, 10),
         'F6': (11, 13, 14, 15)}
AFTER = {'F1A': ('F0A',), 'F1B': ('F0B',), 'F2R': ('F1A',), 'F2L': ('F1B',), 'F3': ('F2R', 'F2L'), 'F4R': ('F3',),
         'F4L': ('F3',), 'F5': ('F4R', 'F4L'), 'F6': ('F5',)}
MSG_US = ((0.8, 1.1),) + ((2.8, 2.17),) * 6 + ((5.6, 2.17),) * 2 + ((2.8, 2.17),) * 2 + ((0.4, 1.1), (0.8, 1.1)) + ((0.4, 1.1),) * 3
SAME_CHIP = (0, 11, 12, 13, 14, 15)
RANK = ('G1', 'G2', 'ATF', 'ATO', 'ATB', 'ATG', 'G3', 'G4', 'PREP')
BACKLOG_US = (8.7, 4.2, 2.5, 11.5)
STEP_RANK = {'F0A': 5.4, 'F0B': -2.2, 'F1A': -0.2, 'F1B': -7.9, 'F2R': 5.1, 'F2L': 1.2, 'F3': 2.0, 'F4R': -3.8, 'F4L': -1.6, 'F5': -8.6, 'F6': 1.8}
SUM_RANK = (2.9, 6.4, 2.0, 13.4)
CHUNK_RANK = 4.27


def plan_order():
    per = N_CHUNKS // N_GROUPS
    todo = {}

    def add(key, needs, sends=()):
        todo[key] = (needs, STEP_US[key[0]] if key[0] in STEP_US else SUM_US[key[0]], sends)

    for g in range(N_GROUPS):
        chunks = range(g * per, (g + 1) * per)
        add(('G1', g), [('G2', g - 1, 1)] if g else [])
        add(('ATF', g), [('F6', 0, c) for c in chunks] + [('PREP',)])
        add(('ATB', g), [('F6', 1, c) for c in chunks] + [('ATF', g)])
        for j in range(2):
            add(('G2', g, j), [('G1', g)])
            add(('ATO', g, j), [('ATF', g)])
            add(('ATG', g, j), [('ATB', g)])
    for j in range(2):
        add(('G3', j), [('G1', g) for g in range(N_GROUPS)])
        add(('G4', j), [('G3', 0), ('G3', 1)])
    add(('PREP',), [('G4', 0), ('G4', 1)])
    for c in range(N_CHUNKS):
        g = c // per
        for a in range(N_SUMS):
            for name in SUM_US:
                needs = [(p, a, c) for p in AFTER.get(name, ())] + [(i, a, c) for i in RECVS.get(name, ())]
                if name in ('F0A', 'F0B'):
                    j = int(name == 'F0B')
                    needs.append((('G2', g, j), ('G4', j), ('ATO', g, j), ('ATG', g, j))[a])
                add((name, a, c), needs, SENDS.get(name, ()))

    def rank(key):
        if key[0] in STEP_US:
            return (1, RANK.index(key[0])) + key[1:]
        return (0, STEP_RANK[key[0]] + SUM_RANK[key[1]] + CHUNK_RANK * key[2])

    now, order, done, free = LOAD_US, [], {}, {}
    while todo:
        ready = {}
        for key, (needs, _, sends) in todo.items():
            if all(n in done for n in needs):
                queue = max([free.get(1 + i % 2, 0.0) for i in sends if i not in SAME_CHIP], default=0.0)
                ready[key] = max([done[n] for n in needs] + [queue - (BACKLOG_US[key[1]] if sends else 0.0)])
        now = max(now, min(ready.values()))
        key = min((k for k, at in ready.items() if at <= now), key=rank)
        _, cost, sends = todo.pop(key)
        now += cost
        done[key] = now
        order.append(key)
        for i in sends:
            link = 0 if i in SAME_CHIP else 1 + i % 2
            wire, delay = MSG_US[i]
            start = max(now, free.get(link, 0.0))
            free[link] = start + wire / N_CHUNKS
            done[(i,) + key[1:]] = free[link] + delay
    return order


def mm(lhs, rhs):
    return jnp.dot(lhs, rhs, preferred_element_type=F32)


def mm_nt(lhs, rhs):
    return lax.dot_general(lhs, rhs, (((1,), (1,)), ((), ())), preferred_element_type=F32)


def mm_tn(lhs, rhs):
    return lax.dot_general(lhs, rhs, (((0,), (0,)), ((), ())), preferred_element_type=F32)


def inv_rms(x_val):
    return lax.rsqrt(jnp.mean(x_val * x_val, axis=-1, keepdims=True) + EPS)


def rms_back(x_val, grad_norm):
    inv = inv_rms(x_val)
    normed = x_val * inv
    return inv * (grad_norm - normed * jnp.mean(grad_norm * normed, axis=-1, keepdims=True))


def block_kernel(n_tp, head_dim, seq_len,
                 lens_hbm, y1_hbm, y2_hbm, dy1_hbm, dy2_hbm, wq_hbm, wk_hbm, wv_hbm, wo_hbm, w1_hbm, w2_hbm,
                 x2, dx1, x1, dx2, ng, nf, act, dpre, attn, dqkv, dyb,
                 w1, w2, wqkv, wo, wq_raw, wq_f, y1, dy2, y2_own, dy1_own, dact, qkv, prob,
                 part, d2d, ring1, ring2,
                 lens, load_sem, send_sem, recv_sem):
    full = (x2, dx1, x1, dx2)
    tokens, width = y1.shape
    ff = w1.shape[1]
    qdim = attn.shape[1]
    n_heads = qdim // head_dim
    chunk = tokens // N_CHUNKS
    half = chunk // 2
    piece = half // (n_tp // 2)
    hw = width // 2
    n_chips = n_tp // 2

    me = lax.axis_index('tp')
    core = lax.rem(me, 2)
    chip = lax.div(me, 2)
    partner = me + 1 - 2 * core
    right = lax.rem(me + 2, n_tp)
    left = lax.rem(me + n_tp - 2, n_tp)
    chip_r = lax.rem(chip + 1, n_chips)
    chip_l = lax.rem(chip + n_chips - 1, n_chips)
    chip_o = lax.rem(chip + 2, n_chips)

    def half_rows(c, k):
        return pl.ds(pl.multiple_of(c * chunk + k * half, half), half)

    def piece_rows(c, x):
        return pl.ds(pl.multiple_of(c * chunk + core * half + x * piece, piece), piece)

    def own_rows(c):
        return pl.ds(c * piece, piece)

    lo, hi = pl.ds(0, hw), pl.ds(hw, hw)

    loads = {}

    def arrived(*names):
        for name in names:
            if name in loads:
                loads.pop(name).wait()

    n_blk = ff // 512

    free_sems = list(range(14))

    def load(name, *copies):
        sem = load_sem.at[free_sems.pop(0)]
        for src, dst in copies:
            pltpu.make_async_copy(src, dst, sem).start()
        whole = copies[0][1] if len(copies) == 1 else {'y2': y2_own, 'dy1': dy1_own}[name[0]]
        loads[name] = pltpu.make_async_copy(whole, whole, sem)

    def load_first():
        groups = [pl.ds(g * (tokens // N_GROUPS), tokens // N_GROUPS) for g in range(N_GROUPS)]
        load(('y1', 0), (y1_hbm.at[groups[0]], y1.at[groups[0]]))
        for j in range(n_blk):
            blk = pl.ds(j * 512, 512)
            load(('w1', j), (w1_hbm.at[:, blk], w1.at[:, blk]))
        for j, cols in enumerate((lo, hi)):
            load(('w2', j), (w2_hbm.at[:, cols], w2.at[:, cols]))
        for g in range(1, N_GROUPS):
            load(('y1', g), (y1_hbm.at[groups[g]], y1.at[groups[g]]))

    def load_rest():
        load(('dy2',), (dy2_hbm, dy2))
        load(('y2',), *((y2_hbm.at[piece_rows(c, chip)], y2_own.at[own_rows(c)]) for c in range(N_CHUNKS)))
        load(('dy1',), *((dy1_hbm.at[piece_rows(c, chip)], dy1_own.at[own_rows(c)]) for c in range(N_CHUNKS)))
        load(('wq',), (wq_hbm, wq_raw))
        load(('wk',), (wk_hbm, wqkv.at[:, pl.ds(qdim, head_dim)]))
        load(('wv',), (wv_hbm, wqkv.at[:, pl.ds(qdim + head_dim, head_dim)]))
        load(('wo',), (wo_hbm, wo))
        load(('lens',), (lens_hbm, lens))

    def shared(a, c):
        return a % 2 * N_CHUNKS + c

    def msg(a, c, i):
        rows_own, rows_r, rows_l, rows_o = (piece_rows(c, x) for x in (chip, chip_r, chip_l, chip_o))
        u = a * N_CHUNKS + c
        slot = pl.ds(u * piece, piece)
        pa, oa = part.at[a], full[a]
        if i == 0:
            src, dst, dev = pa.at[half_rows(c, 1 - core), lo], d2d.at[pl.ds(u * half, half), lo], partner
        elif i == 12:
            src, dst, dev = pa.at[half_rows(c, 1 - core), hi], d2d.at[pl.ds(u * half, half), hi], partner
        elif i == 1:
            src, dst, dev = pa.at[rows_o, lo], ring1.at[0, slot], right
        elif i == 2:
            src, dst, dev = pa.at[rows_o, hi], ring1.at[1, slot], left
        elif i == 3:
            src, dst, dev = pa.at[rows_r, hi], ring2.at[0, slot, hi], right
        elif i == 4:
            src, dst, dev = pa.at[rows_l, lo], ring2.at[1, slot, lo], left
        elif i == 5:
            src, dst, dev = pa.at[rows_r, lo], ring2.at[0, slot, lo], right
        elif i == 6:
            src, dst, dev = pa.at[rows_l, hi], ring2.at[1, slot, hi], left
        elif i == 7:
            src, dst, dev = oa.at[rows_own], oa.at[rows_own], right
        elif i == 8:
            src, dst, dev = oa.at[rows_own], oa.at[rows_own], left
        elif i == 9:
            src, dst, dev = oa.at[rows_l, lo], oa.at[rows_l, lo], right
        elif i == 10:
            src, dst, dev = oa.at[rows_r, hi], oa.at[rows_r, hi], left
        else:
            rows = {11: rows_own, 13: rows_l, 14: rows_r, 15: rows_o}[i]
            src, dst, dev = oa.at[rows], oa.at[rows], partner
        return pltpu.make_async_remote_copy(src, dst, send_sem.at[SEND_SLOT[i]], recv_sem.at[RECV_SLOT[i], shared(a, c)],
                                            device_id={'tp': dev}, device_id_type=MESH)

    def send(a, c, *ids):
        for i in ids:
            msg(a, c, i).start()

    def recv(a, c, *slots):
        u = pl.ds((a * N_CHUNKS + c) * piece, piece)
        own = full[a].at[piece_rows(c, chip)]
        pair = pl.ds((a * N_CHUNKS + c) * half, half)
        whole = (d2d.at[pair, lo], ring1.at[0, u], ring1.at[1, u], ring2.at[:, u],
                 own, own, own, full[a].at[half_rows(c, core)], d2d.at[pair, hi])
        for s in slots:
            pltpu.make_async_copy(whole[s], whole[s], recv_sem.at[s, shared(a, c)]).wait()

    state = {'met': False}

    def met():
        if not state['met']:
            pl.semaphore_wait(barrier, 3)
            state['met'] = True

    def f0a(a, c):
        met()
        send(a, c, 0)

    def f0b(a, c):
        met()
        send(a, c, 12)

    def add_pair(a, c, cols):
        rows = half_rows(c, core)
        part[a, rows, cols] = part[a, rows, cols] + d2d[pl.ds((a * N_CHUNKS + c) * half, half), cols]

    def f1a(a, c):
        recv(a, c, 0)
        add_pair(a, c, lo)
        send(a, c, 1, 4)

    def f1b(a, c):
        recv(a, c, 8)
        add_pair(a, c, hi)
        send(a, c, 2, 3)

    def f2r(a, c):
        recv(a, c, 1)
        rows = piece_rows(c, chip_r)
        part[a, rows, lo] = part[a, rows, lo] + ring1[0, pl.ds((a * N_CHUNKS + c) * piece, piece)]
        send(a, c, 5)

    def f2l(a, c):
        recv(a, c, 2)
        rows = piece_rows(c, chip_l)
        part[a, rows, hi] = part[a, rows, hi] + ring1[1, pl.ds((a * N_CHUNKS + c) * piece, piece)]
        send(a, c, 6)

    def f3(a, c):
        recv(a, c, 3)
        rows = piece_rows(c, chip)
        slot = pl.ds((a * N_CHUNKS + c) * piece, piece)
        total = part[a, rows] + ring2[0, slot] + ring2[1, slot]
        if a == 0:
            arrived(('y2',))
            out = y2_own[own_rows(c)] - total
        elif a == 1:
            arrived(('dy1',))
            out = dy1_own[own_rows(c)] + rms_back(y1[rows], total)
        elif a == 2:
            out = y1[rows] - total
        else:
            out = dy2[rows] + rms_back(x2[rows], total)
        full[a][rows] = out
        send(a, c, 7, 8, 11)

    def f4r(a, c):
        recv(a, c, 4)
        send(a, c, 9, 13)

    def f4l(a, c):
        recv(a, c, 5)
        send(a, c, 10, 14)

    def f5(a, c):
        recv(a, c, 6)
        send(a, c, 15)

    def f6(a, c):
        recv(a, c, 7)

    group = tokens // N_GROUPS

    def group_rows(g):
        return pl.ds(g * group, group)

    def g1(g):
        rows = group_rows(g)
        arrived(('y1', g))
        y_val = y1[rows]
        ng[rows] = (y_val * inv_rms(y_val)).astype(BF16)
        for j in range(n_blk):
            cols = pl.ds(j * 512, 512)
            arrived(('w1', j))
            pre = mm(ng[rows], w1[:, cols])
            th = jnp.tanh(GELU_C * (pre + GELU_A * (pre * pre * pre)))
            act[rows, cols] = (0.5 * pre * (1.0 + th)).astype(BF16)
            dact[rows, cols] = 0.5 * (1.0 + th) + (0.5 * pre) * (1.0 - th * th) * (
                GELU_C * (1.0 + (3.0 * GELU_A) * (pre * pre)))

    def g2(g, j):
        rows, cols = group_rows(g), (lo, hi)[j]
        arrived(('w2', j))
        if g == 0 and j == 1:
            load_rest()
        part[0, rows, cols] = mm(act[rows], w2[:, cols])

    def g3(j):
        arrived(('dy2',))
        cols = pl.ds(j * (ff // 2), ff // 2)
        if j == 0:
            dyb[...] = dy2[...].astype(BF16)
        dpre[:, cols] = (dact[:, cols] * mm_nt(dyb[...], w2[cols])).astype(BF16)

    def g4(j):
        cols = (lo, hi)[j]
        part[1, :, cols] = mm_nt(dpre[...], w1[cols])

    def prep():
        arrived(('wq',))
        wq_f[...] = wq_raw[...].astype(F32)
        for h in range(n_heads):
            wqkv[:, pl.ds(h * head_dim, head_dim)] = wq_f[pl.ds(h, width, stride=n_heads)].astype(BF16)

    def atf(g):
        rows = group_rows(g)
        arrived(('wk',), ('wv',), ('lens',))
        x_val = x2[rows]
        nf[rows] = (x_val * inv_rms(x_val)).astype(BF16)
        qkv[rows] = mm(nf[rows], wqkv[...]).astype(BF16)
        key = qkv[rows, pl.ds(qdim, head_dim)]
        val = qkv[rows, pl.ds(qdim + head_dim, head_dim)]
        n_seqs = group // seq_len
        row_pos = lax.broadcasted_iota(jnp.int32, (group, group), 0)
        col_pos = lax.broadcasted_iota(jnp.int32, (group, group), 1)
        visible = jnp.zeros((group, group), jnp.bool_)
        for s in range(n_seqs):
            base = s * seq_len
            stop = base + lens[g * n_seqs + s]
            visible = visible | ((row_pos >= base) & (row_pos < base + seq_len)
                                 & (col_pos >= base) & (col_pos < stop) & (col_pos <= row_pos))
        for h in range(n_heads):
            cols = pl.ds(h * head_dim, head_dim)
            scores = mm_nt(qkv[rows, cols], key) * (head_dim ** -0.5)
            scores = jnp.where(visible, scores, MASK_VALUE)
            exps = jnp.exp(scores - jnp.max(scores, axis=-1, keepdims=True))
            probs = exps / jnp.sum(exps, axis=-1, keepdims=True)
            prob[h, rows] = probs
            attn[rows, cols] = mm(probs.astype(BF16), val).astype(BF16)

    def ato(g, j):
        rows, cols = group_rows(g), (lo, hi)[j]
        arrived(('wo',))
        part[2, rows, cols] = mm(attn[rows], wo[:, cols])

    def atb(g):
        rows = group_rows(g)
        d_attn = mm_nt(dx1[rows].astype(BF16), wo[...]).astype(BF16)
        key = qkv[rows, pl.ds(qdim, head_dim)]
        val = qkv[rows, pl.ds(qdim + head_dim, head_dim)]
        d_key = jnp.zeros((group, head_dim), F32)
        d_val = jnp.zeros((group, head_dim), F32)
        for h in range(n_heads):
            cols = pl.ds(h * head_dim, head_dim)
            d_head = d_attn[:, h * head_dim:(h + 1) * head_dim]
            probs = prob[h, rows]
            d_probs = mm_nt(d_head, val)
            d_scores = probs * (d_probs - jnp.sum(probs * d_probs, axis=-1, keepdims=True)) * (head_dim ** -0.5)
            d_scores = d_scores.astype(BF16)
            dqkv[rows, cols] = mm(d_scores, key).astype(BF16)
            d_key = d_key + mm_tn(d_scores, qkv[rows, cols])
            d_val = d_val + mm_tn(probs.astype(BF16), d_head)
        dqkv[rows, pl.ds(qdim, head_dim)] = d_key.astype(BF16)
        dqkv[rows, pl.ds(qdim + head_dim, head_dim)] = d_val.astype(BF16)

    def atg(g, j):
        rows, cols = group_rows(g), (lo, hi)[j]
        part[3, rows, cols] = mm_nt(dqkv[rows], wqkv[cols])

    steps = {'F0A': f0a, 'F0B': f0b, 'F1A': f1a, 'F1B': f1b, 'F2R': f2r, 'F2L': f2l, 'F3': f3, 'F4R': f4r, 'F4L': f4l, 'F5': f5, 'F6': f6,
             'G1': g1, 'G2': g2, 'G3': g3, 'G4': g4, 'PREP': prep, 'ATF': atf, 'ATO': ato, 'ATB': atb, 'ATG': atg}
    load_first()
    barrier = pltpu.get_barrier_semaphore()
    for dev in (partner, left, right):
        pl.semaphore_signal(barrier, inc=1, device_id={'tp': dev}, device_id_type=MESH)
    for name, *where in plan_order():
        steps[name](*where)
    for i, sent in enumerate((part, part.at[pl.ds(0, 3)])):
        pltpu.make_async_copy(sent, sent, send_sem.at[i]).wait()


def block_call(n_tp, seq_lens, y_one, y_two, dy_one, dy_two, w_query, w_key, w_value, w_out, w_up, w_down):
    n_batch, seq_len, width = y_one.shape
    tokens = n_batch * seq_len
    n_heads, head_dim = w_query.shape[1], w_query.shape[2]
    ff = w_up.shape[1]
    qdim = n_heads * head_dim
    qkv_dim = qdim + 2 * head_dim
    units = N_SUMS * N_CHUNKS
    half = tokens // N_CHUNKS // 2
    piece = half // (n_tp // 2)
    acts = tuple(v.reshape(tokens, width) for v in (y_one, y_two, dy_one, dy_two))
    weights = (w_query.reshape(width * n_heads, head_dim), w_key.reshape(width, head_dim), w_value.reshape(width, head_dim),
               w_out.reshape(qdim, width), w_up, w_down)
    vm = pltpu.VMEM
    out_shape = [vm((tokens, width), F32)] * 4 + [
        vm((tokens, width), BF16), vm((tokens, width), BF16), vm((tokens, ff), BF16), vm((tokens, ff), BF16),
        vm((tokens, qdim), BF16), vm((tokens, qkv_dim), BF16), vm((tokens, width), BF16)]
    scratch = [
        vm((width, ff), BF16), vm((ff, width), BF16), vm((width, qkv_dim), BF16), vm((qdim, width), BF16),
        vm((width * n_heads, head_dim), BF16), vm((width * n_heads, head_dim), F32),
        vm((tokens, width), F32), vm((tokens, width), F32),
        vm((N_CHUNKS * piece, width), F32), vm((N_CHUNKS * piece, width), F32),
        vm((tokens, ff), F32), vm((tokens, qkv_dim), BF16), vm((n_heads, tokens, tokens // N_GROUPS), F32),
        vm((N_SUMS, tokens, width), F32), vm((units * half, width), F32),
        vm((2, units * piece, width // 2), F32), vm((2, units * piece, width), F32),
        pltpu.SMEM((n_batch,), jnp.int32), pltpu.SemaphoreType.DMA((14,)), pltpu.SemaphoreType.DMA((2,)), pltpu.SemaphoreType.DMA((9, units // 2)),
    ]
    return pl.pallas_call(
        functools.partial(block_kernel, n_tp, head_dim, seq_len),
        out_shape=out_shape,
        in_specs=[ANY] * 11,
        out_specs=[pl.BlockSpec(memory_space=pltpu.VMEM)] * len(out_shape),
        scratch_shapes=scratch,
        name='block_back',
        compiler_params=pltpu.CompilerParams(collective_id=0, has_side_effects=True,
                                             vmem_limit_bytes=46 * 1024 * 1024),
        cost_estimate=pl.CostEstimate(flops=10 ** 10, bytes_accessed=3 * 10 ** 7, transcendentals=10 ** 6),
    )(seq_lens, *acts, *weights)


def grads_kernel(head_dim, n_blk,
                 x2, dx1, x1, dx2, ng, nf, act, dpre, attn, dqkv, e_val,
                 x2_out, dx1_out, x1_out, dx2_out, dwq_out, dwk_out, dwv_out, dwo_out, dw1_out, dw2_out,
                 c_val, dwq, dwk, dwv, dwo, dw1, dw2, out_sem):
    pairs = ((x2, x2_out), (dx1, dx1_out), (x1, x1_out), (dx2, dx2_out), (dw2, dw2_out), (dw1, dw1_out),
             (dwo, dwo_out), (dwq, dwq_out), (dwk, dwk_out), (dwv, dwv_out))

    def store(i, rows=None):
        src, dst = pairs[i] if rows is None else (ref.at[rows] for ref in pairs[i])
        pltpu.make_async_copy(src, dst, out_sem.at[i]).start()

    store(0)
    store(1)
    width, ff = dw1.shape
    qdim = attn.shape[1]
    n_heads = qdim // head_dim
    rows2, rows1 = ff // n_blk, width // n_blk
    for j in range(n_blk):
        rows = pl.ds(j * rows2, rows2)
        dw2[rows] = mm_tn(act[:, rows], e_val[...])
        store(4, rows)
    for j in range(n_blk):
        rows = pl.ds(j * rows1, rows1)
        dw1[rows] = mm_tn(ng[:, rows], dpre[...])
        store(5, rows)
    store(2)
    store(3)
    c_val[...] = dx1[...].astype(BF16)
    for h in range(n_heads):
        rows = pl.ds(h * head_dim, head_dim)
        dwo[rows] = mm_tn(attn[:, rows], c_val[...])
        store(6, rows)
    for j in range(n_blk // 2):
        step = width // (n_blk // 2)
        rows = pl.ds(j * step, step)
        grad = mm_tn(nf[:, rows], dqkv[...])
        for h in range(n_heads):
            dwq[pl.ds(j * step * n_heads + h, step, stride=n_heads)] = grad[:, h * head_dim:(h + 1) * head_dim]
        dwk[rows] = grad[:, qdim:qdim + head_dim]
        dwv[rows] = grad[:, qdim + head_dim:]
        rows_q = pl.ds(j * step * n_heads, step * n_heads)
        store(7, rows_q)
        store(8, rows)
        store(9, rows)
    for i, (src, dst) in enumerate(pairs):
        pltpu.make_async_copy(src, dst, out_sem.at[i]).wait()


def grads_call(n_heads, head_dim, *saved):
    tokens, width = saved[0].shape
    ff, qdim = saved[6].shape[1], n_heads * head_dim
    sds, vm = jax.ShapeDtypeStruct, pltpu.VMEM
    dw_shapes = [(width * n_heads, head_dim), (width, head_dim), (width, head_dim), (qdim, width), (width, ff), (ff, width)]
    scratch = [vm((tokens, width), BF16)] + [vm(s, F32) for s in dw_shapes] + [pltpu.SemaphoreType.DMA((10,))]
    return pl.pallas_call(
        functools.partial(grads_kernel, head_dim, 8),
        out_shape=[sds((tokens, width), F32)] * 4 + [sds(s, F32) for s in dw_shapes],
        in_specs=[pl.BlockSpec(memory_space=pltpu.VMEM)] * len(saved),
        out_specs=[ANY] * 10,
        scratch_shapes=scratch,
        name='weight_grads',
        compiler_params=pltpu.CompilerParams(vmem_limit_bytes=34 * 1024 * 1024),
        cost_estimate=pl.CostEstimate(flops=4 * 10 ** 9, bytes_accessed=4 * 10 ** 7, transcendentals=0),
    )(*saved)


def solution(mesh):
    n_tp = mesh.shape['tp']
    act_spec = P('dp', None, None)
    w_specs = (P(None, None, 'tp', None), P(None, None, 'tp', None), P(None, None, 'tp', None),
               P(None, 'tp', None, None), P(None, None, 'tp'), P(None, 'tp', None))
    g_specs = (P('dp', None, 'tp', None), P('dp', None, 'tp', None), P('dp', None, 'tp', None),
               P('dp', 'tp', None, None), P('dp', None, 'tp'), P('dp', 'tp', None))

    def local_fn(y_one, y_two, dy_one, dy_two, seq_lens, w_query, w_key, w_value, w_out, w_up, w_down):
        n_heads, head_dim = w_query.shape[2], w_query.shape[3]
        ws = tuple(w[0] for w in (w_query, w_key, w_value, w_out, w_up, w_down))
        saved = block_call(n_tp, seq_lens, y_one, y_two, dy_one, dy_two, *ws)
        res = grads_call(n_heads, head_dim, *saved)
        dw = tuple(g.reshape((1,) + w.shape) for g, w in zip(res[4:], ws))
        return tuple(v.reshape(y_one.shape) for v in (res[2], res[0], res[1], res[3])) + dw

    return jax.shard_map(local_fn, mesh=mesh,
                         in_specs=(act_spec,) * 4 + (P('dp'),) + w_specs,
                         out_specs=(act_spec,) * 4 + g_specs,
                         check_vma=False)
```
